128 devices in a mesh: pp: 2 (over core), ep: 64 (over z, y, x).
Axes of the slice: x: 4, y: 4, z: 4, core: 2. Of those that a mesh axis runs over, the one named last changes fastest.
Arguments:
- expert_out: bfloat16 [2, 64, 1536, 2048], P('pp', 'ep')
- expert_ids: int32 [2, 64, 128, 8], P('pp', 'ep')
- slot_ids: int32 [2, 64, 128, 8], P('pp', 'ep')
- gate_vals: float32 [2, 64, 128, 8], P('pp', 'ep')
- residual: bfloat16 [2, 64, 128, 2048], P('pp', 'ep')
- norm_w: float32 [2, 2048], P('pp')
- w_query: bfloat16 [2, 2048, 16, 128], P('pp')
- w_key: bfloat16 [2, 2048, 16, 128], P('pp')
- w_value: bfloat16 [2, 2048, 16, 128], P('pp')
- w_out: bfloat16 [2, 16, 128, 2048], P('pp')
Outputs:
- output: bfloat16 [2, 64, 128, 2048], P('pp', 'ep')
All inputs are finite; a program needn't handle non-finite values.
Results may differ from the reference program's by a relative error of at most 0.0133245.
Values are sent between devices in bfloat16 or wider.
A program may use at most 1 GiB of HBM per device.

```python
import jax
import jax.numpy as jnp
from jax import lax

STAGES = 2
GROUP_SIZE = 64
NUM_MICRO = 1
SEQ_LEN = 128
SEQS_PER_DEV = 1
D_MODEL = 2048
NUM_EXPERTS = 64
TOP_K = 8
NUM_HEADS = 16
HEAD_DIM = 128
SRC_SLOTS = 24

TOKENS_DEV = SEQS_PER_DEV * SEQ_LEN
SEQS_ALL = GROUP_SIZE * SEQS_PER_DEV
CAPACITY = GROUP_SIZE * SRC_SLOTS
NUM_ROWS = STAGES * NUM_MICRO
QKV_WIDTH = NUM_HEADS * HEAD_DIM
NORM_EPS = 1e-6


def block_ranks(block_ids):
    perm_order = jnp.argsort(block_ids, stable=True)
    sorted_ids = block_ids[perm_order]
    group_start = jnp.searchsorted(sorted_ids, sorted_ids, side='left')
    rank_sorted = jnp.arange(block_ids.shape[0]) - group_start
    return jnp.zeros_like(block_ids).at[perm_order].set(rank_sorted)


def draw_routing(route_key):
    key_bias, key_hot, key_shift, key_noise, key_order = jax.random.split(route_key, 5)
    expert_bias = jnp.sum(jax.random.randint(key_bias, (NUM_ROWS, NUM_EXPERTS, 4), 0, 166, jnp.int32), axis=-1)
    hot_expert = jax.random.randint(key_hot, (NUM_ROWS,), 0, NUM_EXPERTS)
    cover_shift = jax.random.randint(key_shift, (NUM_ROWS,), 0, NUM_EXPERTS)
    local_pos = jnp.arange(TOKENS_DEV)
    expert_pos = jnp.arange(NUM_EXPERTS)
    tie_break = (NUM_EXPERTS - 1 - expert_pos).astype(jnp.int32)

    def one_block(flat_idx):
        row_idx = flat_idx // GROUP_SIZE
        blk_idx = flat_idx % GROUP_SIZE
        noise_draws = jnp.sum(jax.random.randint(jax.random.fold_in(key_noise, flat_idx), (TOKENS_DEV, NUM_EXPERTS, 3), 0, 164, jnp.int32), axis=-1)
        token_pos = blk_idx * TOKENS_DEV + local_pos
        is_cover = (token_pos[:, None] + cover_shift[row_idx]) % NUM_EXPERTS == expert_pos[None, :]
        is_hot = expert_pos[None, :] == hot_expert[row_idx]
        score_int = (expert_bias[row_idx][None, :] + noise_draws) * NUM_EXPERTS + tie_break[None, :] + (1 << 22) * is_cover.astype(jnp.int32) + (1 << 23) * is_hot.astype(jnp.int32)
        chosen = lax.top_k(score_int, TOP_K)[1]
        order_bits = jax.random.bits(jax.random.fold_in(key_order, flat_idx), (TOKENS_DEV, TOP_K), jnp.uint32) >> 8
        order_key = order_bits * TOP_K + jnp.arange(TOP_K, dtype=jnp.uint32)[None, :]
        perm_order = jnp.argsort(order_key, axis=1)
        chosen = jnp.take_along_axis(chosen, perm_order, axis=1)
        slot_rank = block_ranks(chosen.reshape(TOKENS_DEV * TOP_K)).reshape(TOKENS_DEV, TOP_K)
        slot_ids = jnp.where(slot_rank < SRC_SLOTS, blk_idx * SRC_SLOTS + slot_rank, -1)
        return chosen.astype(jnp.int32), slot_ids.astype(jnp.int32)

    expert_ids, slot_ids = lax.map(one_block, jnp.arange(NUM_ROWS * GROUP_SIZE))
    route_shape = (NUM_ROWS, SEQS_ALL, SEQ_LEN, TOP_K)
    return expert_ids.reshape(route_shape), slot_ids.reshape(route_shape)


def draw_bf16(draw_key, arr_shape, scale_fac):
    def one_slice(slice_key):
        return (scale_fac * jax.random.normal(slice_key, arr_shape[1:], jnp.float32)).astype(jnp.bfloat16)
    return lax.map(one_slice, jax.random.split(draw_key, arr_shape[0]))


def setup_inputs(seed: int = 0) -> dict:
    root_key = jax.random.key(seed)
    sub_keys = jax.random.split(root_key, 10)
    expert_ids, slot_ids = draw_routing(sub_keys[0])
    gate_vals = jax.nn.softmax(1.5 * jax.random.normal(sub_keys[1], (NUM_ROWS, SEQS_ALL, SEQ_LEN, TOP_K), jnp.float32), axis=-1)
    expert_scale = 1.5 * jnp.exp(0.5 * jax.random.normal(sub_keys[2], (NUM_ROWS * NUM_EXPERTS,), jnp.float32))

    def expert_slab(slab_args):
        slab_key, slab_scale = slab_args
        return (slab_scale * jax.random.normal(slab_key, (CAPACITY, D_MODEL), jnp.float32)).astype(jnp.bfloat16)

    expert_out = lax.map(expert_slab, (jax.random.split(sub_keys[3], NUM_ROWS * NUM_EXPERTS), expert_scale))
    expert_out = expert_out.reshape(NUM_ROWS, NUM_EXPERTS, CAPACITY, D_MODEL)
    residual = draw_bf16(sub_keys[4], (NUM_ROWS * SEQS_ALL, SEQ_LEN, D_MODEL), 1.0)
    residual = residual.reshape(NUM_ROWS, SEQS_ALL, SEQ_LEN, D_MODEL)
    norm_w = 1.0 + 0.4 * jax.random.normal(sub_keys[5], (STAGES, D_MODEL), jnp.float32)
    in_scale = D_MODEL ** -0.5
    out_scale = QKV_WIDTH ** -0.5
    w_query = draw_bf16(sub_keys[6], (STAGES, D_MODEL, NUM_HEADS, HEAD_DIM), 1.5 * in_scale)
    w_key = draw_bf16(sub_keys[7], (STAGES, D_MODEL, NUM_HEADS, HEAD_DIM), 1.5 * in_scale)
    w_value = draw_bf16(sub_keys[8], (STAGES, D_MODEL, NUM_HEADS, HEAD_DIM), in_scale)
    w_out = draw_bf16(sub_keys[9], (STAGES, NUM_HEADS, HEAD_DIM, D_MODEL), out_scale)
    return dict(expert_out=expert_out, expert_ids=expert_ids, slot_ids=slot_ids, gate_vals=gate_vals, residual=residual, norm_w=norm_w, w_query=w_query, w_key=w_key, w_value=w_value, w_out=w_out)


def reference(expert_out, expert_ids, slot_ids, gate_vals, residual, norm_w, w_query, w_key, w_value, w_out):
    causal = jnp.arange(SEQ_LEN)[:, None] >= jnp.arange(SEQ_LEN)[None, :]

    def one_stage(stage_idx):
        src_stage = (stage_idx + STAGES - 1) % STAGES
        stage_norm = norm_w[stage_idx]
        stage_wq = w_query[stage_idx].reshape(D_MODEL, QKV_WIDTH)
        stage_wk = w_key[stage_idx].reshape(D_MODEL, QKV_WIDTH)
        stage_wv = w_value[stage_idx].reshape(D_MODEL, QKV_WIDTH)
        stage_wo = w_out[stage_idx].reshape(QKV_WIDTH, D_MODEL)

        def project(x_in, weight_mat):
            head_out = jnp.dot(x_in, weight_mat, preferred_element_type=jnp.float32).astype(jnp.bfloat16)
            return head_out.reshape(SEQ_LEN, NUM_HEADS, HEAD_DIM).astype(jnp.float32)

        def one_sequence(flat_idx):
            src_row = src_stage * NUM_MICRO + flat_idx // SEQS_ALL
            seq_idx = flat_idx % SEQS_ALL
            ids_seq = expert_ids[src_row, seq_idx]
            slot_seq = slot_ids[src_row, seq_idx]
            is_kept = slot_seq >= 0
            picked = expert_out[src_row, ids_seq, jnp.where(is_kept, slot_seq, 0)].astype(jnp.float32)
            weight = jnp.where(is_kept, gate_vals[src_row, seq_idx], 0.0)
            mixed_sum = residual[src_row, seq_idx].astype(jnp.float32) + jnp.sum(weight[:, :, None] * picked, axis=1)
            y_wide = mixed_sum.astype(jnp.bfloat16).astype(jnp.float32)
            inv_rms = lax.rsqrt(jnp.mean(y_wide * y_wide, axis=-1, keepdims=True) + NORM_EPS)
            x_in = (y_wide * inv_rms * stage_norm).astype(jnp.bfloat16)
            q_heads = project(x_in, stage_wq)
            k_heads = project(x_in, stage_wk)
            v_heads = project(x_in, stage_wv)
            scores = jnp.einsum('qhe,khe->hqk', q_heads, k_heads) * HEAD_DIM ** -0.5
            attn_probs = jax.nn.softmax(jnp.where(causal, scores, -jnp.inf), axis=-1).astype(jnp.bfloat16)
            attn_out = jnp.einsum('hqk,khe->qhe', attn_probs.astype(jnp.float32), v_heads).astype(jnp.bfloat16)
            out_proj = jnp.dot(attn_out.reshape(SEQ_LEN, QKV_WIDTH), stage_wo, preferred_element_type=jnp.float32).astype(jnp.bfloat16)
            return (y_wide + out_proj.astype(jnp.float32)).astype(jnp.bfloat16)

        return lax.map(one_sequence, jnp.arange(NUM_MICRO * SEQS_ALL))

    stage_outs = lax.map(one_stage, jnp.arange(STAGES))
    return stage_outs.reshape(NUM_ROWS, SEQS_ALL, SEQ_LEN, D_MODEL)
```

```python
import functools
import itertools

import jax
import jax.numpy as jnp
from jax import lax
from jax.experimental import pallas as pl
from jax.experimental.pallas import tpu as pltpu
from jax.sharding import PartitionSpec as P

NORM_EPS = 1e-6
MESH = pl.DeviceIdType.MESH
SIDE = 4
CHUNKS = 4
CLASSES = [c for c in itertools.product((0, 1), repeat=3) if any(c)]
CLASS_SIZE = [3 ** (3 - sum(c)) for c in CLASSES]
CLASS_BASE = [sum(CLASS_SIZE[:k]) for k in range(len(CLASSES))]
RELAYED = sum(CLASS_SIZE)
DIRECT = 27


def exchange_kernel(o_ref, kg_ref, h_ref, y_ref, rows, relay, kg_in, h_in, g_mat, side_sem, dir_send, dir_recv, leg1_send, leg1_recv, leg2_send):
    stage = lax.axis_index('pp')
    me = lax.axis_index('ep')
    other = 1 - stage
    pos = (me // 16, (me // 4) % 4, me % 4)
    sign = [1 - 2 * (p % 2) for p in pos]
    slots = rows.shape[2]
    width = rows.shape[3]
    seq, k_rows = g_mat.shape[0] // 3, g_mat.shape[1]

    def at(offset):
        z, y, x = [lax.rem(p + d + SIDE, SIDE) for p, d in zip(pos, offset)]
        return z * 16 + y * 4 + x

    def cube(i):
        return (i // 9 - 1, (i // 3) % 3 - 1, i % 3 - 1)

    def free_offset(cls, i):
        out = []
        for c in cls:
            if c:
                out.append(0)
            else:
                out.append(i % 3 - 1)
                i = i // 3
        return out

    barrier = pltpu.get_barrier_semaphore()

    def hello(i, carry):
        pl.semaphore_signal(barrier, inc=1, device_id=(other, at(cube(i))), device_id_type=MESH)
        return carry

    lax.fori_loop(0, DIRECT, hello, 0)
    for cls in CLASSES:
        peer = at([s * c for s, c in zip(sign, cls)])
        pl.semaphore_signal(barrier, inc=1, device_id=(stage, peer), device_id_type=MESH)
    pl.semaphore_wait(barrier, DIRECT + len(CLASSES))

    side = [
        pltpu.make_async_remote_copy(src_ref=src, dst_ref=dst, send_sem=side_sem.at[0, k], recv_sem=side_sem.at[1, k], device_id=(other, me), device_id_type=MESH)
        for k, (src, dst) in enumerate(((kg_ref, kg_in), (h_ref, h_in)))
    ]
    for copy in side:
        copy.start()

    def block(dest, f):
        return o_ref.at[dest, :, pl.ds(f * width, width)]

    def start_direct(f):
        def body(i, carry):
            dest = at(cube(i))
            pltpu.make_async_remote_copy(src_ref=block(dest, f), dst_ref=rows.at[f, me], send_sem=dir_send.at[f], recv_sem=dir_recv.at[f], device_id=(other, dest), device_id_type=MESH).start()
            return carry
        lax.fori_loop(0, DIRECT, body, 0)

    def start_leg1(f):
        for k, cls in enumerate(CLASSES):
            peer = at([s * c for s, c in zip(sign, cls)])

            def body(i, carry):
                dest = at([2 * c + o for c, o in zip(cls, free_offset(cls, i))])
                pltpu.make_async_remote_copy(src_ref=block(dest, f), dst_ref=relay.at[f, CLASS_BASE[k] + i], send_sem=leg1_send.at[f], recv_sem=leg1_recv.at[f, k], device_id=(stage, peer), device_id_type=MESH).start()
                return carry
            lax.fori_loop(0, CLASS_SIZE[k], body, 0)

    def forward(f):
        for k, cls in enumerate(CLASSES):
            source = at([s * c for s, c in zip(sign, cls)])
            held = relay.at[f, pl.ds(CLASS_BASE[k], CLASS_SIZE[k])]
            pltpu.make_async_copy(held, held, leg1_recv.at[f, k]).wait()

            def body(i, carry):
                dest = at([o - s * c for s, c, o in zip(sign, cls, free_offset(cls, i))])
                pltpu.make_async_remote_copy(src_ref=relay.at[f, CLASS_BASE[k] + i], dst_ref=rows.at[f, source], send_sem=leg2_send.at[f], recv_sem=dir_recv.at[f], device_id=(other, dest), device_id_type=MESH).start()
                return carry
            lax.fori_loop(0, CLASS_SIZE[k], body, 0)

    def build_gates():
        for copy in side:
            copy.wait_recv()
        kg = kg_in[...]
        step = 256
        for b in range(k_rows // step):
            col = (lax.broadcasted_iota(jnp.int32, (seq, step), 1) + b * step).astype(jnp.float32)
            val = jnp.zeros((seq, step), jnp.float32)
            for i in range(8):
                val = jnp.where(kg[:, i:i + 1] == col, kg[:, 8 + i:9 + i], val)
            high = val.astype(jnp.bfloat16)
            rest = val - high.astype(jnp.float32)
            mid = rest.astype(jnp.bfloat16)
            low = (rest - mid.astype(jnp.float32)).astype(jnp.bfloat16)
            for part, piece in enumerate((high, mid, low)):
                g_mat[part * seq:(part + 1) * seq, b * step:(b + 1) * step] = piece

    def combine(f):
        pltpu.make_async_copy(rows.at[f], rows.at[f], dir_recv.at[f]).wait()
        table = rows[f].reshape(k_rows, width)
        sums = jnp.dot(g_mat[...], table, preferred_element_type=jnp.float32)
        mixed = sums[:seq] + (sums[seq:2 * seq] + sums[2 * seq:])
        cols = slice(f * width, (f + 1) * width)
        y_ref[:, cols] = (h_in[:, cols].astype(jnp.float32) + mixed).astype(jnp.bfloat16)

    start_leg1(0)
    start_direct(0)
    start_leg1(1)
    start_direct(1)
    build_gates()
    forward(0)
    for f in range(2, CHUNKS):
        start_leg1(f)
        start_direct(f)
        forward(f - 1)
        combine(f - 2)
    forward(CHUNKS - 1)
    combine(CHUNKS - 2)
    combine(CHUNKS - 1)

    for copy in side:
        copy.wait_send()
    for f in range(CHUNKS):
        pltpu.make_async_copy(rows.at[f, pl.ds(0, DIRECT)], rows.at[f, pl.ds(0, DIRECT)], dir_send.at[f]).wait()
        pltpu.make_async_copy(relay.at[f], relay.at[f], leg1_send.at[f]).wait()
        pltpu.make_async_copy(relay.at[f], relay.at[f], leg2_send.at[f]).wait()


def exchange(o_tab, kg, h):
    n, slots, d = o_tab.shape
    seq = h.shape[0]
    width = d // CHUNKS
    dma = pltpu.SemaphoreType.DMA
    return pl.pallas_call(
        exchange_kernel,
        out_shape=jax.ShapeDtypeStruct((seq, d), jnp.bfloat16),
        in_specs=[pl.BlockSpec(memory_space=pl.ANY), pl.BlockSpec(memory_space=pltpu.VMEM), pl.BlockSpec(memory_space=pltpu.VMEM)],
        out_specs=pl.BlockSpec(memory_space=pltpu.VMEM),
        scratch_shapes=[
            pltpu.VMEM((CHUNKS, n, slots, width), jnp.bfloat16),
            pltpu.VMEM((CHUNKS, RELAYED, slots, width), jnp.bfloat16),
            pltpu.VMEM(kg.shape, jnp.float32),
            pltpu.VMEM((seq, d), jnp.bfloat16),
            pltpu.VMEM((3 * seq, n * slots), jnp.bfloat16),
            dma((2, 2)),
            dma((CHUNKS,)),
            dma((CHUNKS,)),
            dma((CHUNKS,)),
            dma((CHUNKS, len(CLASSES))),
            dma((CHUNKS,)),
        ],
        compiler_params=pltpu.CompilerParams(collective_id=0, has_side_effects=True, vmem_limit_bytes=60 * 1024 * 1024),
        name='exchange',
    )(o_tab, kg, h)


def attention_block(combined, norm_w, w_query, w_key, w_value, w_out):
    y_wide = combined.astype(jnp.float32)
    inv_rms = lax.rsqrt(jnp.mean(y_wide * y_wide, axis=-1, keepdims=True) + NORM_EPS)
    x_in = (y_wide * inv_rms * norm_w).astype(jnp.bfloat16)
    q_heads = jnp.einsum('bld,dhe->blhe', x_in, w_query, preferred_element_type=jnp.float32).astype(jnp.bfloat16)
    k_heads = jnp.einsum('bld,dhe->blhe', x_in, w_key, preferred_element_type=jnp.float32).astype(jnp.bfloat16)
    v_heads = jnp.einsum('bld,dhe->blhe', x_in, w_value, preferred_element_type=jnp.float32).astype(jnp.bfloat16)
    head_dim = w_query.shape[2]
    seq_len = combined.shape[1]
    scores = jnp.einsum('bqhe,bkhe->bhqk', q_heads, k_heads, preferred_element_type=jnp.float32) * (head_dim ** -0.5)
    causal = jnp.arange(seq_len)[:, None] >= jnp.arange(seq_len)[None, :]
    attn_probs = jax.nn.softmax(jnp.where(causal, scores, -jnp.inf), axis=-1).astype(jnp.bfloat16)
    attn_out = jnp.einsum('bhqk,bkhe->bqhe', attn_probs, v_heads, preferred_element_type=jnp.float32).astype(jnp.bfloat16)
    out_proj = jnp.einsum('crif,ife->cre', attn_out, w_out, preferred_element_type=jnp.float32).astype(jnp.bfloat16)
    return (y_wide + out_proj.astype(jnp.float32)).astype(jnp.bfloat16)


def solution(mesh):
    n = mesh.shape['ep']
    tok_spec = P('pp', 'ep', None, None)
    wt_spec = P('pp', None, None, None)

    def device_step(expert_out, expert_ids, slot_ids, gate_vals, residual, norm_w, w_query, w_key, w_value, w_out):
        num_micro, seqs_dev, seq_len, d_model = residual.shape
        slots = expert_out.shape[2] // n
        me = lax.axis_index('ep')
        key = jnp.where(slot_ids >= 0, expert_ids * slots + slot_ids - me * slots, -1)
        kg = jnp.concatenate([key.astype(jnp.float32), gate_vals], axis=-1).reshape(seq_len, -1)
        arrived = exchange(expert_out.reshape(n, slots, d_model), kg, residual.reshape(seq_len, d_model))
        result = attention_block(arrived.reshape(1, seq_len, d_model), norm_w[0], w_query[0], w_key[0], w_value[0], w_out[0])
        return result.reshape(num_micro, seqs_dev, seq_len, d_model)

    return jax.shard_map(device_step, mesh=mesh, in_specs=(tok_spec, tok_spec, tok_spec, tok_spec, tok_spec, P('pp', None), wt_spec, wt_spec, wt_spec, wt_spec), out_specs=tok_spec, check_vma=False)
```

```python
import functools
import itertools

import jax
import jax.numpy as jnp
from jax import lax
from jax.experimental import pallas as pl
from jax.experimental.pallas import tpu as pltpu
from jax.sharding import PartitionSpec as P

NORM_EPS = 1e-6
MESH = pl.DeviceIdType.MESH
SIDE = 4
CHUNKS = 2
CLASSES = [c for c in itertools.product((0, 1), repeat=3) if any(c)]
CLASS_SIZE = [3 ** (3 - sum(c)) for c in CLASSES]
CLASS_BASE = [sum(CLASS_SIZE[:k]) for k in range(len(CLASSES))]
RELAYED = sum(CLASS_SIZE)
DIRECT = 27


def exchange_kernel(o_ref, kg_ref, h_ref, y_ref, rows, relay, kg_in, h_in, g_mat, side_sem, dir_send, dir_recv, leg1_send, leg1_recv, leg2_send):
    stage = lax.axis_index('pp')
    me = lax.axis_index('ep')
    other = 1 - stage
    pos = (me // 16, (me // 4) % 4, me % 4)
    sign = [1 - 2 * (p % 2) for p in pos]
    slots = rows.shape[2]
    width = rows.shape[3]
    seq, k_rows = g_mat.shape[0] // 3, g_mat.shape[1]

    def at(offset):
        z, y, x = [lax.rem(p + d + SIDE, SIDE) for p, d in zip(pos, offset)]
        return z * 16 + y * 4 + x

    def cube(i):
        return ((i + i // 9) % 3 - 1, (i + i // 3) % 3 - 1, i % 3 - 1)

    def free_offset(cls, i):
        out = []
        for c in cls:
            if c:
                out.append(0)
            else:
                out.append(i % 3 - 1)
                i = i // 3
        return out

    barrier = pltpu.get_barrier_semaphore()

    def hello(i, carry):
        pl.semaphore_signal(barrier, inc=1, device_id=(other, at(cube(i))), device_id_type=MESH)
        return carry

    lax.fori_loop(0, DIRECT, hello, 0)
    for cls in CLASSES:
        peer = at([s * c for s, c in zip(sign, cls)])
        pl.semaphore_signal(barrier, inc=1, device_id=(stage, peer), device_id_type=MESH)
    pl.semaphore_wait(barrier, DIRECT + len(CLASSES))

    side = [
        pltpu.make_async_remote_copy(src_ref=src, dst_ref=dst, send_sem=side_sem.at[0, k], recv_sem=side_sem.at[1, k], device_id=(other, me), device_id_type=MESH)
        for k, (src, dst) in enumerate(((kg_ref, kg_in), (h_ref, h_in)))
    ]
    for copy in side:
        copy.start()

    def block(dest, f):
        return o_ref.at[dest, :, pl.ds(f * width, width)]

    def start_direct(f):
        def body(i, carry):
            dest = at(cube(i))
            pltpu.make_async_remote_copy(src_ref=block(dest, f), dst_ref=rows.at[f, me], send_sem=dir_send.at[f], recv_sem=dir_recv.at[f], device_id=(other, dest), device_id_type=MESH).start()
            return carry
        lax.fori_loop(0, DIRECT, body, 0)

    def start_leg1(f):
        for k, cls in enumerate(CLASSES):
            peer = at([s * c for s, c in zip(sign, cls)])

            def body(i, carry):
                dest = at([2 * c + o for c, o in zip(cls, free_offset(cls, i))])
                pltpu.make_async_remote_copy(src_ref=block(dest, f), dst_ref=relay.at[f, CLASS_BASE[k] + i], send_sem=leg1_send.at[f], recv_sem=leg1_recv.at[f, k], device_id=(stage, peer), device_id_type=MESH).start()
                return carry
            lax.fori_loop(0, CLASS_SIZE[k], body, 0)

    def forward(f):
        for k, cls in enumerate(CLASSES):
            source = at([s * c for s, c in zip(sign, cls)])
            held = relay.at[f, pl.ds(CLASS_BASE[k], CLASS_SIZE[k])]
            pltpu.make_async_copy(held, held, leg1_recv.at[f, k]).wait()

            def body(i, carry):
                dest = at([o - s * c for s, c, o in zip(sign, cls, free_offset(cls, i))])
                pltpu.make_async_remote_copy(src_ref=relay.at[f, CLASS_BASE[k] + i], dst_ref=rows.at[f, source], send_sem=leg2_send.at[f], recv_sem=dir_recv.at[f], device_id=(other, dest), device_id_type=MESH).start()
                return carry
            lax.fori_loop(0, CLASS_SIZE[k], body, 0)

    def build_gates():
        for copy in side:
            copy.wait_recv()
        kg = kg_in[...]
        step = 256
        for b in range(k_rows // step):
            col = (lax.broadcasted_iota(jnp.int32, (seq, step), 1) + b * step).astype(jnp.float32)
            val = jnp.zeros((seq, step), jnp.float32)
            for i in range(8):
                val = jnp.where(kg[:, i:i + 1] == col, kg[:, 8 + i:9 + i], val)
            high = val.astype(jnp.bfloat16)
            rest = val - high.astype(jnp.float32)
            mid = rest.astype(jnp.bfloat16)
            low = (rest - mid.astype(jnp.float32)).astype(jnp.bfloat16)
            for part, piece in enumerate((high, mid, low)):
                g_mat[part * seq:(part + 1) * seq, b * step:(b + 1) * step] = piece

    def combine(f):
        pltpu.make_async_copy(rows.at[f], rows.at[f], dir_recv.at[f]).wait()
        table = rows[f].reshape(k_rows, width)
        sums = jnp.dot(g_mat[...], table, preferred_element_type=jnp.float32)
        mixed = sums[:seq] + (sums[seq:2 * seq] + sums[2 * seq:])
        cols = slice(f * width, (f + 1) * width)
        y_ref[:, cols] = (h_in[:, cols].astype(jnp.float32) + mixed).astype(jnp.bfloat16)

    start_leg1(0)
    start_direct(0)
    start_leg1(1)
    start_direct(1)
    build_gates()
    forward(0)
    for f in range(2, CHUNKS):
        start_leg1(f)
        start_direct(f)
        forward(f - 1)
        combine(f - 2)
    forward(CHUNKS - 1)
    combine(CHUNKS - 2)
    combine(CHUNKS - 1)

    for copy in side:
        copy.wait_send()
    for f in range(CHUNKS):
        pltpu.make_async_copy(rows.at[f, pl.ds(0, DIRECT)], rows.at[f, pl.ds(0, DIRECT)], dir_send.at[f]).wait()
        pltpu.make_async_copy(relay.at[f], relay.at[f], leg1_send.at[f]).wait()
        pltpu.make_async_copy(relay.at[f], relay.at[f], leg2_send.at[f]).wait()


def exchange(o_tab, kg, h):
    n, slots, d = o_tab.shape
    seq = h.shape[0]
    width = d // CHUNKS
    dma = pltpu.SemaphoreType.DMA
    return pl.pallas_call(
        exchange_kernel,
        out_shape=jax.ShapeDtypeStruct((seq, d), jnp.bfloat16),
        in_specs=[pl.BlockSpec(memory_space=pl.ANY), pl.BlockSpec(memory_space=pltpu.VMEM), pl.BlockSpec(memory_space=pltpu.VMEM)],
        out_specs=pl.BlockSpec(memory_space=pltpu.VMEM),
        scratch_shapes=[
            pltpu.VMEM((CHUNKS, n, slots, width), jnp.bfloat16),
            pltpu.VMEM((CHUNKS, RELAYED, slots, width), jnp.bfloat16),
            pltpu.VMEM(kg.shape, jnp.float32),
            pltpu.VMEM((seq, d), jnp.bfloat16),
            pltpu.VMEM((3 * seq, n * slots), jnp.bfloat16),
            dma((2, 2)),
            dma((CHUNKS,)),
            dma((CHUNKS,)),
            dma((CHUNKS,)),
            dma((CHUNKS, len(CLASSES))),
            dma((CHUNKS,)),
        ],
        compiler_params=pltpu.CompilerParams(collective_id=0, has_side_effects=True, vmem_limit_bytes=60 * 1024 * 1024),
        name='exchange',
    )(o_tab, kg, h)


def attention_block(combined, norm_w, w_query, w_key, w_value, w_out):
    y_wide = combined.astype(jnp.float32)
    inv_rms = lax.rsqrt(jnp.mean(y_wide * y_wide, axis=-1, keepdims=True) + NORM_EPS)
    x_in = (y_wide * inv_rms * norm_w).astype(jnp.bfloat16)
    q_heads = jnp.einsum('bld,dhe->blhe', x_in, w_query, preferred_element_type=jnp.float32).astype(jnp.bfloat16)
    k_heads = jnp.einsum('bld,dhe->blhe', x_in, w_key, preferred_element_type=jnp.float32).astype(jnp.bfloat16)
    v_heads = jnp.einsum('bld,dhe->blhe', x_in, w_value, preferred_element_type=jnp.float32).astype(jnp.bfloat16)
    head_dim = w_query.shape[2]
    seq_len = combined.shape[1]
    scores = jnp.einsum('bqhe,bkhe->bhqk', q_heads, k_heads, preferred_element_type=jnp.float32) * (head_dim ** -0.5)
    causal = jnp.arange(seq_len)[:, None] >= jnp.arange(seq_len)[None, :]
    attn_probs = jax.nn.softmax(jnp.where(causal, scores, -jnp.inf), axis=-1).astype(jnp.bfloat16)
    attn_out = jnp.einsum('bhqk,bkhe->bqhe', attn_probs, v_heads, preferred_element_type=jnp.float32).astype(jnp.bfloat16)
    out_proj = jnp.einsum('crif,ife->cre', attn_out, w_out, preferred_element_type=jnp.float32).astype(jnp.bfloat16)
    return (y_wide + out_proj.astype(jnp.float32)).astype(jnp.bfloat16)


def solution(mesh):
    n = mesh.shape['ep']
    tok_spec = P('pp', 'ep', None, None)
    wt_spec = P('pp', None, None, None)

    def device_step(expert_out, expert_ids, slot_ids, gate_vals, residual, norm_w, w_query, w_key, w_value, w_out):
        num_micro, seqs_dev, seq_len, d_model = residual.shape
        slots = expert_out.shape[2] // n
        me = lax.axis_index('ep')
        key = jnp.where(slot_ids >= 0, expert_ids * slots + slot_ids - me * slots, -1)
        kg = jnp.concatenate([key.astype(jnp.float32), gate_vals], axis=-1).reshape(seq_len, -1)
        arrived = exchange(expert_out.reshape(n, slots, d_model), kg, residual.reshape(seq_len, d_model))
        result = attention_block(arrived.reshape(1, seq_len, d_model), norm_w[0], w_query[0], w_key[0], w_value[0], w_out[0])
        return result.reshape(num_micro, seqs_dev, seq_len, d_model)

    return jax.shard_map(device_step, mesh=mesh, in_specs=(tok_spec, tok_spec, tok_spec, tok_spec, tok_spec, P('pp', None), wt_spec, wt_spec, wt_spec, wt_spec), out_specs=tok_spec, check_vma=False)
```

```python
import jax
import jax.numpy as jnp
from jax import lax
from jax.experimental import pallas as pl
from jax.experimental.pallas import tpu as pltpu
from jax.sharding import PartitionSpec as P

NORM_EPS = 1e-6
MESH = pl.DeviceIdType.MESH
SIDE = 4
GROUP = 8
COLORS = 3
ORDERS = ((2, 1, 0), (1, 0, 2), (0, 2, 1))
FIRST, SECOND = (0, 3, 1, 2), (0, 3, 1, 2)


def exchange_kernel(o_ref, kg_ref, h_ref, y_ref, rows, held1, held2, tie1, tie2, tie3, kg_in, h_in, g_mat, acc, side_sem, send_sem, recv1, recv2, recv3, recv_rows):
    stage = lax.axis_index('pp')
    me = lax.axis_index('ep')
    other = 1 - stage
    pos = (me // 16, (me // 4) % 4, me % 4)
    sign = [1 - 2 * (p % 2) for p in pos]
    to_a = [lax.rem(p + s + SIDE, SIDE) for p, s in zip(pos, sign)]
    to_b = [lax.rem(p - s + SIDE, SIDE) for p, s in zip(pos, sign)]
    far = [lax.rem(p + 2, SIDE) for p in pos]
    seq = kg_in.shape[0]
    width = 512

    def rank(axis, value):
        z, y, x = [value if k == axis else p for k, p in enumerate(pos)]
        return z * 16 + y * 4 + x

    near_a = [rank(k, to_a[k]) for k in range(3)]
    near_b = [rank(k, to_b[k]) for k in range(3)]

    barrier = pltpu.get_barrier_semaphore()
    peers = [(other, me)]
    for k in range(3):
        for where in (near_a[k], near_b[k]):
            peers += [(stage, where), (other, where)]
    for peer in peers:
        pl.semaphore_signal(barrier, inc=1, device_id=peer, device_id_type=MESH)
    pl.semaphore_wait(barrier, len(peers))

    def send(src, dst, send_s, recv_s, peer):
        pltpu.make_async_remote_copy(src_ref=src, dst_ref=dst, send_sem=send_s, recv_sem=recv_s, device_id=peer, device_id_type=MESH).start()

    def wait(ref, sem):
        pltpu.make_async_copy(ref, ref, sem).wait()

    def table(c, fixed):
        return o_ref.at[tuple(fixed.get(k, slice(None)) for k in range(3)) + (c,)]

    def from_first(c, r1, fixed):
        d1 = ORDERS[c][0]
        if r1 == 0:
            return table(c, {d1: pos[d1], **fixed})
        return held1.at[(c, r1 - 1) + tuple(fixed.get(k, slice(None)) for k in range(3) if k != d1)]

    def phase1():
        for c in range(COLORS):
            d = ORDERS[c][0]
            send(table(c, {d: far[d]}), tie1.at[c], send_sem.at[0, c], recv1.at[c, 0], (stage, near_a[d]))
        for c in range(COLORS):
            d = ORDERS[c][0]
            send(table(c, {d: to_b[d]}), held1.at[c, 2], send_sem.at[0, c], recv1.at[c, 3], (stage, near_b[d]))
        for c in range(COLORS):
            d = ORDERS[c][0]
            send(table(c, {d: to_a[d]}), held1.at[c, 0], send_sem.at[0, c], recv1.at[c, 1], (stage, near_a[d]))

    def forward1():
        for c in range(COLORS):
            d = ORDERS[c][0]
            wait(tie1.at[c], recv1.at[c, 0])
            send(tie1.at[c], held1.at[c, 1], send_sem.at[0, c], recv1.at[c, 2], (stage, near_b[d]))

    def phase2(r1):
        for c in range(COLORS):
            d = ORDERS[c][1]
            if r1:
                wait(held1.at[c, r1 - 1], recv1.at[c, r1])
            send(from_first(c, r1, {d: to_b[d]}), held2.at[c, r1, 2], send_sem.at[1, c], recv2.at[c, r1, 3], (stage, near_b[d]))
            send(from_first(c, r1, {d: far[d]}), tie2.at[c, r1], send_sem.at[1, c], recv2.at[c, r1, 0], (stage, near_a[d]))
            send(from_first(c, r1, {d: to_a[d]}), held2.at[c, r1, 0], send_sem.at[1, c], recv2.at[c, r1, 1], (stage, near_a[d]))

    def forward2(r1):
        for c in range(COLORS):
            d = ORDERS[c][1]
            wait(tie2.at[c, r1], recv2.at[c, r1, 0])
            send(tie2.at[c, r1], held2.at[c, r1, 1], send_sem.at[1, c], recv2.at[c, r1, 2], (stage, near_b[d]))

    def phase3(r1):
        for c in range(COLORS):
            d2, d = ORDERS[c][1:]
            for r2 in (1, 2, 3):
                wait(held2.at[c, r1, r2 - 1], recv2.at[c, r1, r2])

            def piece(near, value):
                if near:
                    return from_first(c, r1, {d2: pos[d2], d: value})
                return held2.at[c, r1, :, value]

            for near in (True, False):
                part = 0 if near else pl.ds(1, 3)
                send(piece(near, far[d]), tie3.at[c, r1, part], send_sem.at[2, c], recv3.at[c, r1], (stage, near_a[d]))
                send(piece(near, to_b[d]), rows.at[r1, c, part, 3], send_sem.at[2, c], recv_rows.at[r1], (other, near_b[d]))
            for near in (True, False):
                part = 0 if near else pl.ds(1, 3)
                send(piece(near, to_a[d]), rows.at[r1, c, part, 1], send_sem.at[2, c], recv_rows.at[r1], (other, near_a[d]))
                send(piece(near, pos[d]), rows.at[r1, c, part, 0], send_sem.at[3, c], recv_rows.at[r1], (other, me))

    def forward3(r1):
        for c in range(COLORS):
            d = ORDERS[c][2]
            wait(tie3.at[c, r1], recv3.at[c, r1])
            send(tie3.at[c, r1], rows.at[r1, c, :, 2], send_sem.at[2, c], recv_rows.at[r1], (other, near_b[d]))

    side = [
        pltpu.make_async_remote_copy(src_ref=src, dst_ref=dst, send_sem=side_sem.at[0, k], recv_sem=side_sem.at[1, k], device_id=(other, me), device_id_type=MESH)
        for k, (src, dst) in enumerate(((kg_ref, kg_in), (h_ref, h_in)))
    ]

    def build_gates():
        for copy in side:
            copy.wait_recv()
        kg = kg_in[...]
        step = 256
        for b in range(g_mat.shape[1] // step):
            col = (lax.broadcasted_iota(jnp.int32, (seq, step), 1) + b * step).astype(jnp.float32)
            val = jnp.zeros((seq, step), jnp.float32)
            for i in range(8):
                val = jnp.where(kg[:, i:i + 1] == col, kg[:, 8 + i:9 + i], val)
            high = val.astype(jnp.bfloat16)
            rest = val - high.astype(jnp.float32)
            mid = rest.astype(jnp.bfloat16)
            low = (rest - mid.astype(jnp.float32)).astype(jnp.bfloat16)
            for part, piece in enumerate((high, mid, low)):
                g_mat[part * seq:(part + 1) * seq, b * step:(b + 1) * step] = piece
        acc[...] = h_in[...].astype(jnp.float32)

    def combine(r1):
        wait(rows.at[r1], recv_rows.at[r1])
        depth = COLORS * 16 * GROUP
        gates = g_mat[:, r1 * depth:(r1 + 1) * depth]
        for b in range(acc.shape[1] // width):
            cols = slice(b * width, (b + 1) * width)
            part = rows[r1, :, :, :, :, cols].reshape(depth, width)
            sums = jnp.dot(gates, part, preferred_element_type=jnp.float32)
            acc[:, cols] += sums[:seq] + (sums[seq:2 * seq] + sums[2 * seq:])

    phase1()
    for copy in side:
        copy.start()
    phase2(0)
    build_gates()
    forward1()
    phase2(3)
    forward2(0)
    phase2(1)
    forward2(3)
    phase2(2)
    phase3(0)
    forward2(1)
    phase3(3)
    forward2(2)
    forward3(0)
    phase3(1)
    forward3(3)
    phase3(2)
    combine(0)
    forward3(1)
    combine(3)
    forward3(2)
    combine(1)
    combine(2)
    y_ref[...] = acc[...].astype(jnp.bfloat16)

    for copy in side:
        copy.wait_send()
    for c in range(COLORS):
        for k in range(3):
            wait(rows.at[:, 0], send_sem.at[k, c])
        wait(rows.at[0, 0], send_sem.at[3, c])


def exchange(o_tab, kg, h):
    seq, d = h.shape
    dma = pltpu.SemaphoreType.DMA
    block = (GROUP, d)

    def buf(*lead):
        return pltpu.VMEM(lead + block, jnp.bfloat16)

    return pl.pallas_call(
        exchange_kernel,
        out_shape=jax.ShapeDtypeStruct((seq, d), jnp.bfloat16),
        in_specs=[pl.BlockSpec(memory_space=pl.ANY), pl.BlockSpec(memory_space=pltpu.VMEM), pl.BlockSpec(memory_space=pltpu.VMEM)],
        out_specs=pl.BlockSpec(memory_space=pltpu.VMEM),
        scratch_shapes=[
            buf(4, COLORS, 4, 4),
            buf(COLORS, 3, 4, 4),
            buf(COLORS, 4, 3, 4),
            buf(COLORS, 4, 4),
            buf(COLORS, 4, 4),
            buf(COLORS, 4, 4),
            pltpu.VMEM(kg.shape, jnp.float32),
            pltpu.VMEM((seq, d), jnp.bfloat16),
            pltpu.VMEM((3 * seq, 64 * COLORS * GROUP), jnp.bfloat16),
            pltpu.VMEM((seq, d), jnp.float32),
            dma((2, 2)),
            dma((4, COLORS)),
            dma((COLORS, 4)),
            dma((COLORS, 4, 4)),
            dma((COLORS, 4)),
            dma((4,)),
        ],
        compiler_params=pltpu.CompilerParams(collective_id=0, has_side_effects=True, vmem_limit_bytes=60 * 1024 * 1024),
        name='exchange',
    )(o_tab, kg, h)


def gate_columns(expert_ids, slot_ids, slots):
    me = lax.axis_index('ep')
    local = slot_ids - me * slots
    colour = local // GROUP
    roles = []
    for shift in (4, 2, 0):
        mine = (me >> shift) & 3
        roles.append(((1 - 2 * (mine & 1)) * (((expert_ids >> shift) & 3) - mine)) & 3)
    first, second, third = [
        jnp.where(colour == 0, roles[ORDERS[0][k]], jnp.where(colour == 1, roles[ORDERS[1][k]], roles[ORDERS[2][k]]))
        for k in range(3)
    ]
    column = (((first * COLORS + colour) * 4 + second) * 4 + third) * GROUP + local % GROUP
    return jnp.where(slot_ids >= 0, column, -1)


def attention_block(combined, norm_w, w_query, w_key, w_value, w_out):
    y_wide = combined.astype(jnp.float32)
    inv_rms = lax.rsqrt(jnp.mean(y_wide * y_wide, axis=-1, keepdims=True) + NORM_EPS)
    x_in = (y_wide * inv_rms * norm_w).astype(jnp.bfloat16)
    q_heads = jnp.einsum('bld,dhe->blhe', x_in, w_query, preferred_element_type=jnp.float32).astype(jnp.bfloat16)
    k_heads = jnp.einsum('bld,dhe->blhe', x_in, w_key, preferred_element_type=jnp.float32).astype(jnp.bfloat16)
    v_heads = jnp.einsum('bld,dhe->blhe', x_in, w_value, preferred_element_type=jnp.float32).astype(jnp.bfloat16)
    head_dim = w_query.shape[2]
    seq_len = combined.shape[1]
    scores = jnp.einsum('bqhe,bkhe->bhqk', q_heads, k_heads, preferred_element_type=jnp.float32) * (head_dim ** -0.5)
    causal = jnp.arange(seq_len)[:, None] >= jnp.arange(seq_len)[None, :]
    attn_probs = jax.nn.softmax(jnp.where(causal, scores, -jnp.inf), axis=-1).astype(jnp.bfloat16)
    attn_out = jnp.einsum('bhqk,bkhe->bqhe', attn_probs, v_heads, preferred_element_type=jnp.float32).astype(jnp.bfloat16)
    out_proj = jnp.einsum('crif,ife->cre', attn_out, w_out, preferred_element_type=jnp.float32).astype(jnp.bfloat16)
    return (y_wide + out_proj.astype(jnp.float32)).astype(jnp.bfloat16)


def solution(mesh):
    n = mesh.shape['ep']
    tok_spec = P('pp', 'ep', None, None)
    wt_spec = P('pp', None, None, None)

    def device_step(expert_out, expert_ids, slot_ids, gate_vals, residual, norm_w, w_query, w_key, w_value, w_out):
        num_micro, seqs_dev, seq_len, d_model = residual.shape
        slots = expert_out.shape[2] // n
        key = gate_columns(expert_ids, slot_ids, slots)
        kg = jnp.concatenate([key.astype(jnp.float32), gate_vals], axis=-1).reshape(seq_len, -1)
        o_tab = expert_out.reshape(SIDE, SIDE, SIDE, COLORS, GROUP, d_model)
        arrived = exchange(o_tab, kg, residual.reshape(seq_len, d_model))
        result = attention_block(arrived.reshape(1, seq_len, d_model), norm_w[0], w_query[0], w_key[0], w_value[0], w_out[0])
        return result.reshape(num_micro, seqs_dev, seq_len, d_model)

    return jax.shard_map(device_step, mesh=mesh, in_specs=(tok_spec, tok_spec, tok_spec, tok_spec, tok_spec, P('pp', None), wt_spec, wt_spec, wt_spec, wt_spec), out_specs=tok_spec, check_vma=False)
```

```python
import jax
import jax.numpy as jnp
from jax import lax
from jax.experimental import pallas as pl
from jax.experimental.pallas import tpu as pltpu
from jax.sharding import PartitionSpec as P

NORM_EPS = 1e-6
MESH = pl.DeviceIdType.MESH
SIDE = 4
GROUP = 8
COLORS = 3
ORDERS = ((2, 1, 0), (1, 0, 2), (0, 2, 1))
FIRST, SECOND = (0, 3, 1, 2), (0, 3, 1, 2)


def stage_kernel(o_ref, ids_ref, slots_ref, gates_ref, h_ref, norm_ref, wq_ref, wk_ref, wv_ref, wo_ref, z_ref, rows, held1, held2, tie1, tie2, tie3, ids_in, slots_in, gates_in, h_in, g_mat, acc, norm_in, flat, wo_in, raw, x_in, a_in, side_sem, local_sem, raw_sem, send_sem, recv1, recv2, recv3, recv_rows):
    stage = lax.axis_index('pp')
    me = lax.axis_index('ep')
    other = 1 - stage
    pos = (me // 16, (me // 4) % 4, me % 4)
    sign = [1 - 2 * (p % 2) for p in pos]
    to_a = [lax.rem(p + s + SIDE, SIDE) for p, s in zip(pos, sign)]
    to_b = [lax.rem(p - s + SIDE, SIDE) for p, s in zip(pos, sign)]
    far = [lax.rem(p + 2, SIDE) for p in pos]
    seq, d_model = h_in.shape
    width = 512
    piece_rows = raw.shape[1]
    pieces = flat.shape[1] // piece_rows

    def rank(axis, value):
        z, y, x = [value if k == axis else p for k, p in enumerate(pos)]
        return z * 16 + y * 4 + x

    near_a = [rank(k, to_a[k]) for k in range(3)]
    near_b = [rank(k, to_b[k]) for k in range(3)]

    barrier = pltpu.get_barrier_semaphore()
    peers = [(other, me)]
    for k in range(3):
        for where in (near_a[k], near_b[k]):
            peers += [(stage, where), (other, where)]
    for peer in peers:
        pl.semaphore_signal(barrier, inc=1, device_id=peer, device_id_type=MESH)
    pl.semaphore_wait(barrier, len(peers))

    def send(src, dst, send_s, recv_s, peer):
        pltpu.make_async_remote_copy(src_ref=src, dst_ref=dst, send_sem=send_s, recv_sem=recv_s, device_id=peer, device_id_type=MESH).start()

    def wait(ref, sem):
        pltpu.make_async_copy(ref, ref, sem).wait()

    def table(c, fixed):
        return o_ref.at[tuple(fixed.get(k, slice(None)) for k in range(3)) + (c,)]

    def from_first(c, r1, fixed):
        d1 = ORDERS[c][0]
        if r1 == 0:
            return table(c, {d1: pos[d1], **fixed})
        return held1.at[(c, r1 - 1) + tuple(fixed.get(k, slice(None)) for k in range(3) if k != d1)]

    def phase1():
        for c in range(COLORS):
            d = ORDERS[c][0]
            send(table(c, {d: far[d]}), tie1.at[c], send_sem.at[0, c], recv1.at[c, 0], (stage, near_a[d]))
        for c in range(COLORS):
            d = ORDERS[c][0]
            send(table(c, {d: to_b[d]}), held1.at[c, 2], send_sem.at[0, c], recv1.at[c, 3], (stage, near_b[d]))
        for c in range(COLORS):
            d = ORDERS[c][0]
            send(table(c, {d: to_a[d]}), held1.at[c, 0], send_sem.at[0, c], recv1.at[c, 1], (stage, near_a[d]))

    def forward1():
        for c in range(COLORS):
            d = ORDERS[c][0]
            wait(tie1.at[c], recv1.at[c, 0])
            send(tie1.at[c], held1.at[c, 1], send_sem.at[0, c], recv1.at[c, 2], (stage, near_b[d]))

    def phase2(r1):
        for c in range(COLORS):
            d = ORDERS[c][1]
            if r1:
                wait(held1.at[c, r1 - 1], recv1.at[c, r1])
            send(from_first(c, r1, {d: to_b[d]}), held2.at[c, r1, 2], send_sem.at[1, c], recv2.at[c, r1, 3], (stage, near_b[d]))
            send(from_first(c, r1, {d: far[d]}), tie2.at[c, r1], send_sem.at[1, c], recv2.at[c, r1, 0], (stage, near_a[d]))
            send(from_first(c, r1, {d: to_a[d]}), held2.at[c, r1, 0], send_sem.at[1, c], recv2.at[c, r1, 1], (stage, near_a[d]))

    def forward2(r1):
        for c in range(COLORS):
            d = ORDERS[c][1]
            wait(tie2.at[c, r1], recv2.at[c, r1, 0])
            send(tie2.at[c, r1], held2.at[c, r1, 1], send_sem.at[1, c], recv2.at[c, r1, 2], (stage, near_b[d]))

    def phase3(r1):
        for c in range(COLORS):
            d2, d = ORDERS[c][1:]
            for r2 in (1, 2, 3):
                wait(held2.at[c, r1, r2 - 1], recv2.at[c, r1, r2])

            def piece(near, value):
                if near:
                    return from_first(c, r1, {d2: pos[d2], d: value})
                return held2.at[c, r1, :, value]

            for near in (True, False):
                part = 0 if near else pl.ds(1, 3)
                send(piece(near, far[d]), tie3.at[c, r1, part], send_sem.at[2, c], recv3.at[c, r1], (stage, near_a[d]))
                send(piece(near, to_b[d]), rows.at[r1, c, part, 3], send_sem.at[2, c], recv_rows.at[r1], (other, near_b[d]))
            for near in (True, False):
                part = 0 if near else pl.ds(1, 3)
                send(piece(near, to_a[d]), rows.at[r1, c, part, 1], send_sem.at[2, c], recv_rows.at[r1], (other, near_a[d]))
                send(piece(near, pos[d]), rows.at[r1, c, part, 0], send_sem.at[3, c], recv_rows.at[r1], (other, me))

    def forward3(r1):
        for c in range(COLORS):
            d = ORDERS[c][2]
            wait(tie3.at[c, r1], recv3.at[c, r1])
            send(tie3.at[c, r1], rows.at[r1, c, :, 2], send_sem.at[2, c], recv_rows.at[r1], (other, near_b[d]))

    side = [
        pltpu.make_async_remote_copy(src_ref=src, dst_ref=dst, send_sem=side_sem.at[0, k], recv_sem=side_sem.at[1, k], device_id=(other, me), device_id_type=MESH)
        for k, (src, dst) in enumerate(((ids_ref, ids_in), (slots_ref, slots_in), (gates_ref, gates_in), (h_ref, h_in)))
    ]
    local = [pltpu.make_async_copy(src, dst, local_sem.at[k]) for k, (src, dst) in enumerate(((norm_ref, norm_in), (wo_ref, wo_in)))]

    def load(i):
        src = (wq_ref, wk_ref, wv_ref)[i // pieces]
        return pltpu.make_async_copy(src.at[pl.ds(i % pieces * piece_rows, piece_rows)], raw.at[i % 2], raw_sem.at[i % 2])

    def flatten(i):
        load(i).wait()
        step = 64

        def body(j, carry):
            at = pl.multiple_of(j * step, step)
            flat[i // pieces, pl.ds(pl.multiple_of(i % pieces * piece_rows + at, step), step), :] = raw[i % 2, pl.ds(at, step)].reshape(step, d_model)
            return carry

        lax.fori_loop(0, piece_rows // step, body, 0)
        if i + 2 < 3 * pieces:
            load(i + 2).start()

    def build_gates():
        for copy in side:
            copy.wait_recv()
        ids, slot = ids_in[...], slots_in[...]
        spot = slot - me * (COLORS * GROUP)
        colour = spot >> 3
        roles = []
        for k, shift in enumerate((4, 2, 0)):
            roles.append((sign[k] * (((ids >> shift) & 3) - pos[k])) & 3)
        first, second, third = [
            jnp.where(colour == 0, roles[ORDERS[0][k]], jnp.where(colour == 1, roles[ORDERS[1][k]], roles[ORDERS[2][k]]))
            for k in range(3)
        ]
        column = (((first * COLORS + colour) * 4 + second) * 4 + third) * GROUP + (spot & 7)
        column = jnp.where(slot >= 0, column, -1).astype(jnp.float32)
        both = jnp.concatenate([column, gates_in[...], jnp.zeros((112, seq), jnp.float32)], axis=0).T
        step = 256
        for b in range(g_mat.shape[1] // step):
            col = (lax.broadcasted_iota(jnp.int32, (seq, step), 1) + b * step).astype(jnp.float32)
            val = jnp.zeros((seq, step), jnp.float32)
            for i in range(8):
                val = jnp.where(both[:, i:i + 1] == col, both[:, 8 + i:9 + i], val)
            high = val.astype(jnp.bfloat16)
            rest = val - high.astype(jnp.float32)
            mid = rest.astype(jnp.bfloat16)
            low = (rest - mid.astype(jnp.float32)).astype(jnp.bfloat16)
            for part, piece in enumerate((high, mid, low)):
                g_mat[part * seq:(part + 1) * seq, b * step:(b + 1) * step] = piece
        acc[...] = h_in[...].astype(jnp.float32)

    def combine(r1):
        wait(rows.at[r1], recv_rows.at[r1])
        depth = COLORS * 16 * GROUP
        gates = g_mat[:, r1 * depth:(r1 + 1) * depth]
        for b in range(acc.shape[1] // width):
            cols = slice(b * width, (b + 1) * width)
            part = rows[r1, :, :, :, :, cols].reshape(depth, width)
            sums = jnp.dot(gates, part, preferred_element_type=jnp.float32)
            acc[:, cols] += sums[:seq] + (sums[seq:2 * seq] + sums[2 * seq:])

    def norm():
        total = jnp.zeros((seq, 1), jnp.float32)
        for b in range(d_model // width):
            cols = slice(b * width, (b + 1) * width)
            y = acc[:, cols].astype(jnp.bfloat16).astype(jnp.float32)
            acc[:, cols] = y
            total += jnp.sum(y * y, axis=1, keepdims=True)
        inv = lax.rsqrt(total * (1.0 / d_model) + NORM_EPS)
        for b in range(d_model // width):
            cols = slice(b * width, (b + 1) * width)
            x_in[:, cols] = (acc[:, cols] * inv * norm_in[:, cols]).astype(jnp.bfloat16)

    head = 128
    pair = 2 * head

    def project(p):
        cols = slice(p * pair, (p + 1) * pair)
        return [jnp.dot(x_in[...], flat[k, :, cols], preferred_element_type=jnp.float32).astype(jnp.bfloat16) for k in range(3)]

    causal = lax.broadcasted_iota(jnp.int32, (seq, seq), 0) >= lax.broadcasted_iota(jnp.int32, (seq, seq), 1)

    def attend(p, qkv):
        for u in range(2):
            q, k, v = [t[:, u * head:(u + 1) * head] for t in qkv]
            scores = lax.dot_general(q, k, (((1,), (1,)), ((), ())), preferred_element_type=jnp.float32) * (head ** -0.5)
            scores = jnp.where(causal, scores, -jnp.inf)
            grown = jnp.exp(scores - jnp.max(scores, axis=1, keepdims=True))
            probs = (grown * (1.0 / jnp.sum(grown, axis=1, keepdims=True))).astype(jnp.bfloat16)
            mixed = jnp.dot(probs, v, preferred_element_type=jnp.float32).astype(jnp.bfloat16)
            at = p * pair + u * head
            a_in[:, at:at + head] = mixed

    phase1()
    for copy in side:
        copy.start()
    phase2(0)
    load(0).start()
    load(1).start()
    for copy in local:
        copy.start()
    build_gates()
    for i in range(12):
        flatten(i)
    forward1()
    phase2(3)
    for i in range(12, 16):
        flatten(i)
    forward2(0)
    phase2(1)
    for i in range(16, 20):
        flatten(i)
    forward2(3)
    phase2(2)
    phase3(0)
    for i in range(20, 24):
        flatten(i)
    forward2(1)
    phase3(3)
    forward2(2)
    forward3(0)
    phase3(1)
    forward3(3)
    phase3(2)
    combine(0)
    forward3(1)
    combine(3)
    forward3(2)
    combine(1)
    for copy in local:
        copy.wait()
    combine(2)
    norm()
    pairs = d_model // pair
    ready = project(0)
    for p in range(pairs):
        later = project(p + 1) if p + 1 < pairs else None
        attend(p, ready)
        ready = later
    for b in range(d_model // pair):
        cols = slice(b * pair, (b + 1) * pair)
        out = jnp.dot(a_in[...], wo_in[:, cols], preferred_element_type=jnp.float32).astype(jnp.bfloat16)
        z_ref[:, cols] = (acc[:, cols] + out.astype(jnp.float32)).astype(jnp.bfloat16)

    for copy in side:
        copy.wait_send()
    for c in range(COLORS):
        for k in range(3):
            wait(rows.at[:, 0], send_sem.at[k, c])
        wait(rows.at[0, 0], send_sem.at[3, c])


def run_stage(o_tab, ids, slots, gates, h, norm_w, wq, wk, wv, wo):
    seq, d = h.shape
    dma = pltpu.SemaphoreType.DMA
    block = (GROUP, d)
    piece = 256

    def buf(*lead):
        return pltpu.VMEM(lead + block, jnp.bfloat16)

    return pl.pallas_call(
        stage_kernel,
        out_shape=jax.ShapeDtypeStruct((seq, d), jnp.bfloat16),
        in_specs=[pl.BlockSpec(memory_space=pl.ANY)] * 10,
        out_specs=pl.BlockSpec(memory_space=pltpu.VMEM),
        scratch_shapes=[
            buf(4, COLORS, 4, 4),
            buf(COLORS, 3, 4, 4),
            buf(COLORS, 4, 3, 4),
            buf(COLORS, 4, 4),
            buf(COLORS, 4, 4),
            buf(COLORS, 4, 4),
            pltpu.VMEM(ids.shape, jnp.int32),
            pltpu.VMEM(slots.shape, jnp.int32),
            pltpu.VMEM(gates.shape, jnp.float32),
            pltpu.VMEM((seq, d), jnp.bfloat16),
            pltpu.VMEM((3 * seq, 64 * COLORS * GROUP), jnp.bfloat16),
            pltpu.VMEM((seq, d), jnp.float32),
            pltpu.VMEM(norm_w.shape, jnp.float32),
            pltpu.VMEM((3, d, d), jnp.bfloat16),
            pltpu.VMEM((d, d), jnp.bfloat16),
            pltpu.VMEM((2, piece) + wq.shape[1:], jnp.bfloat16),
            pltpu.VMEM((seq, d), jnp.bfloat16),
            pltpu.VMEM((seq, d), jnp.bfloat16),
            dma((2, 4)),
            dma((2,)),
            dma((2,)),
            dma((4, COLORS)),
            dma((COLORS, 4)),
            dma((COLORS, 4, 4)),
            dma((COLORS, 4)),
            dma((4,)),
        ],
        compiler_params=pltpu.CompilerParams(collective_id=0, has_side_effects=True, vmem_limit_bytes=67043328),
        name='stage',
    )(o_tab, ids, slots, gates, h, norm_w, wq, wk, wv, wo)


def solution(mesh):
    tok_spec = P('pp', 'ep', None, None)
    wt_spec = P('pp', None, None, None)

    def device_step(expert_out, expert_ids, slot_ids, gate_vals, residual, norm_w, w_query, w_key, w_value, w_out):
        seq_len, d_model = residual.shape[2:]

        def choices(array):
            return array.reshape(seq_len, array.shape[3]).T

        result = run_stage(
            expert_out.reshape(SIDE, SIDE, SIDE, COLORS, GROUP, d_model),
            choices(expert_ids), choices(slot_ids), choices(gate_vals),
            residual.reshape(seq_len, d_model), norm_w, w_query[0], w_key[0], w_value[0], w_out[0].reshape(-1, d_model),
        )
        return result.reshape(residual.shape)

    return jax.shard_map(device_step, mesh=mesh, in_specs=(tok_spec, tok_spec, tok_spec, tok_spec, tok_spec, P('pp', None), wt_spec, wt_spec, wt_spec, wt_spec), out_specs=tok_spec, check_vma=False)
```

```python
import jax
import jax.numpy as jnp
from jax import lax
from jax.experimental import pallas as pl
from jax.experimental.pallas import tpu as pltpu
from jax.sharding import PartitionSpec as P

NORM_EPS = 1e-6
MESH = pl.DeviceIdType.MESH
SIDE = 4
GROUP = 8
COLORS = 3
ORDERS = ((2, 1, 0), (1, 0, 2), (0, 2, 1))
FIRST, SECOND = (0, 3, 1, 2), (0, 3, 1, 2)


def stage_kernel(o_ref, ids_ref, slots_ref, gates_ref, h_ref, norm_ref, wq_ref, wk_ref, wv_ref, wo_ref, z_ref, rows, held1, held2, tie1, tie2, tie3, ids_in, slots_in, gates_in, h_in, g_mat, acc, norm_in, flat, wo_in, raw, x_in, qkv, score, prob, side_sem, local_sem, raw_sem, send_sem, recv1, recv2, recv3, recv_rows):
    stage = lax.axis_index('pp')
    me = lax.axis_index('ep')
    other = 1 - stage
    pos = (me // 16, (me // 4) % 4, me % 4)
    sign = [1 - 2 * (p % 2) for p in pos]
    to_a = [lax.rem(p + s + SIDE, SIDE) for p, s in zip(pos, sign)]
    to_b = [lax.rem(p - s + SIDE, SIDE) for p, s in zip(pos, sign)]
    far = [lax.rem(p + 2, SIDE) for p in pos]
    seq, d_model = h_in.shape
    width = 512
    piece_rows = raw.shape[1]
    pieces = flat.shape[1] // piece_rows

    def rank(axis, value):
        z, y, x = [value if k == axis else p for k, p in enumerate(pos)]
        return z * 16 + y * 4 + x

    near_a = [rank(k, to_a[k]) for k in range(3)]
    near_b = [rank(k, to_b[k]) for k in range(3)]

    barrier = pltpu.get_barrier_semaphore()
    peers = [(other, me)]
    for k in range(3):
        for where in (near_a[k], near_b[k]):
            peers += [(stage, where), (other, where)]
    for peer in peers:
        pl.semaphore_signal(barrier, inc=1, device_id=peer, device_id_type=MESH)
    pl.semaphore_wait(barrier, len(peers))

    def send(src, dst, send_s, recv_s, peer):
        pltpu.make_async_remote_copy(src_ref=src, dst_ref=dst, send_sem=send_s, recv_sem=recv_s, device_id=peer, device_id_type=MESH).start()

    def wait(ref, sem):
        pltpu.make_async_copy(ref, ref, sem).wait()

    def table(c, fixed):
        return o_ref.at[tuple(fixed.get(k, slice(None)) for k in range(3)) + (c,)]

    def from_first(c, r1, fixed):
        d1 = ORDERS[c][0]
        if r1 == 0:
            return table(c, {d1: pos[d1], **fixed})
        return held1.at[(c, r1 - 1) + tuple(fixed.get(k, slice(None)) for k in range(3) if k != d1)]

    def phase1():
        for c in range(COLORS):
            d = ORDERS[c][0]
            send(table(c, {d: far[d]}), tie1.at[c], send_sem.at[0, c], recv1.at[c, 0], (stage, near_a[d]))
        for c in range(COLORS):
            d = ORDERS[c][0]
            send(table(c, {d: to_b[d]}), held1.at[c, 2], send_sem.at[0, c], recv1.at[c, 3], (stage, near_b[d]))
        for c in range(COLORS):
            d = ORDERS[c][0]
            send(table(c, {d: to_a[d]}), held1.at[c, 0], send_sem.at[0, c], recv1.at[c, 1], (stage, near_a[d]))

    def forward1():
        for c in range(COLORS):
            d = ORDERS[c][0]
            wait(tie1.at[c], recv1.at[c, 0])
            send(tie1.at[c], held1.at[c, 1], send_sem.at[0, c], recv1.at[c, 2], (stage, near_b[d]))

    def phase2(r1):
        for c in range(COLORS):
            d = ORDERS[c][1]
            if r1:
                wait(held1.at[c, r1 - 1], recv1.at[c, r1])
            send(from_first(c, r1, {d: to_b[d]}), held2.at[c, r1, 2], send_sem.at[1, c], recv2.at[c, r1, 3], (stage, near_b[d]))
            send(from_first(c, r1, {d: far[d]}), tie2.at[c, r1], send_sem.at[1, c], recv2.at[c, r1, 0], (stage, near_a[d]))
            send(from_first(c, r1, {d: to_a[d]}), held2.at[c, r1, 0], send_sem.at[1, c], recv2.at[c, r1, 1], (stage, near_a[d]))

    def forward2(r1):
        for c in range(COLORS):
            d = ORDERS[c][1]
            wait(tie2.at[c, r1], recv2.at[c, r1, 0])
            send(tie2.at[c, r1], held2.at[c, r1, 1], send_sem.at[1, c], recv2.at[c, r1, 2], (stage, near_b[d]))

    def last(c, r1, value):
        d2, d = ORDERS[c][1:]
        return (0, from_first(c, r1, {d2: pos[d2], d: value})), (pl.ds(1, 3), held2.at[c, r1, :, value])

    def ties3(r1):
        for c in range(COLORS):
            d = ORDERS[c][2]
            for r2 in (1, 2, 3):
                wait(held2.at[c, r1, r2 - 1], recv2.at[c, r1, r2])
            for part, piece in last(c, r1, far[d]):
                send(piece, tie3.at[c, r1, part], send_sem.at[2, c], recv3.at[c, r1], (stage, near_a[d]))

    def to_b3(r1):
        for c in range(COLORS):
            d = ORDERS[c][2]
            for part, piece in last(c, r1, to_b[d]):
                send(piece, rows.at[r1, c, part, 3], send_sem.at[2, c], recv_rows.at[r1], (other, near_b[d]))

    def to_a3(r1):
        for c in range(COLORS):
            d = ORDERS[c][2]
            for part, piece in last(c, r1, to_a[d]):
                send(piece, rows.at[r1, c, part, 1], send_sem.at[2, c], recv_rows.at[r1], (other, near_a[d]))
            for part, piece in last(c, r1, pos[d]):
                send(piece, rows.at[r1, c, part, 0], send_sem.at[3, c], recv_rows.at[r1], (other, me))

    def forward3(r1):
        for c in range(COLORS):
            d = ORDERS[c][2]
            wait(tie3.at[c, r1], recv3.at[c, r1])
            send(tie3.at[c, r1], rows.at[r1, c, :, 2], send_sem.at[2, c], recv_rows.at[r1], (other, near_b[d]))

    side = [
        pltpu.make_async_remote_copy(src_ref=src, dst_ref=dst, send_sem=side_sem.at[0, k], recv_sem=side_sem.at[1, k], device_id=(other, me), device_id_type=MESH)
        for k, (src, dst) in enumerate(((ids_ref, ids_in), (slots_ref, slots_in), (gates_ref, gates_in), (h_ref, h_in)))
    ]
    local = [pltpu.make_async_copy(src, dst, local_sem.at[k]) for k, (src, dst) in enumerate(((norm_ref, norm_in), (wo_ref, wo_in)))]

    def load(i):
        src = (wq_ref, wk_ref, wv_ref)[i // pieces]
        return pltpu.make_async_copy(src.at[pl.ds(i % pieces * piece_rows, piece_rows)], raw.at[i % 2], raw_sem.at[i % 2])

    def flatten(i):
        load(i).wait()
        step = 64

        def body(j, carry):
            at = pl.multiple_of(j * step, step)
            flat[i // pieces, pl.ds(pl.multiple_of(i % pieces * piece_rows + at, step), step), :] = raw[i % 2, pl.ds(at, step)].reshape(step, d_model)
            return carry

        lax.fori_loop(0, piece_rows // step, body, 0)
        if i + 2 < 3 * pieces:
            load(i + 2).start()

    def build_gates():
        for copy in side:
            copy.wait_recv()
        ids, slot = ids_in[...], slots_in[...]
        spot = slot - me * (COLORS * GROUP)
        colour = spot >> 3
        roles = []
        for k, shift in enumerate((4, 2, 0)):
            roles.append((sign[k] * (((ids >> shift) & 3) - pos[k])) & 3)
        first, second, third = [
            jnp.where(colour == 0, roles[ORDERS[0][k]], jnp.where(colour == 1, roles[ORDERS[1][k]], roles[ORDERS[2][k]]))
            for k in range(3)
        ]
        column = (((first * COLORS + colour) * 4 + second) * 4 + third) * GROUP + (spot & 7)
        column = jnp.where(slot >= 0, column, -1).astype(jnp.float32)
        both = jnp.concatenate([column, gates_in[...], jnp.zeros((112, seq), jnp.float32)], axis=0).T
        step = 256
        for b in range(g_mat.shape[1] // step):
            col = (lax.broadcasted_iota(jnp.int32, (seq, step), 1) + b * step).astype(jnp.float32)
            val = jnp.zeros((seq, step), jnp.float32)
            for i in range(8):
                val = jnp.where(both[:, i:i + 1] == col, both[:, 8 + i:9 + i], val)
            high = val.astype(jnp.bfloat16)
            rest = val - high.astype(jnp.float32)
            mid = rest.astype(jnp.bfloat16)
            low = (rest - mid.astype(jnp.float32)).astype(jnp.bfloat16)
            for part, piece in enumerate((high, mid, low)):
                g_mat[part * seq:(part + 1) * seq, b * step:(b + 1) * step] = piece
        acc[...] = h_in[...].astype(jnp.float32)

    def combine(r1):
        wait(rows.at[r1], recv_rows.at[r1])
        depth = COLORS * 16 * GROUP
        gates = g_mat[:, r1 * depth:(r1 + 1) * depth]
        for b in range(acc.shape[1] // width):
            cols = slice(b * width, (b + 1) * width)
            part = rows[r1, :, :, :, :, cols].reshape(depth, width)
            sums = jnp.dot(gates, part, preferred_element_type=jnp.float32)
            acc[:, cols] += sums[:seq] + (sums[seq:2 * seq] + sums[2 * seq:])

    def norm():
        total = jnp.zeros((seq, 1), jnp.float32)
        for b in range(d_model // width):
            cols = slice(b * width, (b + 1) * width)
            y = acc[:, cols].astype(jnp.bfloat16).astype(jnp.float32)
            acc[:, cols] = y
            total += jnp.sum(y * y, axis=1, keepdims=True)
        inv = lax.rsqrt(total * (1.0 / d_model) + NORM_EPS)
        for b in range(d_model // width):
            cols = slice(b * width, (b + 1) * width)
            x_in[:, cols] = (acc[:, cols] * inv * norm_in[:, cols]).astype(jnp.bfloat16)

    head = 128
    pair = 2 * head
    causal = lax.broadcasted_iota(jnp.int32, (seq, seq), 0) >= lax.broadcasted_iota(jnp.int32, (seq, seq), 1)

    def project(k, p):
        cols = slice(p * pair, (p + 1) * pair)
        qkv[k, :, cols] = jnp.dot(x_in[...], flat[k, :, cols], preferred_element_type=jnp.float32).astype(jnp.bfloat16)

    def softmax(h):
        scores = jnp.where(causal, score[h] * (head ** -0.5), -jnp.inf)
        grown = jnp.exp(scores - jnp.max(scores, axis=1, keepdims=True))
        prob[h] = (grown * (1.0 / jnp.sum(grown, axis=1, keepdims=True))).astype(jnp.bfloat16)

    def attend():
        heads = d_model // head
        for k in range(2):
            for p in range(d_model // pair):
                project(k, p)
        for h in range(heads):
            q, k = [qkv[t, :, h * head:(h + 1) * head] for t in range(2)]
            score[h] = lax.dot_general(q, k, (((1,), (1,)), ((), ())), preferred_element_type=jnp.float32)
        for p in range(d_model // pair):
            softmax(2 * p)
            softmax(2 * p + 1)
            project(2, p)
        for h in range(heads):
            cols = slice(h * head, (h + 1) * head)
            x_in[:, cols] = jnp.dot(prob[h], qkv[2, :, cols], preferred_element_type=jnp.float32).astype(jnp.bfloat16)

    phase1()
    for copy in side:
        copy.start()
    phase2(0)
    load(0).start()
    load(1).start()
    for copy in local:
        copy.start()
    build_gates()
    for i in range(12):
        flatten(i)
    forward1()
    phase2(3)
    for i in range(12, 16):
        flatten(i)
    forward2(0)
    phase2(1)
    for i in range(16, 20):
        flatten(i)
    forward2(3)
    phase2(2)
    ties3(0)
    to_b3(0)
    to_a3(0)
    for i in range(20, 24):
        flatten(i)
    forward2(1)
    ties3(3)
    to_b3(3)
    forward2(2)
    forward3(0)
    to_a3(3)
    ties3(1)
    to_b3(1)
    forward3(3)
    ties3(2)
    to_b3(2)
    to_a3(1)
    combine(0)
    forward3(1)
    to_a3(2)
    combine(3)
    for copy in local:
        copy.wait()
    forward3(2)
    combine(1)
    combine(2)
    norm()
    attend()
    for b in range(d_model // pair):
        cols = slice(b * pair, (b + 1) * pair)
        out = jnp.dot(x_in[...], wo_in[:, cols], preferred_element_type=jnp.float32).astype(jnp.bfloat16)
        z_ref[:, cols] = (acc[:, cols] + out.astype(jnp.float32)).astype(jnp.bfloat16)

    for copy in side:
        copy.wait_send()
    for c in range(COLORS):
        for k in range(3):
            wait(rows.at[:, 0], send_sem.at[k, c])
        wait(rows.at[0, 0], send_sem.at[3, c])


def run_stage(o_tab, ids, slots, gates, h, norm_w, wq, wk, wv, wo):
    seq, d = h.shape
    dma = pltpu.SemaphoreType.DMA
    block = (GROUP, d)
    piece = 256

    def buf(*lead):
        return pltpu.VMEM(lead + block, jnp.bfloat16)

    return pl.pallas_call(
        stage_kernel,
        out_shape=pltpu.VMEM((seq, d), jnp.bfloat16),
        in_specs=[pl.BlockSpec(memory_space=pl.ANY)] * 10,
        out_specs=pl.BlockSpec(memory_space=pltpu.VMEM),
        scratch_shapes=[
            buf(4, COLORS, 4, 4),
            buf(COLORS, 3, 4, 4),
            buf(COLORS, 4, 3, 4),
            buf(COLORS, 4, 4),
            buf(COLORS, 4, 4),
            buf(COLORS, 4, 4),
            pltpu.VMEM(ids.shape, jnp.int32),
            pltpu.VMEM(slots.shape, jnp.int32),
            pltpu.VMEM(gates.shape, jnp.float32),
            pltpu.VMEM((seq, d), jnp.bfloat16),
            pltpu.VMEM((3 * seq, 64 * COLORS * GROUP), jnp.bfloat16),
            pltpu.VMEM((seq, d), jnp.float32),
            pltpu.VMEM(norm_w.shape, jnp.float32),
            pltpu.VMEM((3, d, d), jnp.bfloat16),
            pltpu.VMEM((d, d), jnp.bfloat16),
            pltpu.VMEM((2, piece) + wq.shape[1:], jnp.bfloat16),
            pltpu.VMEM((seq, d), jnp.bfloat16),
            pltpu.VMEM((3, seq, d), jnp.bfloat16),
            pltpu.VMEM((wq.shape[1], seq, seq), jnp.float32),
            pltpu.VMEM((wq.shape[1], seq, seq), jnp.bfloat16),
            dma((2, 4)),
            dma((2,)),
            dma((2,)),
            dma((4, COLORS)),
            dma((COLORS, 4)),
            dma((COLORS, 4, 4)),
            dma((COLORS, 4)),
            dma((4,)),
        ],
        compiler_params=pltpu.CompilerParams(collective_id=0, has_side_effects=True, vmem_limit_bytes=62 * 1024 * 1024),
        name='stage',
    )(o_tab, ids, slots, gates, h, norm_w, wq, wk, wv, wo)


def solution(mesh):
    tok_spec = P('pp', 'ep', None, None)
    wt_spec = P('pp', None, None, None)

    def device_step(expert_out, expert_ids, slot_ids, gate_vals, residual, norm_w, w_query, w_key, w_value, w_out):
        seq_len, d_model = residual.shape[2:]

        def choices(array):
            return array.reshape(seq_len, array.shape[3]).T

        result = run_stage(
            expert_out.reshape(SIDE, SIDE, SIDE, COLORS, GROUP, d_model),
            choices(expert_ids), choices(slot_ids), choices(gate_vals),
            residual.reshape(seq_len, d_model), norm_w, w_query[0], w_key[0], w_value[0], w_out[0].reshape(-1, d_model),
        )
        return result.reshape(residual.shape)

    return jax.shard_map(device_step, mesh=mesh, in_specs=(tok_spec, tok_spec, tok_spec, tok_spec, tok_spec, P('pp', None), wt_spec, wt_spec, wt_spec, wt_spec), out_specs=tok_spec, check_vma=False)
```

```python
import jax
import jax.numpy as jnp
from jax import lax
from jax.experimental import pallas as pl
from jax.experimental.pallas import tpu as pltpu
from jax.sharding import PartitionSpec as P

NORM_EPS = 1e-6
MESH = pl.DeviceIdType.MESH
SIDE = 4
GROUP = 8
COLORS = 3
ORDERS = ((2, 1, 0), (1, 0, 2), (0, 2, 1))
WIDE, NARROW = 1536, 512


def stage_kernel(o_ref, ids_ref, slots_ref, gates_ref, h_ref, norm_ref, wq_ref, wk_ref, wv_ref, wo_ref, z_ref, wide, narrow, held1, held2, tie1, tie2, tie3, ids_in, slots_in, gates_in, g_wide, g_narrow, acc, norm_in, flat, wo_in, raw, x_in, part, qkv, side_sem, local_sem, raw_sem, send_sem, recv1, recv2, recv3_wide, recv3_narrow, recv_wide, recv_narrow):
    stage = lax.axis_index('pp')
    me = lax.axis_index('ep')
    other = 1 - stage
    pos = (me // 16, (me // 4) % 4, me % 4)
    sign = [1 - 2 * (p % 2) for p in pos]
    to_a = [lax.rem(p + s + SIDE, SIDE) for p, s in zip(pos, sign)]
    to_b = [lax.rem(p - s + SIDE, SIDE) for p, s in zip(pos, sign)]
    far = [lax.rem(p + 2, SIDE) for p in pos]
    seq, d_model = x_in.shape
    width = 512
    depth, piece_rows = raw.shape[:2]
    pieces = flat.shape[1] // piece_rows

    def rank(axis, value):
        z, y, x = [value if k == axis else p for k, p in enumerate(pos)]
        return z * 16 + y * 4 + x

    near_a = [rank(k, to_a[k]) for k in range(3)]
    near_b = [rank(k, to_b[k]) for k in range(3)]

    barrier = pltpu.get_barrier_semaphore()
    peers = [(other, me)]
    for k in range(3):
        for where in (near_a[k], near_b[k]):
            peers += [(stage, where), (other, where)]
    for peer in peers:
        pl.semaphore_signal(barrier, inc=1, device_id=peer, device_id_type=MESH)
    pl.semaphore_wait(barrier, len(peers))

    def send(src, dst, send_s, recv_s, peer):
        pltpu.make_async_remote_copy(src_ref=src, dst_ref=dst, send_sem=send_s, recv_sem=recv_s, device_id=peer, device_id_type=MESH).start()

    def wait(ref, sem):
        pltpu.make_async_copy(ref, ref, sem).wait()

    def table(c, fixed):
        return o_ref.at[tuple(fixed.get(k, slice(None)) for k in range(3)) + (c,)]

    def from_first(c, r1, fixed):
        d1 = ORDERS[c][0]
        if r1 == 0:
            return table(c, {d1: pos[d1], **fixed})
        return held1.at[(c, r1 - 1) + tuple(fixed.get(k, slice(None)) for k in range(3) if k != d1)]

    def phase1():
        for c in range(COLORS):
            d = ORDERS[c][0]
            send(table(c, {d: far[d]}), tie1.at[c], send_sem.at[0, c], recv1.at[c, 0], (stage, near_a[d]))
        for c in range(COLORS):
            d = ORDERS[c][0]
            send(table(c, {d: to_b[d]}), held1.at[c, 2], send_sem.at[0, c], recv1.at[c, 3], (stage, near_b[d]))
        for c in range(COLORS):
            d = ORDERS[c][0]
            send(table(c, {d: to_a[d]}), held1.at[c, 0], send_sem.at[0, c], recv1.at[c, 1], (stage, near_a[d]))

    def forward1():
        for c in range(COLORS):
            d = ORDERS[c][0]
            wait(tie1.at[c], recv1.at[c, 0])
            send(tie1.at[c], held1.at[c, 1], send_sem.at[3, c], recv1.at[c, 2], (stage, near_b[d]))

    def phase2(r1):
        for c in range(COLORS):
            d = ORDERS[c][1]
            if r1:
                wait(held1.at[c, r1 - 1], recv1.at[c, r1])
            send(from_first(c, r1, {d: to_b[d]}), held2.at[c, r1, 2], send_sem.at[1, c], recv2.at[c, r1, 3], (stage, near_b[d]))
            send(from_first(c, r1, {d: far[d]}), tie2.at[c, r1], send_sem.at[1, c], recv2.at[c, r1, 0], (stage, near_a[d]))
            send(from_first(c, r1, {d: to_a[d]}), held2.at[c, r1, 0], send_sem.at[1, c], recv2.at[c, r1, 1], (stage, near_a[d]))

    def forward2(r1):
        for c in range(COLORS):
            d = ORDERS[c][1]
            wait(tie2.at[c, r1], recv2.at[c, r1, 0])
            send(tie2.at[c, r1], held2.at[c, r1, 1], send_sem.at[4, c], recv2.at[c, r1, 2], (stage, near_b[d]))

    first_cols, last_cols = pl.ds(0, WIDE), pl.ds(WIDE, NARROW)

    def wide_from(c, r1, value):
        d2, d = ORDERS[c][1:]
        return (0, from_first(c, r1, {d2: pos[d2], d: value}).at[:, first_cols]), (pl.ds(1, 3), held2.at[c, r1, :, value, :, first_cols])

    def wide_ties(r1):
        for c in range(COLORS):
            d = ORDERS[c][2]
            for r2 in (1, 2, 3):
                wait(held2.at[c, r1, r2 - 1], recv2.at[c, r1, r2])
            for some, piece in wide_from(c, r1, far[d]):
                send(piece, tie3.at[c, r1, some].at[..., first_cols], send_sem.at[2, c], recv3_wide.at[c, r1], (stage, near_a[d]))

    def wide_to_b(r1):
        for c in range(COLORS):
            d = ORDERS[c][2]
            for some, piece in wide_from(c, r1, to_b[d]):
                send(piece, wide.at[r1, c, some, 3], send_sem.at[2, c], recv_wide.at[r1], (other, near_b[d]))

    def wide_to_a(r1):
        for c in range(COLORS):
            d = ORDERS[c][2]
            for some, piece in wide_from(c, r1, to_a[d]):
                send(piece, wide.at[r1, c, some, 1], send_sem.at[2, c], recv_wide.at[r1], (other, near_a[d]))
            for some, piece in wide_from(c, r1, pos[d]):
                send(piece, wide.at[r1, c, some, 0], send_sem.at[6, c], recv_wide.at[r1], (other, me))

    def wide_forward(r1):
        for c in range(COLORS):
            d = ORDERS[c][2]
            held = tie3.at[c, r1, :, :, first_cols]
            wait(held, recv3_wide.at[c, r1])
            send(held, wide.at[r1, c, :, 2], send_sem.at[5, c], recv_wide.at[r1], (other, near_b[d]))

    def narrow_from(c, value):
        d1, d2, d = ORDERS[c]
        kept = {d2: pos[d2], d: value}
        rest = tuple(kept[k] for k in range(3) if k != d1)
        return (
            (0, 0, table(c, {d1: pos[d1], **kept}).at[:, last_cols]),
            (pl.ds(1, 3), 0, held1.at[(c, slice(None)) + rest + (slice(None), last_cols)]),
            (slice(None), pl.ds(1, 3), held2.at[c, :, :, value, :, last_cols]),
        )

    def narrow_ties():
        for c in range(COLORS):
            d = ORDERS[c][2]
            for r1, r2, piece in narrow_from(c, far[d]):
                send(piece, tie3.at[c, r1, r2, :, last_cols], send_sem.at[2, c], recv3_narrow.at[c], (stage, near_a[d]))

    def narrow_to(values, near, role, own=False):
        for c in range(COLORS):
            d = ORDERS[c][2]
            for r1, r2, piece in narrow_from(c, values[d]):
                send(piece, narrow.at[(role + 1) % 4, r1, c, r2], send_sem.at[6 if own else 2, c], recv_narrow.at[(role + 1) % 4], (other, me if own else near[d]))

    def narrow_forward():
        for c in range(COLORS):
            d = ORDERS[c][2]
            held = tie3.at[c, :, :, :, last_cols]
            wait(held, recv3_narrow.at[c])
            send(held, narrow.at[3, :, c], send_sem.at[5, c], recv_narrow.at[3], (other, near_b[d]))

    side = [
        pltpu.make_async_remote_copy(src_ref=src, dst_ref=dst, send_sem=side_sem.at[0, k], recv_sem=side_sem.at[1, k], device_id=(other, me), device_id_type=MESH)
        for k, (src, dst) in enumerate(((ids_ref, ids_in), (slots_ref, slots_in), (gates_ref, gates_in), (h_ref, x_in)))
    ]
    local = [pltpu.make_async_copy(src, dst, local_sem.at[k]) for k, (src, dst) in enumerate(((norm_ref, norm_in), (wo_ref, wo_in)))]

    weights = (wq_ref, wk_ref, wv_ref)

    def load(k, i):
        slot = lax.rem(i, depth)
        return pltpu.make_async_copy(weights[k].at[pl.ds(pl.multiple_of(i * piece_rows, piece_rows), piece_rows)], raw.at[slot], raw_sem.at[slot])

    def flatten(k, start, stop):
        step = 64

        def body(i, carry):
            load(k, i).wait()
            for j in range(0, piece_rows, step):
                flat[k, pl.ds(pl.multiple_of(i * piece_rows + j, step), step), :] = raw[lax.rem(i, depth), pl.ds(j, step)].reshape(step, d_model)

            @pl.when(i + depth < pieces)
            def _():
                load(k, i + depth).start()

            return carry

        if start == 0:
            for i in range(depth):
                load(k, i).start()
        lax.fori_loop(start, stop, body, 0)

    def build_gates():
        for copy in side:
            copy.wait_recv()
        ids, slot = ids_in[...], slots_in[...]
        spot = slot - me * (COLORS * GROUP)
        colour = spot >> 3
        roles = []
        for k, shift in enumerate((4, 2, 0)):
            roles.append((sign[k] * (((ids >> shift) & 3) - pos[k])) & 3)
        first, second, third = [
            jnp.where(colour == 0, roles[ORDERS[0][k]], jnp.where(colour == 1, roles[ORDERS[1][k]], roles[ORDERS[2][k]]))
            for k in range(3)
        ]
        in_wide = (((first * COLORS + colour) * 4 + second) * 4 + third) * GROUP + (spot & 7)
        in_narrow = ((((third + 1) & 3) * 4 + first) * COLORS + colour) * (4 * GROUP) + second * GROUP + (spot & 7)
        columns = [jnp.where(slot >= 0, c, -1).astype(jnp.float32) for c in (in_wide, in_narrow)]
        both = jnp.concatenate([*columns, gates_in[...], jnp.zeros((104, seq), jnp.float32)], axis=0).T
        step = 256
        for which, g_mat in enumerate((g_wide, g_narrow)):
            for b in range(g_mat.shape[1] // step):
                col = (lax.broadcasted_iota(jnp.int32, (seq, step), 1) + b * step).astype(jnp.float32)
                val = jnp.zeros((seq, step), jnp.float32)
                for i in range(8):
                    at = which * 8 + i
                    val = jnp.where(both[:, at:at + 1] == col, both[:, 16 + i:17 + i], val)
                high = val.astype(jnp.bfloat16)
                rest = val - high.astype(jnp.float32)
                mid = rest.astype(jnp.bfloat16)
                low = (rest - mid.astype(jnp.float32)).astype(jnp.bfloat16)
                for third_of, piece in enumerate((high, mid, low)):
                    g_mat[third_of * seq:(third_of + 1) * seq, b * step:(b + 1) * step] = piece
        acc[...] = x_in[...].astype(jnp.float32)

    def add_rows(gates, blocks, cols):
        sums = jnp.dot(gates, blocks, preferred_element_type=jnp.float32)
        acc[:, cols] += sums[:seq] + (sums[seq:2 * seq] + sums[2 * seq:])

    def combine_wide(r1):
        wait(wide.at[r1], recv_wide.at[r1])
        count = COLORS * 16 * GROUP
        for b in range(WIDE // width):
            cols = slice(b * width, (b + 1) * width)
            add_rows(g_wide[:, r1 * count:(r1 + 1) * count], wide[r1, :, :, :, :, cols].reshape(count, width), cols)

    def combine_narrow(roles):
        for r in range(2 * roles, 2 * roles + 2):
            wait(narrow.at[r], recv_narrow.at[r])
        count = 2 * COLORS * 16 * GROUP
        blocks = narrow[2 * roles:2 * roles + 2].reshape(count, NARROW)
        add_rows(g_narrow[:, roles * count:(roles + 1) * count], blocks, slice(WIDE, d_model))

    def square_sum(lo, hi):
        total = jnp.zeros((seq, 1), jnp.float32)
        for b in range(lo, hi, width):
            y = acc[:, b:b + width].astype(jnp.bfloat16).astype(jnp.float32)
            acc[:, b:b + width] = y
            total += jnp.sum(y * y, axis=1, keepdims=True)
        return total

    def inverse_rms(total, count):
        return lax.rsqrt(total * (1.0 / count) + NORM_EPS)

    def scale(lo, hi, inv):
        for b in range(lo, hi, width):
            x_in[:, b:b + width] = (acc[:, b:b + width] * inv * norm_in[:, b:b + width]).astype(jnp.bfloat16)

    head = 128
    pair = 2 * head
    causal = lax.broadcasted_iota(jnp.int32, (seq, seq), 0) >= lax.broadcasted_iota(jnp.int32, (seq, seq), 1)

    def project_wide():
        for k in range(3):
            for b in range(0, d_model, pair):
                part[k, :, b:b + pair] = jnp.dot(x_in[:, :WIDE], flat[k, :WIDE, b:b + pair], preferred_element_type=jnp.float32)

    def project(k, p, ratio):
        cols = slice(p * pair, (p + 1) * pair)
        rest = jnp.dot(x_in[:, WIDE:], flat[k, WIDE:, cols], preferred_element_type=jnp.float32)
        qkv[k, :, cols] = (part[k, :, cols] * ratio + rest).astype(jnp.bfloat16)

    def softmax(cols):
        scores = jnp.where(causal, part[0, :, cols] * (head ** -0.5), -jnp.inf)
        grown = jnp.exp(scores - jnp.max(scores, axis=1, keepdims=True))
        qkv[0, :, cols] = (grown * (1.0 / jnp.sum(grown, axis=1, keepdims=True))).astype(jnp.bfloat16)

    def attend(ratio):
        spans = [slice(h * head, (h + 1) * head) for h in range(d_model // head)]
        for k in range(2):
            for p in range(d_model // pair):
                project(k, p, ratio)
        for cols in spans:
            part[0, :, cols] = lax.dot_general(qkv[0, :, cols], qkv[1, :, cols], (((1,), (1,)), ((), ())), preferred_element_type=jnp.float32)
        for p in range(d_model // pair):
            softmax(spans[2 * p])
            softmax(spans[2 * p + 1])
            project(2, p, ratio)
        for cols in spans:
            x_in[:, cols] = jnp.dot(qkv[0, :, cols], qkv[2, :, cols], preferred_element_type=jnp.float32).astype(jnp.bfloat16)

    phase1()
    for copy in side:
        copy.start()
    phase2(0)
    for copy in local:
        copy.start()
    build_gates()
    flatten(0, 0, pieces)
    flatten(1, 0, pieces // 2)
    forward1()
    phase2(3)
    flatten(1, pieces // 2, pieces)
    forward2(0)
    phase2(1)
    flatten(2, 0, pieces // 2)
    forward2(3)
    phase2(2)
    wide_ties(0)
    wide_to_b(0)
    wide_to_a(0)
    flatten(2, pieces // 2, pieces)
    forward2(1)
    wide_ties(3)
    wide_to_b(3)
    forward2(2)
    wide_forward(0)
    wide_to_a(3)
    wide_ties(1)
    wide_to_b(1)
    wide_forward(3)
    wide_ties(2)
    wide_to_b(2)
    wide_to_a(1)
    combine_wide(0)
    wide_forward(1)
    narrow_ties()
    narrow_to(to_b, near_b, 3)
    wide_to_a(2)
    combine_wide(3)
    narrow_to(to_a, near_a, 1)
    narrow_to(pos, None, 0, own=True)
    wide_forward(2)
    for copy in local:
        copy.wait()
    narrow_forward()
    combine_wide(1)
    combine_wide(2)
    wide_total = square_sum(0, WIDE)
    wide_inv = inverse_rms(wide_total, WIDE)
    scale(0, WIDE, wide_inv)
    project_wide()
    combine_narrow(0)
    combine_narrow(1)
    inv = inverse_rms(wide_total + square_sum(WIDE, d_model), d_model)
    scale(WIDE, d_model, inv)
    attend(jnp.where(wide_inv > 0.0, inv / wide_inv, 0.0))
    for b in range(d_model // pair):
        cols = slice(b * pair, (b + 1) * pair)
        out = jnp.dot(x_in[...], wo_in[:, cols], preferred_element_type=jnp.float32).astype(jnp.bfloat16)
        z_ref[:, cols] = (acc[:, cols] + out.astype(jnp.float32)).astype(jnp.bfloat16)

    for copy in side:
        copy.wait_send()
    for c in range(COLORS):
        for k, ref in enumerate((held1, held2, held2, tie1, tie2, tie3, tie3)):
            wait(ref.at[c], send_sem.at[k, c])


def run_stage(o_tab, ids, slots, gates, h, norm_w, wq, wk, wv, wo):
    seq, d = h.shape
    dma = pltpu.SemaphoreType.DMA
    block = (GROUP, d)
    piece = 128

    def buf(*lead):
        return pltpu.VMEM(lead + block, jnp.bfloat16)

    return pl.pallas_call(
        stage_kernel,
        out_shape=pltpu.VMEM((seq, d), jnp.bfloat16),
        in_specs=[pl.BlockSpec(memory_space=pl.ANY)] * 10,
        out_specs=pl.BlockSpec(memory_space=pltpu.VMEM),
        scratch_shapes=[
            pltpu.VMEM((4, COLORS, 4, 4, GROUP, WIDE), jnp.bfloat16),
            pltpu.VMEM((4, 4, COLORS, 4, GROUP, NARROW), jnp.bfloat16),
            buf(COLORS, 3, 4, 4),
            buf(COLORS, 4, 3, 4),
            buf(COLORS, 4, 4),
            buf(COLORS, 4, 4),
            buf(COLORS, 4, 4),
            pltpu.VMEM(ids.shape, jnp.int32),
            pltpu.VMEM(slots.shape, jnp.int32),
            pltpu.VMEM(gates.shape, jnp.float32),
            pltpu.VMEM((3 * seq, 64 * COLORS * GROUP), jnp.bfloat16),
            pltpu.VMEM((3 * seq, 64 * COLORS * GROUP), jnp.bfloat16),
            pltpu.VMEM((seq, d), jnp.float32),
            pltpu.VMEM(norm_w.shape, jnp.float32),
            pltpu.VMEM((3, d, d), jnp.bfloat16),
            pltpu.VMEM((d, d), jnp.bfloat16),
            pltpu.VMEM((3, piece) + wq.shape[1:], jnp.bfloat16),
            pltpu.VMEM((seq, d), jnp.bfloat16),
            pltpu.VMEM((3, seq, d), jnp.float32),
            pltpu.VMEM((3, seq, d), jnp.bfloat16),
            dma((2, 4)),
            dma((2,)),
            dma((3,)),
            dma((7, COLORS)),
            dma((COLORS, 4)),
            dma((COLORS, 4, 4)),
            dma((COLORS, 4)),
            dma((COLORS,)),
            dma((4,)),
            dma((4,)),
        ],
        compiler_params=pltpu.CompilerParams(collective_id=0, has_side_effects=True, vmem_limit_bytes=63 * 1024 * 1024),
        name='stage',
    )(o_tab, ids, slots, gates, h, norm_w, wq, wk, wv, wo)


def solution(mesh):
    tok_spec = P('pp', 'ep', None, None)
    wt_spec = P('pp', None, None, None)

    def device_step(expert_out, expert_ids, slot_ids, gate_vals, residual, norm_w, w_query, w_key, w_value, w_out):
        seq_len, d_model = residual.shape[2:]

        def choices(array):
            return array.reshape(seq_len, array.shape[3]).T

        result = run_stage(
            expert_out.reshape(SIDE, SIDE, SIDE, COLORS, GROUP, d_model),
            choices(expert_ids), choices(slot_ids), choices(gate_vals),
            residual.reshape(seq_len, d_model), norm_w, w_query[0], w_key[0], w_value[0], w_out[0].reshape(-1, d_model),
        )
        return result.reshape(residual.shape)

    return jax.shard_map(device_step, mesh=mesh, in_specs=(tok_spec, tok_spec, tok_spec, tok_spec, tok_spec, P('pp', None), wt_spec, wt_spec, wt_spec, wt_spec), out_specs=tok_spec, check_vma=False)
```

```python
import jax
import jax.numpy as jnp
from jax import lax
from jax.experimental import pallas as pl
from jax.experimental.pallas import tpu as pltpu
from jax.sharding import PartitionSpec as P

NORM_EPS = 1e-6
MESH = pl.DeviceIdType.MESH
SIDE = 4
GROUP = 8
COLORS = 3
ORDERS = ((2, 1, 0), (1, 0, 2), (0, 2, 1))
WIDE, NARROW = 1280, 768


def stage_kernel(o_ref, ids_ref, slots_ref, gates_ref, h_ref, norm_ref, wq_ref, wk_ref, wv_ref, wo_ref, z_ref, wide, narrow, held1, held2, tie1, tie2, tie3, ids_in, slots_in, gates_in, g_wide, g_narrow, acc, norm_in, flat, wo_in, raw, x_in, part, qkv, side_sem, local_sem, raw_sem, send_sem, recv1, recv2, recv3_wide, recv3_narrow, recv_wide, recv_narrow):
    stage = lax.axis_index('pp')
    me = lax.axis_index('ep')
    other = 1 - stage
    pos = (me // 16, (me // 4) % 4, me % 4)
    sign = [1 - 2 * (p % 2) for p in pos]
    to_a = [lax.rem(p + s + SIDE, SIDE) for p, s in zip(pos, sign)]
    to_b = [lax.rem(p - s + SIDE, SIDE) for p, s in zip(pos, sign)]
    far = [lax.rem(p + 2, SIDE) for p in pos]
    seq, d_model = x_in.shape
    depth, piece_rows = raw.shape[:2]
    pieces = flat.shape[1] // piece_rows

    def rank(axis, value):
        z, y, x = [value if k == axis else p for k, p in enumerate(pos)]
        return z * 16 + y * 4 + x

    near_a = [rank(k, to_a[k]) for k in range(3)]
    near_b = [rank(k, to_b[k]) for k in range(3)]

    barrier = pltpu.get_barrier_semaphore()
    peers = [(other, me)]
    for k in range(3):
        for where in (near_a[k], near_b[k]):
            peers += [(stage, where), (other, where)]
    for peer in peers:
        pl.semaphore_signal(barrier, inc=1, device_id=peer, device_id_type=MESH)
    pl.semaphore_wait(barrier, len(peers))

    def send(src, dst, send_s, recv_s, peer):
        pltpu.make_async_remote_copy(src_ref=src, dst_ref=dst, send_sem=send_s, recv_sem=recv_s, device_id=peer, device_id_type=MESH).start()

    def wait(ref, sem):
        pltpu.make_async_copy(ref, ref, sem).wait()

    def table(c, fixed):
        return o_ref.at[tuple(fixed.get(k, slice(None)) for k in range(3)) + (c,)]

    def from_first(c, r1, fixed):
        d1 = ORDERS[c][0]
        if r1 == 0:
            return table(c, {d1: pos[d1], **fixed})
        return held1.at[(c, r1 - 1) + tuple(fixed.get(k, slice(None)) for k in range(3) if k != d1)]

    def phase1():
        for c in range(COLORS):
            d = ORDERS[c][0]
            send(table(c, {d: far[d]}), tie1.at[c], send_sem.at[0, c], recv1.at[c, 0], (stage, near_a[d]))
        for c in range(COLORS):
            d = ORDERS[c][0]
            send(table(c, {d: to_b[d]}), held1.at[c, 2], send_sem.at[0, c], recv1.at[c, 3], (stage, near_b[d]))
        for c in range(COLORS):
            d = ORDERS[c][0]
            send(table(c, {d: to_a[d]}), held1.at[c, 0], send_sem.at[0, c], recv1.at[c, 1], (stage, near_a[d]))

    def forward1():
        for c in range(COLORS):
            d = ORDERS[c][0]
            wait(tie1.at[c], recv1.at[c, 0])
            send(tie1.at[c], held1.at[c, 1], send_sem.at[3, c], recv1.at[c, 2], (stage, near_b[d]))

    def phase2(r1):
        for c in range(COLORS):
            d = ORDERS[c][1]
            if r1:
                wait(held1.at[c, r1 - 1], recv1.at[c, r1])
            send(from_first(c, r1, {d: to_b[d]}), held2.at[c, r1, 2], send_sem.at[1, c], recv2.at[c, r1, 3], (stage, near_b[d]))
            send(from_first(c, r1, {d: far[d]}), tie2.at[c, r1], send_sem.at[1, c], recv2.at[c, r1, 0], (stage, near_a[d]))
            send(from_first(c, r1, {d: to_a[d]}), held2.at[c, r1, 0], send_sem.at[1, c], recv2.at[c, r1, 1], (stage, near_a[d]))

    def forward2(r1):
        for c in range(COLORS):
            d = ORDERS[c][1]
            wait(tie2.at[c, r1], recv2.at[c, r1, 0])
            send(tie2.at[c, r1], held2.at[c, r1, 1], send_sem.at[4, c], recv2.at[c, r1, 2], (stage, near_b[d]))

    first_cols, last_cols = pl.ds(0, WIDE), pl.ds(WIDE, NARROW)

    def wide_from(c, r1, value):
        d2, d = ORDERS[c][1:]
        return (0, from_first(c, r1, {d2: pos[d2], d: value}).at[:, first_cols]), (pl.ds(1, 3), held2.at[c, r1, :, value, :, first_cols])

    def wide_ties(r1):
        for c in range(COLORS):
            d = ORDERS[c][2]
            for r2 in (1, 2, 3):
                wait(held2.at[c, r1, r2 - 1], recv2.at[c, r1, r2])
            for some, piece in wide_from(c, r1, far[d]):
                send(piece, tie3.at[c, r1, some].at[..., first_cols], send_sem.at[2, c], recv3_wide.at[c, r1], (stage, near_a[d]))

    def wide_to_b(r1):
        for c in range(COLORS):
            d = ORDERS[c][2]
            for some, piece in wide_from(c, r1, to_b[d]):
                send(piece, wide.at[r1, c, some, 3], send_sem.at[2, c], recv_wide.at[r1], (other, near_b[d]))

    def wide_to_a(r1):
        for c in range(COLORS):
            d = ORDERS[c][2]
            for some, piece in wide_from(c, r1, to_a[d]):
                send(piece, wide.at[r1, c, some, 1], send_sem.at[2, c], recv_wide.at[r1], (other, near_a[d]))
            for some, piece in wide_from(c, r1, pos[d]):
                send(piece, wide.at[r1, c, some, 0], send_sem.at[6, c], recv_wide.at[r1], (other, me))

    def wide_forward(r1):
        for c in range(COLORS):
            d = ORDERS[c][2]
            held = tie3.at[c, r1, :, :, first_cols]
            wait(held, recv3_wide.at[c, r1])
            send(held, wide.at[r1, c, :, 2], send_sem.at[5, c], recv_wide.at[r1], (other, near_b[d]))

    def narrow_from(c, value):
        d1, d2, d = ORDERS[c]
        kept = {d2: pos[d2], d: value}
        rest = tuple(kept[k] for k in range(3) if k != d1)
        return (
            (0, 0, table(c, {d1: pos[d1], **kept}).at[:, last_cols]),
            (pl.ds(1, 3), 0, held1.at[(c, slice(None)) + rest + (slice(None), last_cols)]),
            (slice(None), pl.ds(1, 3), held2.at[c, :, :, value, :, last_cols]),
        )

    def narrow_ties():
        for c in range(COLORS):
            d = ORDERS[c][2]
            for r1, r2, piece in narrow_from(c, far[d]):
                send(piece, tie3.at[c, r1, r2, :, last_cols], send_sem.at[2, c], recv3_narrow.at[c], (stage, near_a[d]))

    def narrow_to(values, near, role, own=False):
        for c in range(COLORS):
            d = ORDERS[c][2]
            for r1, r2, piece in narrow_from(c, values[d]):
                send(piece, narrow.at[(role + 1) % 4, r1, c, r2], send_sem.at[6 if own else 2, c], recv_narrow.at[(role + 1) % 4], (other, me if own else near[d]))

    def narrow_forward():
        for c in range(COLORS):
            d = ORDERS[c][2]
            held = tie3.at[c, :, :, :, last_cols]
            wait(held, recv3_narrow.at[c])
            send(held, narrow.at[3, :, c], send_sem.at[5, c], recv_narrow.at[3], (other, near_b[d]))

    side = [
        pltpu.make_async_remote_copy(src_ref=src, dst_ref=dst, send_sem=side_sem.at[0, k], recv_sem=side_sem.at[1, k], device_id=(other, me), device_id_type=MESH)
        for k, (src, dst) in enumerate(((ids_ref, ids_in), (slots_ref, slots_in), (gates_ref, gates_in), (h_ref, x_in)))
    ]
    local = [pltpu.make_async_copy(src, dst, local_sem.at[k]) for k, (src, dst) in enumerate(((norm_ref, norm_in), (wo_ref, wo_in)))]

    weights = (wq_ref, wk_ref, wv_ref)

    def load(k, i):
        slot = lax.rem(i, depth)
        return pltpu.make_async_copy(weights[k].at[pl.ds(pl.multiple_of(i * piece_rows, piece_rows), piece_rows)], raw.at[slot], raw_sem.at[slot])

    def flatten(k, start, stop):
        step = 64

        def body(i, carry):
            load(k, i).wait()
            for j in range(0, piece_rows, step):
                flat[k, pl.ds(pl.multiple_of(i * piece_rows + j, step), step), :] = raw[lax.rem(i, depth), pl.ds(j, step)].reshape(step, d_model)

            @pl.when(i + depth < pieces)
            def _():
                load(k, i + depth).start()

            return carry

        if start == 0:
            for i in range(depth):
                load(k, i).start()
        lax.fori_loop(start, stop, body, 0)

    def build_gates():
        for copy in side:
            copy.wait_recv()
        ids, slot = ids_in[...], slots_in[...]
        spot = slot - me * (COLORS * GROUP)
        colour = spot >> 3
        roles = []
        for k, shift in enumerate((4, 2, 0)):
            roles.append((sign[k] * (((ids >> shift) & 3) - pos[k])) & 3)
        first, second, third = [
            jnp.where(colour == 0, roles[ORDERS[0][k]], jnp.where(colour == 1, roles[ORDERS[1][k]], roles[ORDERS[2][k]]))
            for k in range(3)
        ]
        in_wide = (((first * COLORS + colour) * 4 + second) * 4 + third) * GROUP + (spot & 7)
        in_narrow = ((((third + 1) & 3) * 4 + first) * COLORS + colour) * (4 * GROUP) + second * GROUP + (spot & 7)
        columns = [jnp.where(slot >= 0, c, -1).astype(jnp.float32) for c in (in_wide, in_narrow)]
        both = jnp.concatenate([*columns, gates_in[...], jnp.zeros((104, seq), jnp.float32)], axis=0).T
        step = 256
        for which, g_mat in enumerate((g_wide, g_narrow)):
            for b in range(g_mat.shape[1] // step):
                col = (lax.broadcasted_iota(jnp.int32, (seq, step), 1) + b * step).astype(jnp.float32)
                val = jnp.zeros((seq, step), jnp.float32)
                for i in range(8):
                    at = which * 8 + i
                    val = jnp.where(both[:, at:at + 1] == col, both[:, 16 + i:17 + i], val)
                high = val.astype(jnp.bfloat16)
                rest = val - high.astype(jnp.float32)
                mid = rest.astype(jnp.bfloat16)
                low = (rest - mid.astype(jnp.float32)).astype(jnp.bfloat16)
                for third_of, piece in enumerate((high, mid, low)):
                    g_mat[third_of * seq:(third_of + 1) * seq, b * step:(b + 1) * step] = piece
        acc[...] = x_in[...].astype(jnp.float32)

    def add_rows(gates, blocks, cols):
        sums = jnp.dot(gates, blocks, preferred_element_type=jnp.float32)
        acc[:, cols] += sums[:seq] + (sums[seq:2 * seq] + sums[2 * seq:])

    def combine_wide(r1):
        wait(wide.at[r1], recv_wide.at[r1])
        count = COLORS * 16 * GROUP
        for cols in spans(0, WIDE):
            add_rows(g_wide[:, r1 * count:(r1 + 1) * count], wide[r1, :, :, :, :, cols].reshape(count, -1), cols)

    def combine_narrow(roles):
        for r in range(2 * roles, 2 * roles + 2):
            wait(narrow.at[r], recv_narrow.at[r])
        count = 2 * COLORS * 16 * GROUP
        for cols in spans(0, NARROW):
            blocks = narrow[2 * roles:2 * roles + 2, :, :, :, :, cols].reshape(count, -1)
            add_rows(g_narrow[:, roles * count:(roles + 1) * count], blocks, slice(WIDE + cols.start, WIDE + cols.stop))

    def square_sum(lo, hi):
        total = jnp.zeros((seq, 1), jnp.float32)
        for cols in spans(lo, hi):
            y = acc[:, cols].astype(jnp.bfloat16).astype(jnp.float32)
            acc[:, cols] = y
            total += jnp.sum(y * y, axis=1, keepdims=True)
        return total

    def inverse_rms(total, count):
        return lax.rsqrt(total * (1.0 / count) + NORM_EPS)

    def scale(lo, hi, inv):
        for cols in spans(lo, hi):
            x_in[:, cols] = (acc[:, cols] * inv * norm_in[:, cols]).astype(jnp.bfloat16)

    head = 128
    pair = 2 * head
    causal = lax.broadcasted_iota(jnp.int32, (seq, seq), 0) >= lax.broadcasted_iota(jnp.int32, (seq, seq), 1)

    def project_wide():
        for k in range(3):
            for b in range(0, d_model, pair):
                part[k, :, b:b + pair] = jnp.dot(x_in[:, :WIDE], flat[k, :WIDE, b:b + pair], preferred_element_type=jnp.float32)

    def project(k, p, ratio):
        cols = slice(p * pair, (p + 1) * pair)
        rest = jnp.dot(x_in[:, WIDE:], flat[k, WIDE:, cols], preferred_element_type=jnp.float32)
        qkv[k, :, cols] = (part[k, :, cols] * ratio + rest).astype(jnp.bfloat16)

    def softmax(cols):
        scores = jnp.where(causal, part[0, :, cols] * (head ** -0.5), -jnp.inf)
        grown = jnp.exp(scores - jnp.max(scores, axis=1, keepdims=True))
        qkv[0, :, cols] = (grown * (1.0 / jnp.sum(grown, axis=1, keepdims=True))).astype(jnp.bfloat16)

    def attend(ratio):
        heads = [slice(h * head, (h + 1) * head) for h in range(d_model // head)]
        for k in range(2):
            for p in range(d_model // pair):
                project(k, p, ratio)
        for cols in heads:
            part[0, :, cols] = lax.dot_general(qkv[0, :, cols], qkv[1, :, cols], (((1,), (1,)), ((), ())), preferred_element_type=jnp.float32)
        for p in range(d_model // pair):
            softmax(heads[2 * p])
            softmax(heads[2 * p + 1])
            project(2, p, ratio)
        for cols in heads:
            x_in[:, cols] = jnp.dot(qkv[0, :, cols], qkv[2, :, cols], preferred_element_type=jnp.float32).astype(jnp.bfloat16)

    phase1()
    for copy in side:
        copy.start()
    phase2(0)
    for copy in local:
        copy.start()
    build_gates()
    flatten(0, 0, pieces)
    flatten(1, 0, pieces // 2)
    forward1()
    phase2(3)
    flatten(1, pieces // 2, pieces)
    forward2(0)
    phase2(1)
    flatten(2, 0, pieces // 2)
    forward2(3)
    phase2(2)
    wide_ties(0)
    wide_to_b(0)
    wide_to_a(0)
    flatten(2, pieces // 2, pieces)
    forward2(1)
    wide_ties(3)
    wide_to_b(3)
    forward2(2)
    wide_forward(0)
    wide_to_a(3)
    wide_ties(1)
    wide_to_b(1)
    wide_forward(3)
    wide_ties(2)
    wide_to_b(2)
    wide_to_a(1)
    combine_wide(0)
    wide_forward(1)
    narrow_ties()
    narrow_to(to_b, near_b, 3)
    wide_to_a(2)
    combine_wide(3)
    narrow_to(to_a, near_a, 1)
    narrow_to(pos, None, 0, own=True)
    wide_forward(2)
    for copy in local:
        copy.wait()
    narrow_forward()
    combine_wide(1)
    combine_wide(2)
    wide_total = square_sum(0, WIDE)
    wide_inv = inverse_rms(wide_total, WIDE)
    scale(0, WIDE, wide_inv)
    project_wide()
    combine_narrow(0)
    combine_narrow(1)
    inv = inverse_rms(wide_total + square_sum(WIDE, d_model), d_model)
    scale(WIDE, d_model, inv)
    attend(jnp.where(wide_inv > 0.0, inv / wide_inv, 0.0))
    for b in range(d_model // pair):
        cols = slice(b * pair, (b + 1) * pair)
        out = jnp.dot(x_in[...], wo_in[:, cols], preferred_element_type=jnp.float32).astype(jnp.bfloat16)
        z_ref[:, cols] = (acc[:, cols] + out.astype(jnp.float32)).astype(jnp.bfloat16)

    for copy in side:
        copy.wait_send()
    for c in range(COLORS):
        for k, ref in enumerate((held1, held2, held2, tie1, tie2, tie3, tie3)):
            wait(ref.at[c], send_sem.at[k, c])


def spans(lo, hi):
    return [slice(b, min(b + 512, hi)) for b in range(lo, hi, 512)]


def run_stage(o_tab, ids, slots, gates, h, norm_w, wq, wk, wv, wo):
    seq, d = h.shape
    dma = pltpu.SemaphoreType.DMA
    block = (GROUP, d)
    piece = 128

    def buf(*lead):
        return pltpu.VMEM(lead + block, jnp.bfloat16)

    return pl.pallas_call(
        stage_kernel,
        out_shape=pltpu.VMEM((seq, d), jnp.bfloat16),
        in_specs=[pl.BlockSpec(memory_space=pl.ANY)] * 10,
        out_specs=pl.BlockSpec(memory_space=pltpu.VMEM),
        scratch_shapes=[
            pltpu.VMEM((4, COLORS, 4, 4, GROUP, WIDE), jnp.bfloat16),
            pltpu.VMEM((4, 4, COLORS, 4, GROUP, NARROW), jnp.bfloat16),
            buf(COLORS, 3, 4, 4),
            buf(COLORS, 4, 3, 4),
            buf(COLORS, 4, 4),
            buf(COLORS, 4, 4),
            buf(COLORS, 4, 4),
            pltpu.VMEM(ids.shape, jnp.int32),
            pltpu.VMEM(slots.shape, jnp.int32),
            pltpu.VMEM(gates.shape, jnp.float32),
            pltpu.VMEM((3 * seq, 64 * COLORS * GROUP), jnp.bfloat16),
            pltpu.VMEM((3 * seq, 64 * COLORS * GROUP), jnp.bfloat16),
            pltpu.VMEM((seq, d), jnp.float32),
            pltpu.VMEM(norm_w.shape, jnp.float32),
            pltpu.VMEM((3, d, d), jnp.bfloat16),
            pltpu.VMEM((d, d), jnp.bfloat16),
            pltpu.VMEM((3, piece) + wq.shape[1:], jnp.bfloat16),
            pltpu.VMEM((seq, d), jnp.bfloat16),
            pltpu.VMEM((3, seq, d), jnp.float32),
            pltpu.VMEM((3, seq, d), jnp.bfloat16),
            dma((2, 4)),
            dma((2,)),
            dma((3,)),
            dma((7, COLORS)),
            dma((COLORS, 4)),
            dma((COLORS, 4, 4)),
            dma((COLORS, 4)),
            dma((COLORS,)),
            dma((4,)),
            dma((4,)),
        ],
        compiler_params=pltpu.CompilerParams(collective_id=0, has_side_effects=True, vmem_limit_bytes=63 * 1024 * 1024),
        name='stage',
    )(o_tab, ids, slots, gates, h, norm_w, wq, wk, wv, wo)


def solution(mesh):
    tok_spec = P('pp', 'ep', None, None)
    wt_spec = P('pp', None, None, None)

    def device_step(expert_out, expert_ids, slot_ids, gate_vals, residual, norm_w, w_query, w_key, w_value, w_out):
        seq_len, d_model = residual.shape[2:]

        def choices(array):
            return array.reshape(seq_len, array.shape[3]).T

        result = run_stage(
            expert_out.reshape(SIDE, SIDE, SIDE, COLORS, GROUP, d_model),
            choices(expert_ids), choices(slot_ids), choices(gate_vals),
            residual.reshape(seq_len, d_model), norm_w, w_query[0], w_key[0], w_value[0], w_out[0].reshape(-1, d_model),
        )
        return result.reshape(residual.shape)

    return jax.shard_map(device_step, mesh=mesh, in_specs=(tok_spec, tok_spec, tok_spec, tok_spec, tok_spec, P('pp', None), wt_spec, wt_spec, wt_spec, wt_spec), out_specs=tok_spec, check_vma=False)
```

```python
import jax
import jax.numpy as jnp
from jax import lax
from jax.experimental import pallas as pl
from jax.experimental.pallas import tpu as pltpu
from jax.sharding import PartitionSpec as P

NORM_EPS = 1e-6
MESH = pl.DeviceIdType.MESH
SIDE = 4
GROUP = 8
COLORS = 3
ORDERS = ((2, 1, 0), (1, 0, 2), (0, 2, 1))
WIDE, NARROW = 1024, 512


def stage_kernel(o_ref, ids_ref, slots_ref, gates_ref, h_ref, norm_ref, wq_ref, wk_ref, wv_ref, wo_ref, z_ref, wide, narrow, held1, held2, tie1, tie2, tie3, ids_in, slots_in, gates_in, g_wide, g_narrow, acc, norm_in, flat, wo_in, raw, x_in, part, qkv, side_sem, local_sem, raw_sem, send_sem, recv1, recv2, recv3_wide, recv3_narrow, recv_wide, recv_narrow):
    stage = lax.axis_index('pp')
    me = lax.axis_index('ep')
    other = 1 - stage
    pos = (me // 16, (me // 4) % 4, me % 4)
    sign = [1 - 2 * (p % 2) for p in pos]
    to_a = [lax.rem(p + s + SIDE, SIDE) for p, s in zip(pos, sign)]
    to_b = [lax.rem(p - s + SIDE, SIDE) for p, s in zip(pos, sign)]
    far = [lax.rem(p + 2, SIDE) for p in pos]
    seq, d_model = x_in.shape
    depth, piece_rows = raw.shape[:2]
    pieces = flat.shape[1] // piece_rows

    def rank(axis, value):
        z, y, x = [value if k == axis else p for k, p in enumerate(pos)]
        return z * 16 + y * 4 + x

    near_a = [rank(k, to_a[k]) for k in range(3)]
    near_b = [rank(k, to_b[k]) for k in range(3)]

    barrier = pltpu.get_barrier_semaphore()
    peers = [(other, me)]
    for k in range(3):
        for where in (near_a[k], near_b[k]):
            peers += [(stage, where), (other, where)]
    for peer in peers:
        pl.semaphore_signal(barrier, inc=1, device_id=peer, device_id_type=MESH)
    pl.semaphore_wait(barrier, len(peers))

    def send(src, dst, send_s, recv_s, peer):
        pltpu.make_async_remote_copy(src_ref=src, dst_ref=dst, send_sem=send_s, recv_sem=recv_s, device_id=peer, device_id_type=MESH).start()

    def wait(ref, sem):
        pltpu.make_async_copy(ref, ref, sem).wait()

    def table(c, fixed):
        return o_ref.at[tuple(fixed.get(k, slice(None)) for k in range(3)) + (c,)]

    def from_first(c, r1, fixed):
        d1 = ORDERS[c][0]
        if r1 == 0:
            return table(c, {d1: pos[d1], **fixed})
        return held1.at[(c, r1 - 1) + tuple(fixed.get(k, slice(None)) for k in range(3) if k != d1)]

    def phase1():
        for c in range(COLORS):
            d = ORDERS[c][0]
            for half in range(2):
                send(table(c, {d: far[d], (d == 0) * 1: pl.ds(2 * half, 2)}), tie1.at[c, pl.ds(2 * half, 2)], send_sem.at[0, c], recv1.at[c, 4 * half], (stage, near_a[d]))
        for c in range(COLORS):
            d = ORDERS[c][0]
            send(table(c, {d: to_b[d]}), held1.at[c, 2], send_sem.at[0, c], recv1.at[c, 3], (stage, near_b[d]))
        for c in range(COLORS):
            d = ORDERS[c][0]
            send(table(c, {d: to_a[d]}), held1.at[c, 0], send_sem.at[0, c], recv1.at[c, 1], (stage, near_a[d]))

    def forward1(half):
        some = pl.ds(2 * half, 2)
        for c in range(COLORS):
            d = ORDERS[c][0]
            wait(tie1.at[c, some], recv1.at[c, 4 * half])
            send(tie1.at[c, some], held1.at[c, 1, some], send_sem.at[3, c], recv1.at[c, 2], (stage, near_b[d]))

    def phase2(r1):
        for c in range(COLORS):
            d = ORDERS[c][1]
            if r1:
                wait(held1.at[c, r1 - 1], recv1.at[c, r1])
            send(from_first(c, r1, {d: to_b[d]}), held2.at[c, r1, 2], send_sem.at[1, c], recv2.at[c, r1, 3], (stage, near_b[d]))
            send(from_first(c, r1, {d: far[d]}), tie2.at[c, r1], send_sem.at[1, c], recv2.at[c, r1, 0], (stage, near_a[d]))
            send(from_first(c, r1, {d: to_a[d]}), held2.at[c, r1, 0], send_sem.at[1, c], recv2.at[c, r1, 1], (stage, near_a[d]))

    def forward2(r1):
        for c in range(COLORS):
            d = ORDERS[c][1]
            wait(tie2.at[c, r1], recv2.at[c, r1, 0])
            send(tie2.at[c, r1], held2.at[c, r1, 1], send_sem.at[4, c], recv2.at[c, r1, 2], (stage, near_b[d]))

    first_cols = pl.ds(0, WIDE)
    narrow_at = (WIDE, WIDE + NARROW)
    narrow_cols = [pl.ds(at, NARROW) for at in narrow_at]

    def wide_from(c, r1, value):
        d2, d = ORDERS[c][1:]
        return (0, from_first(c, r1, {d2: pos[d2], d: value}).at[:, first_cols]), (pl.ds(1, 3), held2.at[c, r1, :, value, :, first_cols])

    def wide_ties(r1):
        for c in range(COLORS):
            d = ORDERS[c][2]
            for r2 in (1, 2, 3):
                wait(held2.at[c, r1, r2 - 1], recv2.at[c, r1, r2])
            for some, piece in wide_from(c, r1, far[d]):
                send(piece, tie3.at[c, r1, some].at[..., first_cols], send_sem.at[2, c], recv3_wide.at[c, r1], (stage, near_a[d]))

    def wide_to_b(r1):
        for c in range(COLORS):
            d = ORDERS[c][2]
            for some, piece in wide_from(c, r1, to_b[d]):
                send(piece, wide.at[r1, c, some, 3], send_sem.at[2, c], recv_wide.at[r1], (other, near_b[d]))

    def wide_to_a(r1):
        for c in range(COLORS):
            d = ORDERS[c][2]
            for some, piece in wide_from(c, r1, to_a[d]):
                send(piece, wide.at[r1, c, some, 1], send_sem.at[2, c], recv_wide.at[r1], (other, near_a[d]))
            for some, piece in wide_from(c, r1, pos[d]):
                send(piece, wide.at[r1, c, some, 0], send_sem.at[6, c], recv_wide.at[r1], (other, me))

    def wide_forward(r1):
        for c in range(COLORS):
            d = ORDERS[c][2]
            held = tie3.at[c, r1, :, :, first_cols]
            wait(held, recv3_wide.at[c, r1])
            send(held, wide.at[r1, c, :, 2], send_sem.at[5, c], recv_wide.at[r1], (other, near_b[d]))

    def narrow_from(n, c, value):
        d1, d2, d = ORDERS[c]
        kept = {d2: pos[d2], d: value}
        rest = tuple(kept[k] for k in range(3) if k != d1)
        cols = narrow_cols[n]
        return (
            (0, 0, table(c, {d1: pos[d1], **kept}).at[:, cols]),
            (pl.ds(1, 3), 0, held1.at[(c, slice(None)) + rest + (slice(None), cols)]),
            (slice(None), pl.ds(1, 3), held2.at[c, :, :, value, :, cols]),
        )

    def narrow_ties(n):
        for c in range(COLORS):
            d = ORDERS[c][2]
            for r1, r2, piece in narrow_from(n, c, far[d]):
                send(piece, tie3.at[c, r1, r2, :, narrow_cols[n]], send_sem.at[2, c], recv3_narrow.at[n, c], (stage, near_a[d]))

    def narrow_to(n, values, near, role, own=False):
        for c in range(COLORS):
            d = ORDERS[c][2]
            for r1, r2, piece in narrow_from(n, c, values[d]):
                send(piece, narrow.at[n, (role + 1) % 4, r1, c, r2], send_sem.at[6 if own else 2, c], recv_narrow.at[n, (role + 1) % 4], (other, me if own else near[d]))

    def narrow_forward(n):
        for c in range(COLORS):
            d = ORDERS[c][2]
            held = tie3.at[c, :, :, :, narrow_cols[n]]
            wait(held, recv3_narrow.at[n, c])
            send(held, narrow.at[n, 3, :, c], send_sem.at[5, c], recv_narrow.at[n, 3], (other, near_b[d]))

    side = [
        pltpu.make_async_remote_copy(src_ref=src, dst_ref=dst, send_sem=side_sem.at[0, k], recv_sem=side_sem.at[1, k], device_id=(other, me), device_id_type=MESH)
        for k, (src, dst) in enumerate(((ids_ref, ids_in), (slots_ref, slots_in), (gates_ref, gates_in), (h_ref, x_in)))
    ]
    local = [pltpu.make_async_copy(src, dst, local_sem.at[k]) for k, (src, dst) in enumerate(((norm_ref, norm_in), (wo_ref, wo_in)))]

    weights = (wq_ref, wk_ref, wv_ref)

    def load(k, i):
        slot = lax.rem(i, depth)
        return pltpu.make_async_copy(weights[k].at[pl.ds(pl.multiple_of(i * piece_rows, piece_rows), piece_rows)], raw.at[slot], raw_sem.at[slot])

    def flatten(k, start, stop):
        step = 64

        def body(i, carry):
            load(k, i).wait()
            for j in range(0, piece_rows, step):
                flat[k, pl.ds(pl.multiple_of(i * piece_rows + j, step), step), :] = raw[lax.rem(i, depth), pl.ds(j, step)].reshape(step, d_model)

            @pl.when(i + depth < pieces)
            def _():
                load(k, i + depth).start()

            return carry

        if start == 0:
            for i in range(depth):
                load(k, i).start()
        lax.fori_loop(start, stop, body, 0)

    def build_gates():
        for copy in side:
            copy.wait_recv()
        ids, slot = ids_in[...], slots_in[...]
        spot = slot - me * (COLORS * GROUP)
        colour = spot >> 3
        roles = []
        for k, shift in enumerate((4, 2, 0)):
            roles.append((sign[k] * (((ids >> shift) & 3) - pos[k])) & 3)
        first, second, third = [
            jnp.where(colour == 0, roles[ORDERS[0][k]], jnp.where(colour == 1, roles[ORDERS[1][k]], roles[ORDERS[2][k]]))
            for k in range(3)
        ]
        in_wide = (((first * COLORS + colour) * 4 + second) * 4 + third) * GROUP + (spot & 7)
        in_narrow = ((((third + 1) & 3) * 4 + first) * COLORS + colour) * (4 * GROUP) + second * GROUP + (spot & 7)
        columns = [jnp.where(slot >= 0, c, -1).astype(jnp.float32) for c in (in_wide, in_narrow)]
        both = jnp.concatenate([*columns, gates_in[...], jnp.zeros((104, seq), jnp.float32)], axis=0).T
        step = 256
        for which, g_mat in enumerate((g_wide, g_narrow)):
            for b in range(g_mat.shape[1] // step):
                col = (lax.broadcasted_iota(jnp.int32, (seq, step), 1) + b * step).astype(jnp.float32)
                val = jnp.zeros((seq, step), jnp.float32)
                for i in range(8):
                    at = which * 8 + i
                    val = jnp.where(both[:, at:at + 1] == col, both[:, 16 + i:17 + i], val)
                high = val.astype(jnp.bfloat16)
                rest = val - high.astype(jnp.float32)
                mid = rest.astype(jnp.bfloat16)
                low = (rest - mid.astype(jnp.float32)).astype(jnp.bfloat16)
                for third_of, piece in enumerate((high, mid, low)):
                    g_mat[third_of * seq:(third_of + 1) * seq, b * step:(b + 1) * step] = piece
        acc[...] = x_in[...].astype(jnp.float32)

    def add_rows(gates, blocks, cols):
        sums = jnp.dot(gates, blocks, preferred_element_type=jnp.float32)
        acc[:, cols] += sums[:seq] + (sums[seq:2 * seq] + sums[2 * seq:])

    def combine_wide(r1):
        wait(wide.at[r1], recv_wide.at[r1])
        count = COLORS * 16 * GROUP
        for cols in spans(0, WIDE):
            add_rows(g_wide[:, r1 * count:(r1 + 1) * count], wide[r1, :, :, :, :, cols].reshape(count, -1), cols)

    def combine_narrow(n, roles):
        for r in range(2 * roles, 2 * roles + 2):
            wait(narrow.at[n, r], recv_narrow.at[n, r])
        count = 2 * COLORS * 16 * GROUP
        blocks = narrow[n, 2 * roles:2 * roles + 2].reshape(count, NARROW)
        add_rows(g_narrow[:, roles * count:(roles + 1) * count], blocks, slice(narrow_at[n], narrow_at[n] + NARROW))

    def square_sum(lo, hi):
        total = jnp.zeros((seq, 1), jnp.float32)
        for cols in spans(lo, hi):
            y = acc[:, cols].astype(jnp.bfloat16).astype(jnp.float32)
            acc[:, cols] = y
            total += jnp.sum(y * y, axis=1, keepdims=True)
        return total

    def inverse_rms(total, count):
        return lax.rsqrt(total * (1.0 / count) + NORM_EPS)

    def scale(lo, hi, inv):
        for cols in spans(lo, hi):
            x_in[:, cols] = (acc[:, cols] * inv * norm_in[:, cols]).astype(jnp.bfloat16)

    head = 128
    pair = 2 * head
    causal = lax.broadcasted_iota(jnp.int32, (seq, seq), 0) >= lax.broadcasted_iota(jnp.int32, (seq, seq), 1)

    def project_wide():
        for k in range(3):
            for b in range(0, d_model, pair):
                part[k, :, b:b + pair] = jnp.dot(x_in[:, :WIDE], flat[k, :WIDE, b:b + pair], preferred_element_type=jnp.float32)

    def project(k, p, n, ratio):
        cols = slice(p * pair, (p + 1) * pair)
        rows = slice(narrow_at[n], narrow_at[n] + NARROW)
        total = part[k, :, cols] * ratio + jnp.dot(x_in[:, rows], flat[k, rows, cols], preferred_element_type=jnp.float32)
        if n == 0:
            part[k, :, cols] = total
        else:
            qkv[k, :, cols] = total.astype(jnp.bfloat16)

    def grow(total, inv, n):
        stop = narrow_at[n] + NARROW
        total = total + square_sum(narrow_at[n], stop)
        new_inv = inverse_rms(total, stop)
        scale(narrow_at[n], stop, new_inv)
        return total, new_inv, jnp.where(inv > 0.0, new_inv / inv, 0.0)

    def softmax(cols):
        scores = jnp.where(causal, part[0, :, cols] * (head ** -0.5), -jnp.inf)
        grown = jnp.exp(scores - jnp.max(scores, axis=1, keepdims=True))
        qkv[0, :, cols] = (grown * (1.0 / jnp.sum(grown, axis=1, keepdims=True))).astype(jnp.bfloat16)

    def attend(ratio):
        heads = [slice(h * head, (h + 1) * head) for h in range(d_model // head)]
        for k in range(2):
            for p in range(d_model // pair):
                project(k, p, 1, ratio)
        for cols in heads:
            part[0, :, cols] = lax.dot_general(qkv[0, :, cols], qkv[1, :, cols], (((1,), (1,)), ((), ())), preferred_element_type=jnp.float32)
        for p in range(d_model // pair):
            softmax(heads[2 * p])
            softmax(heads[2 * p + 1])
            project(2, p, 1, ratio)
        for cols in heads:
            x_in[:, cols] = jnp.dot(qkv[0, :, cols], qkv[2, :, cols], preferred_element_type=jnp.float32).astype(jnp.bfloat16)

    phase1()
    for copy in side:
        copy.start()
    phase2(0)
    for copy in local:
        copy.start()
    build_gates()
    flatten(0, 0, pieces // 2)
    forward1(0)
    flatten(0, pieces // 2, pieces)
    forward1(1)
    phase2(3)
    flatten(1, 0, pieces)
    forward2(0)
    phase2(1)
    flatten(2, 0, pieces // 2)
    forward2(3)
    phase2(2)
    wide_ties(0)
    wide_to_b(0)
    flatten(2, pieces // 2, pieces)
    forward2(1)
    wide_ties(3)
    wide_to_b(3)
    wide_to_a(0)
    forward2(2)
    wide_ties(1)
    wide_to_b(1)
    wide_to_a(3)
    wide_forward(0)
    wide_forward(3)
    wide_ties(2)
    wide_to_b(2)
    wide_to_a(1)
    narrow_ties(0)
    wide_to_a(2)
    narrow_ties(1)
    for n in range(2):
        narrow_to(n, to_a, near_a, 1)
        narrow_to(n, pos, None, 0, own=True)
    wide_forward(1)
    narrow_to(0, to_b, near_b, 3)
    combine_wide(0)
    wide_forward(2)
    narrow_to(1, to_b, near_b, 3)
    for copy in local:
        copy.wait()
    combine_wide(3)
    combine_wide(1)
    narrow_forward(0)
    combine_wide(2)
    narrow_forward(1)
    total = square_sum(0, WIDE)
    inv = inverse_rms(total, WIDE)
    scale(0, WIDE, inv)
    project_wide()
    combine_narrow(0, 0)
    combine_narrow(0, 1)
    total, inv, ratio = grow(total, inv, 0)
    for k in range(3):
        for p in range(d_model // pair):
            project(k, p, 0, ratio)
    combine_narrow(1, 0)
    combine_narrow(1, 1)
    total, inv, ratio = grow(total, inv, 1)
    attend(ratio)
    for b in range(d_model // pair):
        cols = slice(b * pair, (b + 1) * pair)
        out = jnp.dot(x_in[...], wo_in[:, cols], preferred_element_type=jnp.float32).astype(jnp.bfloat16)
        z_ref[:, cols] = (acc[:, cols] + out.astype(jnp.float32)).astype(jnp.bfloat16)

    for copy in side:
        copy.wait_send()
    for c in range(COLORS):
        for k, ref in enumerate((held1, held2, held2, tie1, tie2, tie3, tie3)):
            wait(ref.at[c], send_sem.at[k, c])


def spans(lo, hi):
    return [slice(b, min(b + 512, hi)) for b in range(lo, hi, 512)]


def run_stage(o_tab, ids, slots, gates, h, norm_w, wq, wk, wv, wo):
    seq, d = h.shape
    dma = pltpu.SemaphoreType.DMA
    block = (GROUP, d)
    piece = 128

    def buf(*lead):
        return pltpu.VMEM(lead + block, jnp.bfloat16)

    return pl.pallas_call(
        stage_kernel,
        out_shape=pltpu.VMEM((seq, d), jnp.bfloat16),
        in_specs=[pl.BlockSpec(memory_space=pl.ANY)] * 10,
        out_specs=pl.BlockSpec(memory_space=pltpu.VMEM),
        scratch_shapes=[
            pltpu.VMEM((4, COLORS, 4, 4, GROUP, WIDE), jnp.bfloat16),
            pltpu.VMEM((2, 4, 4, COLORS, 4, GROUP, NARROW), jnp.bfloat16),
            buf(COLORS, 3, 4, 4),
            buf(COLORS, 4, 3, 4),
            buf(COLORS, 4, 4),
            buf(COLORS, 4, 4),
            buf(COLORS, 4, 4),
            pltpu.VMEM(ids.shape, jnp.int32),
            pltpu.VMEM(slots.shape, jnp.int32),
            pltpu.VMEM(gates.shape, jnp.float32),
            pltpu.VMEM((3 * seq, 64 * COLORS * GROUP), jnp.bfloat16),
            pltpu.VMEM((3 * seq, 64 * COLORS * GROUP), jnp.bfloat16),
            pltpu.VMEM((seq, d), jnp.float32),
            pltpu.VMEM(norm_w.shape, jnp.float32),
            pltpu.VMEM((3, d, d), jnp.bfloat16),
            pltpu.VMEM((d, d), jnp.bfloat16),
            pltpu.VMEM((3, piece) + wq.shape[1:], jnp.bfloat16),
            pltpu.VMEM((seq, d), jnp.bfloat16),
            pltpu.VMEM((3, seq, d), jnp.float32),
            pltpu.VMEM((3, seq, d), jnp.bfloat16),
            dma((2, 4)),
            dma((2,)),
            dma((3,)),
            dma((7, COLORS)),
            dma((COLORS, 5)),
            dma((COLORS, 4, 4)),
            dma((COLORS, 4)),
            dma((2, COLORS)),
            dma((4,)),
            dma((2, 4)),
        ],
        compiler_params=pltpu.CompilerParams(collective_id=0, has_side_effects=True, vmem_limit_bytes=63 * 1024 * 1024),
        name='stage',
    )(o_tab, ids, slots, gates, h, norm_w, wq, wk, wv, wo)


def solution(mesh):
    tok_spec = P('pp', 'ep', None, None)
    wt_spec = P('pp', None, None, None)

    def device_step(expert_out, expert_ids, slot_ids, gate_vals, residual, norm_w, w_query, w_key, w_value, w_out):
        seq_len, d_model = residual.shape[2:]

        def choices(array):
            return array.reshape(seq_len, array.shape[3]).T

        result = run_stage(
            expert_out.reshape(SIDE, SIDE, SIDE, COLORS, GROUP, d_model),
            choices(expert_ids), choices(slot_ids), choices(gate_vals),
            residual.reshape(seq_len, d_model), norm_w, w_query[0], w_key[0], w_value[0], w_out[0].reshape(-1, d_model),
        )
        return result.reshape(residual.shape)

    return jax.shard_map(device_step, mesh=mesh, in_specs=(tok_spec, tok_spec, tok_spec, tok_spec, tok_spec, P('pp', None), wt_spec, wt_spec, wt_spec, wt_spec), out_specs=tok_spec, check_vma=False)
```

```python
import jax
import jax.numpy as jnp
from jax import lax
from jax.experimental import pallas as pl
from jax.experimental.pallas import tpu as pltpu
from jax.sharding import PartitionSpec as P

NORM_EPS = 1e-6
MESH = pl.DeviceIdType.MESH
SIDE = 4
COLORS = 3
SLOTS = 24
ORDERS = ((2, 1, 0), (1, 0, 2), (0, 2, 1))
WIDTHS = (640, 640, 768)
STARTS = (0, 640, 1280)
COLS = [slice(at, at + w) for at, w in zip(STARTS, WIDTHS)]
SPANS = [pl.ds(at, w) for at, w in zip(STARTS, WIDTHS)]
HELD = 16 * SLOTS
LOW, HIGH = pl.ds(0, 64), pl.ds(64, 64)


def stage_kernel(o_ref, ids_ref, slots_ref, gates_ref, h_ref, norm_ref, wq_ref, wk_ref, wv_ref, wo_ref, z_ref, *scratch):
    held1, tie1, held2, tie2, mine = [scratch[3 * k:3 * k + 3] for k in range(5)]
    (sums, tin, got, ids_in, slots_in, gates_in, g_mat, norm_in, flat, wo_in, raw, x_in, qkv,
     kg_sem, side_sem, local_sem, mine_sem, raw_sem, send_sem, recv1, recv2, tin_sem, got_sem) = scratch[15:]
    stage = lax.axis_index('pp')
    me = lax.axis_index('ep')
    other = 1 - stage
    pos = (me // 16, (me // 4) % 4, me % 4)
    sign = [1 - 2 * (p % 2) for p in pos]
    to_a = [lax.rem(p + s + SIDE, SIDE) for p, s in zip(pos, sign)]
    to_b = [lax.rem(p - s + SIDE, SIDE) for p, s in zip(pos, sign)]
    far = [lax.rem(p + 2, SIDE) for p in pos]
    seq, d_model = x_in.shape
    depth, piece_rows = raw.shape[:2]
    pieces = flat.shape[1] // piece_rows

    def rank(axis, value):
        z, y, x = [value if k == axis else p for k, p in enumerate(pos)]
        return z * 16 + y * 4 + x

    near_a = [rank(k, to_a[k]) for k in range(3)]
    near_b = [rank(k, to_b[k]) for k in range(3)]
    remote = [rank(k, far[k]) for k in range(3)]

    barrier = pltpu.get_barrier_semaphore()
    peers = [(other, me)]
    for k in range(3):
        peers.append((stage, remote[k]))
        for where in (near_a[k], near_b[k]):
            peers += [(stage, where), (other, where)]
    for peer in peers:
        pl.semaphore_signal(barrier, inc=1, device_id=peer, device_id_type=MESH)
    pl.semaphore_wait(barrier, len(peers))

    def copy_to(src, dst, send_s, recv_s, peer):
        return pltpu.make_async_remote_copy(src_ref=src, dst_ref=dst, send_sem=send_s, recv_sem=recv_s, device_id=peer, device_id_type=MESH)

    def send(*args):
        copy_to(*args).start()

    def wait(ref, sem):
        pltpu.make_async_copy(ref, ref, sem).wait()

    def table(c, fixed):
        return o_ref.at[tuple(fixed.get(k, slice(None)) for k in range(3)) + (slice(None), SPANS[c])]

    def from_first(c, r1, fixed):
        d1 = ORDERS[c][0]
        if r1 == 0:
            return table(c, {d1: pos[d1], **fixed})
        return held1[c].at[(r1 - 1,) + tuple(fixed.get(k, slice(None)) for k in range(3) if k != d1)]

    def phase1():
        for c in range(COLORS):
            d = ORDERS[c][0]
            for half in range(2):
                some = pl.ds(2 * half, 2)
                send(table(c, {d: far[d], (d == 0) * 1: some}), tie1[c].at[some], send_sem.at[0, c], recv1.at[c, 4 * half], (stage, near_a[d]))
        for c in range(COLORS):
            d = ORDERS[c][0]
            send(table(c, {d: to_b[d]}), held1[c].at[2], send_sem.at[0, c], recv1.at[c, 3], (stage, near_b[d]))
        for c in range(COLORS):
            d = ORDERS[c][0]
            send(table(c, {d: to_a[d]}), held1[c].at[0], send_sem.at[0, c], recv1.at[c, 1], (stage, near_a[d]))

    def forward1(half):
        some = pl.ds(2 * half, 2)
        for c in range(COLORS):
            d = ORDERS[c][0]
            wait(tie1[c].at[some], recv1.at[c, 4 * half])
            send(tie1[c].at[some], held1[c].at[1, some], send_sem.at[3, c], recv1.at[c, 2], (stage, near_b[d]))

    def phase2(r1):
        for c in range(COLORS):
            d = ORDERS[c][1]
            if r1:
                wait(held1[c].at[r1 - 1], recv1.at[c, r1])
            send(from_first(c, r1, {d: to_b[d]}), held2[c].at[r1, 2], send_sem.at[1, c], recv2.at[c, r1, 3], (stage, near_b[d]))
            send(from_first(c, r1, {d: far[d]}), tie2[c].at[r1], send_sem.at[1, c], recv2.at[c, r1, 0], (stage, near_a[d]))
            send(from_first(c, r1, {d: to_a[d]}), held2[c].at[r1, 0], send_sem.at[1, c], recv2.at[c, r1, 1], (stage, near_a[d]))

    def forward2(r1):
        for c in range(COLORS):
            d = ORDERS[c][1]
            wait(tie2[c].at[r1], recv2.at[c, r1, 0])
            send(tie2[c].at[r1], held2[c].at[r1, 1], send_sem.at[4, c], recv2.at[c, r1, 2], (stage, near_b[d]))

    def partial(c, role):
        d1, d2, d = ORDERS[c]
        value = (pos, to_a, far, to_b)[role][d]
        kept = {d2: pos[d2], d: value}
        near = held1[c][(slice(None),) + tuple(kept[k] for k in range(3) if k != d1)]
        blocks = jnp.concatenate([held2[c][:, :, value].reshape(12 * SLOTS, -1), near.reshape(3 * SLOTS, -1), mine[c][value]], axis=0)
        part = jnp.dot(g_mat[c * 4 + role], blocks, preferred_element_type=jnp.float32)
        sums[role, :, COLS[c]] = part[:seq] + (part[seq:2 * seq] + part[2 * seq:])

    def send_sums(c, role):
        d = ORDERS[c][2]
        if role == 2:
            send(sums.at[2, LOW, SPANS[c]], tin.at[LOW, SPANS[c]], send_sem.at[2, c], tin_sem.at[c, 0], (stage, near_a[d]))
            send(sums.at[2, HIGH, SPANS[c]], tin.at[HIGH, SPANS[c]], send_sem.at[2, c], tin_sem.at[c, 1], (stage, near_b[d]))
        elif role == 3:
            send(sums.at[3, HIGH, SPANS[c]], got.at[2, HIGH, SPANS[c]], send_sem.at[2, c], got_sem.at[2, c], (other, near_b[d]))
        elif role == 1:
            send(sums.at[1, LOW, SPANS[c]], got.at[1, LOW, SPANS[c]], send_sem.at[2, c], got_sem.at[1, c], (other, near_a[d]))
        else:
            send(sums.at[0, :, SPANS[c]], got.at[0, :, SPANS[c]], send_sem.at[5, c], got_sem.at[0, c], (other, me))

    def merge(c, low):
        wait(tin.at[LOW if low else HIGH, SPANS[c]], tin_sem.at[c, 0 if low else 1])
        role, rows = (3, slice(0, 64)) if low else (1, slice(64, 128))
        sums[role, rows, COLS[c]] += tin[rows, COLS[c]]

    def send_merged(c, low):
        d = ORDERS[c][2]
        if low:
            send(sums.at[3, LOW, SPANS[c]], got.at[2, LOW, SPANS[c]], send_sem.at[2, c], got_sem.at[2, c], (other, near_b[d]))
        else:
            send(sums.at[1, HIGH, SPANS[c]], got.at[1, HIGH, SPANS[c]], send_sem.at[2, c], got_sem.at[1, c], (other, near_a[d]))

    choices = ((ids_ref, ids_in), (slots_ref, slots_in), (gates_ref, gates_in))

    def send_choices():
        for k, (src, dst) in enumerate(choices):
            pltpu.make_async_copy(src, dst.at[9], local_sem.at[2 + k]).start()
            for axis in range(3):
                for role, peer in ((1, near_a[axis]), (2, remote[axis]), (3, near_b[axis])):
                    send(src, dst.at[axis * 3 + role - 1], kg_sem.at[0, k], kg_sem.at[1, k], (stage, peer))

    side = copy_to(h_ref, x_in, side_sem.at[0], side_sem.at[1], (other, me))
    local = [pltpu.make_async_copy(src, dst, local_sem.at[k]) for k, (src, dst) in enumerate(((norm_ref, norm_in), (wo_ref, wo_in)))]
    own = [pltpu.make_async_copy(table(c, {ORDERS[c][0]: pos[ORDERS[c][0]], ORDERS[c][1]: pos[ORDERS[c][1]]}), mine[c], mine_sem.at[c]) for c in range(COLORS)]

    def build_gates():
        for k, (src, dst) in enumerate(choices):
            pltpu.make_async_copy(src, dst.at[9], local_sem.at[2 + k]).wait()
            wait(dst.at[pl.ds(0, 9)], kg_sem.at[1, k])
        columns = []
        for c in range(COLORS):
            d1, d2, d = ORDERS[c]
            for role in range(4):
                value = (pos, to_a, far, to_b)[role][d]
                which = 9 if role == 0 else d * 3 + role - 1
                ids, slot = ids_in[which], slots_in[which]
                at = [(ids >> shift) & 3 for shift in (4, 2, 0)]
                first, second = [(sign[k] * (at[k] - pos[k])) & 3 for k in (d1, d2)]
                block = jnp.where(second > 0, first * 3 + second - 1, jnp.where(first > 0, 11 + first, 15))
                column = block * SLOTS + slot - rank(d, value) * SLOTS
                columns.append(jnp.where((slot >= 0) & (at[d] == pos[d]), column, -1).astype(jnp.float32))
        places = jnp.concatenate(columns + [jnp.zeros((32, seq), jnp.float32)], axis=0).T
        gates = jnp.concatenate([gates_in[k] for k in range(10)] + [jnp.zeros((48, seq), jnp.float32)], axis=0).T
        step = 128
        for c in range(COLORS):
            for role in range(4):
                g = 8 * (9 if role == 0 else ORDERS[c][2] * 3 + role - 1)
                p = 8 * (c * 4 + role)
                for b in range(0, HELD, step):
                    col = (lax.broadcasted_iota(jnp.int32, (seq, step), 1) + b).astype(jnp.float32)
                    val = jnp.zeros((seq, step), jnp.float32)
                    for i in range(8):
                        val = jnp.where(places[:, p + i:p + i + 1] == col, gates[:, g + i:g + i + 1], val)
                    high = val.astype(jnp.bfloat16)
                    rest = val - high.astype(jnp.float32)
                    mid = rest.astype(jnp.bfloat16)
                    low = (rest - mid.astype(jnp.float32)).astype(jnp.bfloat16)
                    for k, piece in enumerate((high, mid, low)):
                        g_mat[c * 4 + role, k * seq:(k + 1) * seq, b:b + step] = piece

    weights = (wq_ref, wk_ref, wv_ref)

    def load(k, i):
        slot = lax.rem(i, depth)
        return pltpu.make_async_copy(weights[k].at[pl.ds(pl.multiple_of(i * piece_rows, piece_rows), piece_rows)], raw.at[slot], raw_sem.at[slot])

    def flatten(k, start, stop):
        step = 64

        def body(i, carry):
            load(k, i).wait()
            for j in range(0, piece_rows, step):
                flat[k, pl.ds(pl.multiple_of(i * piece_rows + j, step), step), :] = raw[lax.rem(i, depth), pl.ds(j, step)].reshape(step, d_model)

            @pl.when(i + depth < pieces)
            def _():
                load(k, i + depth).start()

            return carry

        if start == 0:
            for i in range(depth):
                load(k, i).start()
        lax.fori_loop(start, stop, body, 0)

    head = 128
    pair = 2 * head
    causal = lax.broadcasted_iota(jnp.int32, (seq, seq), 0) >= lax.broadcasted_iota(jnp.int32, (seq, seq), 1)

    def norm():
        side.wait_recv()
        total = jnp.zeros((seq, 1), jnp.float32)
        for c in range(COLORS):
            for slot in range(3):
                wait(got.at[slot, :, SPANS[c]], got_sem.at[slot, c])
        for cols in spans(0, d_model):
            y = x_in[:, cols].astype(jnp.float32) + (got[0, :, cols] + (got[1, :, cols] + got[2, :, cols]))
            y = y.astype(jnp.bfloat16).astype(jnp.float32)
            got[0, :, cols] = y
            total += jnp.sum(y * y, axis=1, keepdims=True)
        inv = lax.rsqrt(total * (1.0 / d_model) + NORM_EPS)
        for cols in spans(0, d_model):
            x_in[:, cols] = (got[0, :, cols] * inv * norm_in[:, cols]).astype(jnp.bfloat16)

    def project(k, p):
        cols = slice(p * pair, (p + 1) * pair)
        qkv[k, :, cols] = jnp.dot(x_in[...], flat[k, :, cols], preferred_element_type=jnp.float32).astype(jnp.bfloat16)

    def softmax(cols):
        scores = jnp.where(causal, tin[:, cols] * (head ** -0.5), -jnp.inf)
        grown = jnp.exp(scores - jnp.max(scores, axis=1, keepdims=True))
        qkv[0, :, cols] = (grown * (1.0 / jnp.sum(grown, axis=1, keepdims=True))).astype(jnp.bfloat16)

    def attend():
        heads = [slice(h * head, (h + 1) * head) for h in range(d_model // head)]
        for k in range(2):
            for p in range(d_model // pair):
                project(k, p)
        for cols in heads:
            tin[:, cols] = lax.dot_general(qkv[0, :, cols], qkv[1, :, cols], (((1,), (1,)), ((), ())), preferred_element_type=jnp.float32)
        for p in range(d_model // pair):
            softmax(heads[2 * p])
            softmax(heads[2 * p + 1])
            project(2, p)
        for cols in heads:
            x_in[:, cols] = jnp.dot(qkv[0, :, cols], qkv[2, :, cols], preferred_element_type=jnp.float32).astype(jnp.bfloat16)

    phase1()
    send_choices()
    side.start()
    phase2(0)
    for copy in local + own:
        copy.start()
    build_gates()
    flatten(0, 0, pieces // 4)
    forward1(0)
    flatten(0, pieces // 4, pieces)
    forward1(1)
    phase2(3)
    flatten(1, 0, pieces)
    forward2(0)
    phase2(1)
    flatten(2, 0, pieces // 2)
    forward2(3)
    phase2(2)
    flatten(2, pieces // 2, pieces)
    forward2(1)
    for copy in own:
        copy.wait()
    forward2(2)
    for c in range(COLORS):
        for r1 in range(4):
            for r2 in (1, 2, 3):
                wait(held2[c].at[r1, r2 - 1], recv2.at[c, r1, r2])
    before = None
    for role in (2, 3, 1, 0):
        for c in range(COLORS):
            partial(c, role)
            if before is not None:
                send_sums(*before)
            before = (c, role)
    send_sums(*before)
    before = None
    for low in (True, False):
        for c in range(COLORS):
            merge(c, low)
            if before is not None:
                send_merged(*before)
            before = (c, low)
    for copy in local:
        copy.wait()
    send_merged(*before)
    norm()
    attend()
    for p in range(d_model // pair):
        cols = slice(p * pair, (p + 1) * pair)
        out = jnp.dot(x_in[...], wo_in[:, cols], preferred_element_type=jnp.float32).astype(jnp.bfloat16)
        z_ref[:, cols] = (got[0, :, cols] + out.astype(jnp.float32)).astype(jnp.bfloat16)

    side.wait_send()
    for k, (src, dst) in enumerate(choices):
        wait(dst.at[pl.ds(0, 9)], kg_sem.at[0, k])
    for c in range(COLORS):
        wait(held1[c], send_sem.at[0, c])
        wait(held2[c], send_sem.at[1, c])
        wait(sums.at[pl.ds(1, 3), :, SPANS[c]], send_sem.at[2, c])
        wait(tie1[c], send_sem.at[3, c])
        wait(tie2[c], send_sem.at[4, c])
        wait(sums.at[0, :, SPANS[c]], send_sem.at[5, c])


def spans(lo, hi):
    return [slice(b, min(b + 512, hi)) for b in range(lo, hi, 512)]


def run_stage(o_tab, ids, slots, gates, h, norm_w, wq, wk, wv, wo):
    seq, d = h.shape
    dma = pltpu.SemaphoreType.DMA
    piece = 128

    def per_colour(*lead):
        return [pltpu.VMEM(lead + (SLOTS, w), jnp.bfloat16) for w in WIDTHS]

    return pl.pallas_call(
        stage_kernel,
        out_shape=pltpu.VMEM((seq, d), jnp.bfloat16),
        in_specs=[pl.BlockSpec(memory_space=pl.ANY)] * 10,
        out_specs=pl.BlockSpec(memory_space=pltpu.VMEM),
        scratch_shapes=[
            *per_colour(3, 4, 4),
            *per_colour(4, 4),
            *per_colour(4, 3, 4),
            *per_colour(4, 4),
            *per_colour(4),
            pltpu.VMEM((4, seq, d), jnp.float32),
            pltpu.VMEM((seq, d), jnp.float32),
            pltpu.VMEM((3, seq, d), jnp.float32),
            pltpu.VMEM((10,) + ids.shape, jnp.int32),
            pltpu.VMEM((10,) + slots.shape, jnp.int32),
            pltpu.VMEM((10,) + gates.shape, jnp.float32),
            pltpu.VMEM((4 * COLORS, 3 * seq, HELD), jnp.bfloat16),
            pltpu.VMEM(norm_w.shape, jnp.float32),
            pltpu.VMEM((3, d, d), jnp.bfloat16),
            pltpu.VMEM((d, d), jnp.bfloat16),
            pltpu.VMEM((3, piece) + wq.shape[1:], jnp.bfloat16),
            pltpu.VMEM((seq, d), jnp.bfloat16),
            pltpu.VMEM((3, seq, d), jnp.bfloat16),
            dma((2, 3)),
            dma((2,)),
            dma((5,)),
            dma((COLORS,)),
            dma((3,)),
            dma((6, COLORS)),
            dma((COLORS, 5)),
            dma((COLORS, 4, 4)),
            dma((COLORS, 2)),
            dma((3, COLORS)),
        ],
        compiler_params=pltpu.CompilerParams(collective_id=0, has_side_effects=True, vmem_limit_bytes=66400000),
        name='stage',
    )(o_tab, ids, slots, gates, h, norm_w, wq, wk, wv, wo)


def solution(mesh):
    tok_spec = P('pp', 'ep', None, None)
    wt_spec = P('pp', None, None, None)

    def device_step(expert_out, expert_ids, slot_ids, gate_vals, residual, norm_w, w_query, w_key, w_value, w_out):
        seq_len, d_model = residual.shape[2:]

        def choices(array):
            return array.reshape(seq_len, array.shape[3]).T

        result = run_stage(
            expert_out.reshape(SIDE, SIDE, SIDE, SLOTS, d_model),
            choices(expert_ids), choices(slot_ids), choices(gate_vals),
            residual.reshape(seq_len, d_model), norm_w, w_query[0], w_key[0], w_value[0], w_out[0].reshape(-1, d_model),
        )
        return result.reshape(residual.shape)

    return jax.shard_map(device_step, mesh=mesh, in_specs=(tok_spec, tok_spec, tok_spec, tok_spec, tok_spec, P('pp', None), wt_spec, wt_spec, wt_spec, wt_spec), out_specs=tok_spec, check_vma=False)
```

```python
import jax
import jax.numpy as jnp
from jax import lax
from jax.experimental import pallas as pl
from jax.experimental.pallas import tpu as pltpu
from jax.sharding import PartitionSpec as P

NORM_EPS = 1e-6
MESH = pl.DeviceIdType.MESH
SIDE = 4
COLORS = 3
SLOTS = 24
ORDERS = ((2, 1, 0), (1, 0, 2), (0, 2, 1))
WIDTHS = (640, 640, 768)
STARTS = (0, 640, 1280)
COLS = [slice(at, at + w) for at, w in zip(STARTS, WIDTHS)]
SPANS = [pl.ds(at, w) for at, w in zip(STARTS, WIDTHS)]
HELD = 16 * SLOTS
LOW, HIGH = pl.ds(0, 64), pl.ds(64, 64)


def stage_kernel(o_ref, ids_ref, slots_ref, gates_ref, h_ref, norm_ref, wq_ref, wk_ref, wv_ref, wo_ref, z_ref, *scratch):
    held1, tie1, held2, tie2, mine = [scratch[3 * k:3 * k + 3] for k in range(5)]
    (sums, tin, got, ids_in, slots_in, gates_in, g_mat, norm_in, flat, wo_in, raw, x_in, qkv,
     kg_sem, side_sem, local_sem, mine_sem, raw_sem, send_sem, recv1, recv2, tin_sem, got_sem) = scratch[15:]
    stage = lax.axis_index('pp')
    me = lax.axis_index('ep')
    other = 1 - stage
    pos = (me // 16, (me // 4) % 4, me % 4)
    sign = [1 - 2 * (p % 2) for p in pos]
    to_a = [lax.rem(p + s + SIDE, SIDE) for p, s in zip(pos, sign)]
    to_b = [lax.rem(p - s + SIDE, SIDE) for p, s in zip(pos, sign)]
    far = [lax.rem(p + 2, SIDE) for p in pos]
    seq, d_model = x_in.shape
    depth, piece_rows = raw.shape[:2]
    pieces = flat.shape[1] // piece_rows

    def rank(axis, value):
        z, y, x = [value if k == axis else p for k, p in enumerate(pos)]
        return z * 16 + y * 4 + x

    near_a = [rank(k, to_a[k]) for k in range(3)]
    near_b = [rank(k, to_b[k]) for k in range(3)]
    remote = [rank(k, far[k]) for k in range(3)]

    barrier = pltpu.get_barrier_semaphore()
    peers = [(other, me)]
    for k in range(3):
        peers.append((stage, remote[k]))
        for where in (near_a[k], near_b[k]):
            peers += [(stage, where), (other, where)]
    for peer in peers:
        pl.semaphore_signal(barrier, inc=1, device_id=peer, device_id_type=MESH)
    pl.semaphore_wait(barrier, len(peers))

    def copy_to(src, dst, send_s, recv_s, peer):
        return pltpu.make_async_remote_copy(src_ref=src, dst_ref=dst, send_sem=send_s, recv_sem=recv_s, device_id=peer, device_id_type=MESH)

    def send(*args):
        copy_to(*args).start()

    def wait(ref, sem):
        pltpu.make_async_copy(ref, ref, sem).wait()

    def table(c, fixed):
        return o_ref.at[tuple(fixed.get(k, slice(None)) for k in range(3)) + (slice(None), SPANS[c])]

    def from_first(c, r1, fixed):
        d1 = ORDERS[c][0]
        if r1 == 0:
            return table(c, {d1: pos[d1], **fixed})
        return held1[c].at[(r1 - 1,) + tuple(fixed.get(k, slice(None)) for k in range(3) if k != d1)]

    def phase1():
        for c in range(COLORS):
            d = ORDERS[c][0]
            for half in range(2):
                some = pl.ds(2 * half, 2)
                send(table(c, {d: far[d], (d == 0) * 1: some}), tie1[c].at[some], send_sem.at[0, c], recv1.at[c, 4 * half], (stage, near_a[d]))
        for c in range(COLORS):
            d = ORDERS[c][0]
            send(table(c, {d: to_b[d]}), held1[c].at[2], send_sem.at[0, c], recv1.at[c, 3], (stage, near_b[d]))
        for c in range(COLORS):
            d = ORDERS[c][0]
            send(table(c, {d: to_a[d]}), held1[c].at[0], send_sem.at[0, c], recv1.at[c, 1], (stage, near_a[d]))

    def forward1(half):
        some = pl.ds(2 * half, 2)
        for c in range(COLORS):
            d = ORDERS[c][0]
            wait(tie1[c].at[some], recv1.at[c, 4 * half])
            send(tie1[c].at[some], held1[c].at[1, some], send_sem.at[3, c], recv1.at[c, 2], (stage, near_b[d]))

    def phase2(r1):
        for c in range(COLORS):
            d = ORDERS[c][1]
            if r1:
                wait(held1[c].at[r1 - 1], recv1.at[c, r1])
            send(from_first(c, r1, {d: to_b[d]}), held2[c].at[r1, 2], send_sem.at[1, c], recv2.at[c, r1, 3], (stage, near_b[d]))
            send(from_first(c, r1, {d: far[d]}), tie2[c].at[r1], send_sem.at[1, c], recv2.at[c, r1, 0], (stage, near_a[d]))
            send(from_first(c, r1, {d: to_a[d]}), held2[c].at[r1, 0], send_sem.at[1, c], recv2.at[c, r1, 1], (stage, near_a[d]))

    def forward2(r1):
        for c in range(COLORS):
            d = ORDERS[c][1]
            wait(tie2[c].at[r1], recv2.at[c, r1, 0])
            send(tie2[c].at[r1], held2[c].at[r1, 1], send_sem.at[4, c], recv2.at[c, r1, 2], (stage, near_b[d]))

    def partial(c, role):
        d1, d2, d = ORDERS[c]
        value = (pos, to_a, far, to_b)[role][d]
        kept = {d2: pos[d2], d: value}
        near = held1[c][(slice(None),) + tuple(kept[k] for k in range(3) if k != d1)]
        blocks = jnp.concatenate([held2[c][:, :, value].reshape(12 * SLOTS, -1), near.reshape(3 * SLOTS, -1), mine[c][value]], axis=0)
        part = jnp.dot(g_mat[c * 4 + role], blocks, preferred_element_type=jnp.float32)
        sums[role, :, COLS[c]] = part[:seq] + (part[seq:2 * seq] + part[2 * seq:])

    def send_sums(c, role):
        d = ORDERS[c][2]
        if role == 2:
            send(sums.at[2, LOW, SPANS[c]], tin.at[LOW, SPANS[c]], send_sem.at[2, c], tin_sem.at[c, 0], (stage, near_a[d]))
            send(sums.at[2, HIGH, SPANS[c]], tin.at[HIGH, SPANS[c]], send_sem.at[2, c], tin_sem.at[c, 1], (stage, near_b[d]))
        elif role == 3:
            send(sums.at[3, HIGH, SPANS[c]], got.at[2, HIGH, SPANS[c]], send_sem.at[2, c], got_sem.at[2, c], (other, near_b[d]))
        elif role == 1:
            send(sums.at[1, LOW, SPANS[c]], got.at[1, LOW, SPANS[c]], send_sem.at[2, c], got_sem.at[1, c], (other, near_a[d]))
        else:
            send(sums.at[0, :, SPANS[c]], got.at[0, :, SPANS[c]], send_sem.at[5, c], got_sem.at[0, c], (other, me))

    def merge(c, low):
        wait(tin.at[LOW if low else HIGH, SPANS[c]], tin_sem.at[c, 0 if low else 1])
        role, rows = (3, slice(0, 64)) if low else (1, slice(64, 128))
        sums[role, rows, COLS[c]] += tin[rows, COLS[c]]

    def send_merged(c, low):
        d = ORDERS[c][2]
        if low:
            send(sums.at[3, LOW, SPANS[c]], got.at[2, LOW, SPANS[c]], send_sem.at[2, c], got_sem.at[2, c], (other, near_b[d]))
        else:
            send(sums.at[1, HIGH, SPANS[c]], got.at[1, HIGH, SPANS[c]], send_sem.at[2, c], got_sem.at[1, c], (other, near_a[d]))

    choices = ((ids_ref, ids_in), (slots_ref, slots_in), (gates_ref, gates_in))

    def send_choices():
        for k, (src, dst) in enumerate(choices):
            pltpu.make_async_copy(src, dst.at[9], local_sem.at[2 + k]).start()
            for axis in range(3):
                for role, peer in ((1, near_a[axis]), (2, remote[axis]), (3, near_b[axis])):
                    send(src, dst.at[axis * 3 + role - 1], kg_sem.at[0, k], kg_sem.at[1, k], (stage, peer))

    side = copy_to(h_ref, x_in, side_sem.at[0], side_sem.at[1], (other, me))
    local = [pltpu.make_async_copy(src, dst, local_sem.at[k]) for k, (src, dst) in enumerate(((norm_ref, norm_in), (wo_ref, wo_in)))]
    own = [pltpu.make_async_copy(table(c, {ORDERS[c][0]: pos[ORDERS[c][0]], ORDERS[c][1]: pos[ORDERS[c][1]]}), mine[c], mine_sem.at[c]) for c in range(COLORS)]

    def build_gates():
        for k, (src, dst) in enumerate(choices):
            pltpu.make_async_copy(src, dst.at[9], local_sem.at[2 + k]).wait()
            wait(dst.at[pl.ds(0, 9)], kg_sem.at[1, k])
        columns = []
        for c in range(COLORS):
            d1, d2, d = ORDERS[c]
            for role in range(4):
                value = (pos, to_a, far, to_b)[role][d]
                which = 9 if role == 0 else d * 3 + role - 1
                ids, slot = ids_in[which], slots_in[which]
                at = [(ids >> shift) & 3 for shift in (4, 2, 0)]
                first, second = [(sign[k] * (at[k] - pos[k])) & 3 for k in (d1, d2)]
                block = jnp.where(second > 0, first * 3 + second - 1, jnp.where(first > 0, 11 + first, 15))
                column = block * SLOTS + slot - rank(d, value) * SLOTS
                columns.append(jnp.where((slot >= 0) & (at[d] == pos[d]), column, -1).astype(jnp.float32))
        places = jnp.concatenate(columns + [jnp.zeros((32, seq), jnp.float32)], axis=0).T
        gates = jnp.concatenate([gates_in[k] for k in range(10)] + [jnp.zeros((48, seq), jnp.float32)], axis=0).T
        step = 128
        for c in range(COLORS):
            for role in range(4):
                g = 8 * (9 if role == 0 else ORDERS[c][2] * 3 + role - 1)
                p = 8 * (c * 4 + role)
                for b in range(0, HELD, step):
                    col = (lax.broadcasted_iota(jnp.int32, (seq, step), 1) + b).astype(jnp.float32)
                    val = jnp.zeros((seq, step), jnp.float32)
                    for i in range(8):
                        val = jnp.where(places[:, p + i:p + i + 1] == col, gates[:, g + i:g + i + 1], val)
                    high = val.astype(jnp.bfloat16)
                    rest = val - high.astype(jnp.float32)
                    mid = rest.astype(jnp.bfloat16)
                    low = (rest - mid.astype(jnp.float32)).astype(jnp.bfloat16)
                    for k, piece in enumerate((high, mid, low)):
                        g_mat[c * 4 + role, k * seq:(k + 1) * seq, b:b + step] = piece

    weights = (wq_ref, wk_ref, wv_ref)

    def load(k, i):
        slot = lax.rem(i, depth)
        return pltpu.make_async_copy(weights[k].at[pl.ds(pl.multiple_of(i * piece_rows, piece_rows), piece_rows)], raw.at[slot], raw_sem.at[slot])

    def flatten(k, start, stop):
        step = 64

        def body(i, carry):
            load(k, i).wait()
            for j in range(0, piece_rows, step):
                flat[k, pl.ds(pl.multiple_of(i * piece_rows + j, step), step), :] = raw[lax.rem(i, depth), pl.ds(j, step)].reshape(step, d_model)

            @pl.when(i + depth < pieces)
            def _():
                load(k, i + depth).start()

            return carry

        if start == 0:
            for i in range(depth):
                load(k, i).start()
        lax.fori_loop(start, stop, body, 0)

    head = 128
    pair = 2 * head
    causal = lax.broadcasted_iota(jnp.int32, (seq, seq), 0) >= lax.broadcasted_iota(jnp.int32, (seq, seq), 1)

    def norm():
        side.wait_recv()
        total = jnp.zeros((seq, 1), jnp.float32)
        for c in range(COLORS):
            for slot in range(3):
                wait(got.at[slot, :, SPANS[c]], got_sem.at[slot, c])
        for cols in spans(0, d_model):
            y = x_in[:, cols].astype(jnp.float32) + (got[0, :, cols] + (got[1, :, cols] + got[2, :, cols]))
            y = y.astype(jnp.bfloat16).astype(jnp.float32)
            got[0, :, cols] = y
            total += jnp.sum(y * y, axis=1, keepdims=True)
        inv = lax.rsqrt(total * (1.0 / d_model) + NORM_EPS)
        for cols in spans(0, d_model):
            x_in[:, cols] = (got[0, :, cols] * inv * norm_in[:, cols]).astype(jnp.bfloat16)

    def project(k, p):
        cols = slice(p * pair, (p + 1) * pair)
        qkv[k, :, cols] = jnp.dot(x_in[...], flat[k, :, cols], preferred_element_type=jnp.float32).astype(jnp.bfloat16)

    def softmax(cols):
        scores = jnp.where(causal, tin[:, cols] * (head ** -0.5), -jnp.inf)
        grown = jnp.exp(scores - jnp.max(scores, axis=1, keepdims=True))
        qkv[0, :, cols] = (grown * (1.0 / jnp.sum(grown, axis=1, keepdims=True))).astype(jnp.bfloat16)

    def attend():
        heads = [slice(h * head, (h + 1) * head) for h in range(d_model // head)]
        for k in range(2):
            for p in range(d_model // pair):
                project(k, p)
        for cols in heads:
            tin[:, cols] = lax.dot_general(qkv[0, :, cols], qkv[1, :, cols], (((1,), (1,)), ((), ())), preferred_element_type=jnp.float32)
        for p in range(d_model // pair):
            softmax(heads[2 * p])
            softmax(heads[2 * p + 1])
            project(2, p)
        for cols in heads:
            x_in[:, cols] = jnp.dot(qkv[0, :, cols], qkv[2, :, cols], preferred_element_type=jnp.float32).astype(jnp.bfloat16)

    send_choices()
    phase1()
    side.start()
    phase2(0)
    for copy in local + own:
        copy.start()
    build_gates()
    flatten(0, 0, pieces // 4)
    forward1(0)
    flatten(0, pieces // 4, pieces)
    forward1(1)
    phase2(3)
    flatten(1, 0, pieces)
    forward2(0)
    phase2(1)
    flatten(2, 0, pieces // 2)
    forward2(3)
    phase2(2)
    flatten(2, pieces // 2, pieces)
    forward2(1)
    for copy in own:
        copy.wait()
    forward2(2)
    for c in range(COLORS):
        for r1 in range(4):
            for r2 in (1, 2, 3):
                wait(held2[c].at[r1, r2 - 1], recv2.at[c, r1, r2])
    before = None
    for role in (2, 3, 1, 0):
        for c in range(COLORS):
            partial(c, role)
            if before is not None:
                send_sums(*before)
            before = (c, role)
    send_sums(*before)
    before = None
    for low in (True, False):
        for c in range(COLORS):
            merge(c, low)
            if before is not None:
                send_merged(*before)
            before = (c, low)
    for copy in local:
        copy.wait()
    send_merged(*before)
    norm()
    attend()
    for p in range(d_model // pair):
        cols = slice(p * pair, (p + 1) * pair)
        out = jnp.dot(x_in[...], wo_in[:, cols], preferred_element_type=jnp.float32).astype(jnp.bfloat16)
        z_ref[:, cols] = (got[0, :, cols] + out.astype(jnp.float32)).astype(jnp.bfloat16)

    side.wait_send()
    for k, (src, dst) in enumerate(choices):
        wait(dst.at[pl.ds(0, 9)], kg_sem.at[0, k])
    for c in range(COLORS):
        wait(held1[c], send_sem.at[0, c])
        wait(held2[c], send_sem.at[1, c])
        wait(sums.at[pl.ds(1, 3), :, SPANS[c]], send_sem.at[2, c])
        wait(tie1[c], send_sem.at[3, c])
        wait(tie2[c], send_sem.at[4, c])
        wait(sums.at[0, :, SPANS[c]], send_sem.at[5, c])


def spans(lo, hi):
    return [slice(b, min(b + 512, hi)) for b in range(lo, hi, 512)]


def run_stage(o_tab, ids, slots, gates, h, norm_w, wq, wk, wv, wo):
    seq, d = h.shape
    dma = pltpu.SemaphoreType.DMA
    piece = 128

    def per_colour(*lead):
        return [pltpu.VMEM(lead + (SLOTS, w), jnp.bfloat16) for w in WIDTHS]

    return pl.pallas_call(
        stage_kernel,
        out_shape=pltpu.VMEM((seq, d), jnp.bfloat16),
        in_specs=[pl.BlockSpec(memory_space=pl.ANY)] * 10,
        out_specs=pl.BlockSpec(memory_space=pltpu.VMEM),
        scratch_shapes=[
            *per_colour(3, 4, 4),
            *per_colour(4, 4),
            *per_colour(4, 3, 4),
            *per_colour(4, 4),
            *per_colour(4),
            pltpu.VMEM((4, seq, d), jnp.float32),
            pltpu.VMEM((seq, d), jnp.float32),
            pltpu.VMEM((3, seq, d), jnp.float32),
            pltpu.VMEM((10,) + ids.shape, jnp.int32),
            pltpu.VMEM((10,) + slots.shape, jnp.int32),
            pltpu.VMEM((10,) + gates.shape, jnp.float32),
            pltpu.VMEM((4 * COLORS, 3 * seq, HELD), jnp.bfloat16),
            pltpu.VMEM(norm_w.shape, jnp.float32),
            pltpu.VMEM((3, d, d), jnp.bfloat16),
            pltpu.VMEM((d, d), jnp.bfloat16),
            pltpu.VMEM((3, piece) + wq.shape[1:], jnp.bfloat16),
            pltpu.VMEM((seq, d), jnp.bfloat16),
            pltpu.VMEM((3, seq, d), jnp.bfloat16),
            dma((2, 3)),
            dma((2,)),
            dma((5,)),
            dma((COLORS,)),
            dma((3,)),
            dma((6, COLORS)),
            dma((COLORS, 5)),
            dma((COLORS, 4, 4)),
            dma((COLORS, 2)),
            dma((3, COLORS)),
        ],
        compiler_params=pltpu.CompilerParams(collective_id=0, has_side_effects=True, vmem_limit_bytes=66400000),
        name='stage',
    )(o_tab, ids, slots, gates, h, norm_w, wq, wk, wv, wo)


def solution(mesh):
    tok_spec = P('pp', 'ep', None, None)
    wt_spec = P('pp', None, None, None)

    def device_step(expert_out, expert_ids, slot_ids, gate_vals, residual, norm_w, w_query, w_key, w_value, w_out):
        seq_len, d_model = residual.shape[2:]

        def choices(array):
            return array.reshape(seq_len, array.shape[3]).T

        result = run_stage(
            expert_out.reshape(SIDE, SIDE, SIDE, SLOTS, d_model),
            choices(expert_ids), choices(slot_ids), choices(gate_vals),
            residual.reshape(seq_len, d_model), norm_w, w_query[0], w_key[0], w_value[0], w_out[0].reshape(-1, d_model),
        )
        return result.reshape(residual.shape)

    return jax.shard_map(device_step, mesh=mesh, in_specs=(tok_spec, tok_spec, tok_spec, tok_spec, tok_spec, P('pp', None), wt_spec, wt_spec, wt_spec, wt_spec), out_specs=tok_spec, check_vma=False)
```

```python
import jax
import jax.numpy as jnp
from jax import lax
from jax.experimental import pallas as pl
from jax.experimental.pallas import tpu as pltpu
from jax.sharding import PartitionSpec as P

NORM_EPS = 1e-6
MESH = pl.DeviceIdType.MESH
SIDE = 4
COLORS = 3
SLOTS = 24
ORDERS = ((2, 1, 0), (1, 0, 2), (0, 2, 1))
WIDTHS = (640, 640, 768)
STARTS = (0, 640, 1280)
COLS = [slice(at, at + w) for at, w in zip(STARTS, WIDTHS)]
SPANS = [pl.ds(at, w) for at, w in zip(STARTS, WIDTHS)]
HELD = 16 * SLOTS
LOW, HIGH = pl.ds(0, 64), pl.ds(64, 64)


def stage_kernel(o_ref, ids_ref, slots_ref, gates_ref, h_ref, norm_ref, wq_ref, wk_ref, wv_ref, wo_ref, z_ref, *scratch):
    held1, tie1, held2, tie2, mine = [scratch[3 * k:3 * k + 3] for k in range(5)]
    (sums, tin, got, ids_in, slots_in, gates_in, g_mat, norm_in, flat, wo_in, raw, x_in, qkv,
     kg_sem, side_sem, local_sem, mine_sem, raw_sem, send_sem, recv1, recv2, tin_sem, got_sem) = scratch[15:]
    stage = lax.axis_index('pp')
    me = lax.axis_index('ep')
    other = 1 - stage
    pos = (me // 16, (me // 4) % 4, me % 4)
    sign = [1 - 2 * (p % 2) for p in pos]
    to_a = [lax.rem(p + s + SIDE, SIDE) for p, s in zip(pos, sign)]
    to_b = [lax.rem(p - s + SIDE, SIDE) for p, s in zip(pos, sign)]
    far = [lax.rem(p + 2, SIDE) for p in pos]
    seq, d_model = x_in.shape
    depth, piece_rows = raw.shape[:2]
    pieces = flat.shape[1] // piece_rows

    def rank(axis, value):
        z, y, x = [value if k == axis else p for k, p in enumerate(pos)]
        return z * 16 + y * 4 + x

    near_a = [rank(k, to_a[k]) for k in range(3)]
    near_b = [rank(k, to_b[k]) for k in range(3)]
    remote = [rank(k, far[k]) for k in range(3)]

    barrier = pltpu.get_barrier_semaphore()
    peers = [(other, me)]
    for k in range(3):
        peers.append((stage, remote[k]))
        for where in (near_a[k], near_b[k]):
            peers += [(stage, where), (other, where)]
    for peer in peers:
        pl.semaphore_signal(barrier, inc=1, device_id=peer, device_id_type=MESH)
    pl.semaphore_wait(barrier, len(peers))

    def copy_to(src, dst, send_s, recv_s, peer):
        return pltpu.make_async_remote_copy(src_ref=src, dst_ref=dst, send_sem=send_s, recv_sem=recv_s, device_id=peer, device_id_type=MESH)

    def send(*args):
        copy_to(*args).start()

    def wait(ref, sem):
        pltpu.make_async_copy(ref, ref, sem).wait()

    def table(c, fixed):
        return o_ref.at[tuple(fixed.get(k, slice(None)) for k in range(3)) + (slice(None), SPANS[c])]

    def from_first(c, r1, fixed):
        d1 = ORDERS[c][0]
        if r1 == 0:
            return table(c, {d1: pos[d1], **fixed})
        return held1[c].at[(r1 - 1,) + tuple(fixed.get(k, slice(None)) for k in range(3) if k != d1)]

    def phase1():
        for c in range(COLORS):
            d = ORDERS[c][0]
            for half in range(2):
                some = pl.ds(2 * half, 2)
                send(table(c, {d: far[d], (d == 0) * 1: some}), tie1[c].at[some], send_sem.at[0, c], recv1.at[c, 4 * half], (stage, near_a[d]))
        for c in range(COLORS):
            d = ORDERS[c][0]
            send(table(c, {d: to_b[d]}), held1[c].at[2], send_sem.at[0, c], recv1.at[c, 3], (stage, near_b[d]))
        for c in range(COLORS):
            d = ORDERS[c][0]
            send(table(c, {d: to_a[d]}), held1[c].at[0], send_sem.at[0, c], recv1.at[c, 1], (stage, near_a[d]))

    def forward1(half):
        some = pl.ds(2 * half, 2)
        for c in range(COLORS):
            d = ORDERS[c][0]
            wait(tie1[c].at[some], recv1.at[c, 4 * half])
            send(tie1[c].at[some], held1[c].at[1, some], send_sem.at[3, c], recv1.at[c, 2], (stage, near_b[d]))

    def phase2(r1):
        for c in range(COLORS):
            d = ORDERS[c][1]
            if r1:
                wait(held1[c].at[r1 - 1], recv1.at[c, r1])
            send(from_first(c, r1, {d: to_b[d]}), held2[c].at[r1, 2], send_sem.at[1, c], recv2.at[c, r1, 3], (stage, near_b[d]))
            send(from_first(c, r1, {d: far[d]}), tie2[c].at[r1], send_sem.at[1, c], recv2.at[c, r1, 0], (stage, near_a[d]))

    def direct2(r1):
        for c in range(COLORS):
            d = ORDERS[c][1]
            send(from_first(c, r1, {d: to_a[d]}), held2[c].at[r1, 0], send_sem.at[1, c], recv2.at[c, r1, 1], (stage, near_a[d]))

    def forward2(r1):
        for c in range(COLORS):
            d = ORDERS[c][1]
            wait(tie2[c].at[r1], recv2.at[c, r1, 0])
            send(tie2[c].at[r1], held2[c].at[r1, 1], send_sem.at[4, c], recv2.at[c, r1, 2], (stage, near_b[d]))

    def partial(c, role):
        d1, d2, d = ORDERS[c]
        value = (pos, to_a, far, to_b)[role][d]
        kept = {d2: pos[d2], d: value}
        near = held1[c][(slice(None),) + tuple(kept[k] for k in range(3) if k != d1)]
        blocks = jnp.concatenate([held2[c][:, :, value].reshape(12 * SLOTS, -1), near.reshape(3 * SLOTS, -1), mine[c][value]], axis=0)
        part = jnp.dot(g_mat[c * 4 + role], blocks, preferred_element_type=jnp.float32)
        sums[role, :, COLS[c]] = part[:seq] + (part[seq:2 * seq] + part[2 * seq:])

    def send_sums(c, role):
        d = ORDERS[c][2]
        if role == 2:
            send(sums.at[2, LOW, SPANS[c]], tin.at[LOW, SPANS[c]], send_sem.at[2, c], tin_sem.at[c, 0], (stage, near_a[d]))
            send(sums.at[2, HIGH, SPANS[c]], tin.at[HIGH, SPANS[c]], send_sem.at[2, c], tin_sem.at[c, 1], (stage, near_b[d]))
        elif role == 3:
            send(sums.at[3, HIGH, SPANS[c]], got.at[2, HIGH, SPANS[c]], send_sem.at[2, c], got_sem.at[2, c], (other, near_b[d]))
        elif role == 1:
            send(sums.at[1, LOW, SPANS[c]], got.at[1, LOW, SPANS[c]], send_sem.at[2, c], got_sem.at[1, c], (other, near_a[d]))
        else:
            send(sums.at[0, :, SPANS[c]], got.at[0, :, SPANS[c]], send_sem.at[5, c], got_sem.at[0, c], (other, me))

    def merge(c, low):
        wait(tin.at[LOW if low else HIGH, SPANS[c]], tin_sem.at[c, 0 if low else 1])
        role, rows = (3, slice(0, 64)) if low else (1, slice(64, 128))
        sums[role, rows, COLS[c]] += tin[rows, COLS[c]]

    def send_merged(c, low):
        d = ORDERS[c][2]
        if low:
            send(sums.at[3, LOW, SPANS[c]], got.at[2, LOW, SPANS[c]], send_sem.at[2, c], got_sem.at[2, c], (other, near_b[d]))
        else:
            send(sums.at[1, HIGH, SPANS[c]], got.at[1, HIGH, SPANS[c]], send_sem.at[2, c], got_sem.at[1, c], (other, near_a[d]))

    choices = ((ids_ref, ids_in), (slots_ref, slots_in), (gates_ref, gates_in))

    def send_choices():
        for k, (src, dst) in enumerate(choices):
            pltpu.make_async_copy(src, dst.at[9], local_sem.at[2 + k]).start()
            for axis in range(3):
                for role, peer in ((1, near_a[axis]), (2, remote[axis]), (3, near_b[axis])):
                    send(src, dst.at[axis * 3 + role - 1], kg_sem.at[0, k], kg_sem.at[1, k], (stage, peer))

    side = copy_to(h_ref, x_in, side_sem.at[0], side_sem.at[1], (other, me))
    local = [pltpu.make_async_copy(src, dst, local_sem.at[k]) for k, (src, dst) in enumerate(((norm_ref, norm_in), (wo_ref, wo_in)))]
    own = [pltpu.make_async_copy(table(c, {ORDERS[c][0]: pos[ORDERS[c][0]], ORDERS[c][1]: pos[ORDERS[c][1]]}), mine[c], mine_sem.at[c]) for c in range(COLORS)]

    def build_gates():
        for k, (src, dst) in enumerate(choices):
            pltpu.make_async_copy(src, dst.at[9], local_sem.at[2 + k]).wait()
            wait(dst.at[pl.ds(0, 9)], kg_sem.at[1, k])
        columns = []
        for c in range(COLORS):
            d1, d2, d = ORDERS[c]
            for role in range(4):
                value = (pos, to_a, far, to_b)[role][d]
                which = 9 if role == 0 else d * 3 + role - 1
                ids, slot = ids_in[which], slots_in[which]
                at = [(ids >> shift) & 3 for shift in (4, 2, 0)]
                first, second = [(sign[k] * (at[k] - pos[k])) & 3 for k in (d1, d2)]
                block = jnp.where(second > 0, first * 3 + second - 1, jnp.where(first > 0, 11 + first, 15))
                column = block * SLOTS + slot - rank(d, value) * SLOTS
                columns.append(jnp.where((slot >= 0) & (at[d] == pos[d]), column, -1).astype(jnp.float32))
        places = jnp.concatenate(columns + [jnp.zeros((32, seq), jnp.float32)], axis=0).T
        gates = jnp.concatenate([gates_in[k] for k in range(10)] + [jnp.zeros((48, seq), jnp.float32)], axis=0).T
        step = 128
        for c in range(COLORS):
            for role in range(4):
                g = 8 * (9 if role == 0 else ORDERS[c][2] * 3 + role - 1)
                p = 8 * (c * 4 + role)
                for b in range(0, HELD, step):
                    col = (lax.broadcasted_iota(jnp.int32, (seq, step), 1) + b).astype(jnp.float32)
                    val = jnp.zeros((seq, step), jnp.float32)
                    for i in range(8):
                        val = jnp.where(places[:, p + i:p + i + 1] == col, gates[:, g + i:g + i + 1], val)
                    high = val.astype(jnp.bfloat16)
                    rest = val - high.astype(jnp.float32)
                    mid = rest.astype(jnp.bfloat16)
                    low = (rest - mid.astype(jnp.float32)).astype(jnp.bfloat16)
                    for k, piece in enumerate((high, mid, low)):
                        g_mat[c * 4 + role, k * seq:(k + 1) * seq, b:b + step] = piece

    weights = (wq_ref, wk_ref, wv_ref)

    def load(k, i):
        slot = lax.rem(i, depth)
        return pltpu.make_async_copy(weights[k].at[pl.ds(pl.multiple_of(i * piece_rows, piece_rows), piece_rows)], raw.at[slot], raw_sem.at[slot])

    def flatten(k, start, stop):
        step = 64

        def body(i, carry):
            load(k, i).wait()
            for j in range(0, piece_rows, step):
                flat[k, pl.ds(pl.multiple_of(i * piece_rows + j, step), step), :] = raw[lax.rem(i, depth), pl.ds(j, step)].reshape(step, d_model)

            @pl.when(i + depth < pieces)
            def _():
                load(k, i + depth).start()

            return carry

        if start == 0:
            for i in range(depth):
                load(k, i).start()
        lax.fori_loop(start, stop, body, 0)

    head = 128
    pair = 2 * head
    causal = lax.broadcasted_iota(jnp.int32, (seq, seq), 0) >= lax.broadcasted_iota(jnp.int32, (seq, seq), 1)

    def norm():
        side.wait_recv()
        total = jnp.zeros((seq, 1), jnp.float32)
        for c in range(COLORS):
            for slot in range(3):
                wait(got.at[slot, :, SPANS[c]], got_sem.at[slot, c])
        for cols in spans(0, d_model):
            y = x_in[:, cols].astype(jnp.float32) + (got[0, :, cols] + (got[1, :, cols] + got[2, :, cols]))
            y = y.astype(jnp.bfloat16).astype(jnp.float32)
            got[0, :, cols] = y
            total += jnp.sum(y * y, axis=1, keepdims=True)
        inv = lax.rsqrt(total * (1.0 / d_model) + NORM_EPS)
        for cols in spans(0, d_model):
            x_in[:, cols] = (got[0, :, cols] * inv * norm_in[:, cols]).astype(jnp.bfloat16)

    def project(k, p):
        cols = slice(p * pair, (p + 1) * pair)
        qkv[k, :, cols] = jnp.dot(x_in[...], flat[k, :, cols], preferred_element_type=jnp.float32).astype(jnp.bfloat16)

    def softmax(cols):
        scores = jnp.where(causal, tin[:, cols] * (head ** -0.5), -jnp.inf)
        grown = jnp.exp(scores - jnp.max(scores, axis=1, keepdims=True))
        qkv[0, :, cols] = (grown * (1.0 / jnp.sum(grown, axis=1, keepdims=True))).astype(jnp.bfloat16)

    def attend():
        heads = [slice(h * head, (h + 1) * head) for h in range(d_model // head)]
        for k in range(2):
            for p in range(d_model // pair):
                project(k, p)
        for cols in heads:
            tin[:, cols] = lax.dot_general(qkv[0, :, cols], qkv[1, :, cols], (((1,), (1,)), ((), ())), preferred_element_type=jnp.float32)
        for p in range(d_model // pair):
            softmax(heads[2 * p])
            softmax(heads[2 * p + 1])
            project(2, p)
        for cols in heads:
            x_in[:, cols] = jnp.dot(qkv[0, :, cols], qkv[2, :, cols], preferred_element_type=jnp.float32).astype(jnp.bfloat16)

    send_choices()
    phase1()
    side.start()
    phase2(0)
    direct2(0)
    for copy in local + own:
        copy.start()
    build_gates()
    flatten(0, 0, pieces // 4)
    forward1(0)
    flatten(0, pieces // 4, pieces)
    forward1(1)
    phase2(3)
    direct2(3)
    flatten(1, 0, pieces)
    forward2(0)
    phase2(1)
    phase2(2)
    direct2(1)
    direct2(2)
    flatten(2, 0, pieces // 2)
    forward2(3)
    flatten(2, pieces // 2, pieces)
    forward2(1)
    for copy in own:
        copy.wait()
    forward2(2)
    for c in range(COLORS):
        for r1 in range(4):
            for r2 in (1, 2, 3):
                wait(held2[c].at[r1, r2 - 1], recv2.at[c, r1, r2])
    before = None
    for role in (2, 3, 1, 0):
        for c in range(COLORS):
            partial(c, role)
            if before is not None:
                send_sums(*before)
            before = (c, role)
    send_sums(*before)
    before = None
    for low in (True, False):
        for c in range(COLORS):
            merge(c, low)
            if before is not None:
                send_merged(*before)
            before = (c, low)
    for copy in local:
        copy.wait()
    send_merged(*before)
    norm()
    attend()
    for p in range(d_model // pair):
        cols = slice(p * pair, (p + 1) * pair)
        out = jnp.dot(x_in[...], wo_in[:, cols], preferred_element_type=jnp.float32).astype(jnp.bfloat16)
        z_ref[:, cols] = (got[0, :, cols] + out.astype(jnp.float32)).astype(jnp.bfloat16)

    side.wait_send()
    for k, (src, dst) in enumerate(choices):
        wait(dst.at[pl.ds(0, 9)], kg_sem.at[0, k])
    for c in range(COLORS):
        wait(held1[c], send_sem.at[0, c])
        wait(held2[c], send_sem.at[1, c])
        wait(sums.at[pl.ds(1, 3), :, SPANS[c]], send_sem.at[2, c])
        wait(tie1[c], send_sem.at[3, c])
        wait(tie2[c], send_sem.at[4, c])
        wait(sums.at[0, :, SPANS[c]], send_sem.at[5, c])


def spans(lo, hi):
    return [slice(b, min(b + 512, hi)) for b in range(lo, hi, 512)]


def run_stage(o_tab, ids, slots, gates, h, norm_w, wq, wk, wv, wo):
    seq, d = h.shape
    dma = pltpu.SemaphoreType.DMA
    piece = 128

    def per_colour(*lead):
        return [pltpu.VMEM(lead + (SLOTS, w), jnp.bfloat16) for w in WIDTHS]

    return pl.pallas_call(
        stage_kernel,
        out_shape=pltpu.VMEM((seq, d), jnp.bfloat16),
        in_specs=[pl.BlockSpec(memory_space=pl.ANY)] * 10,
        out_specs=pl.BlockSpec(memory_space=pltpu.VMEM),
        scratch_shapes=[
            *per_colour(3, 4, 4),
            *per_colour(4, 4),
            *per_colour(4, 3, 4),
            *per_colour(4, 4),
            *per_colour(4),
            pltpu.VMEM((4, seq, d), jnp.float32),
            pltpu.VMEM((seq, d), jnp.float32),
            pltpu.VMEM((3, seq, d), jnp.float32),
            pltpu.VMEM((10,) + ids.shape, jnp.int32),
            pltpu.VMEM((10,) + slots.shape, jnp.int32),
            pltpu.VMEM((10,) + gates.shape, jnp.float32),
            pltpu.VMEM((4 * COLORS, 3 * seq, HELD), jnp.bfloat16),
            pltpu.VMEM(norm_w.shape, jnp.float32),
            pltpu.VMEM((3, d, d), jnp.bfloat16),
            pltpu.VMEM((d, d), jnp.bfloat16),
            pltpu.VMEM((3, piece) + wq.shape[1:], jnp.bfloat16),
            pltpu.VMEM((seq, d), jnp.bfloat16),
            pltpu.VMEM((3, seq, d), jnp.bfloat16),
            dma((2, 3)),
            dma((2,)),
            dma((5,)),
            dma((COLORS,)),
            dma((3,)),
            dma((6, COLORS)),
            dma((COLORS, 5)),
            dma((COLORS, 4, 4)),
            dma((COLORS, 2)),
            dma((3, COLORS)),
        ],
        compiler_params=pltpu.CompilerParams(collective_id=0, has_side_effects=True, vmem_limit_bytes=66400000),
        name='stage',
    )(o_tab, ids, slots, gates, h, norm_w, wq, wk, wv, wo)


def solution(mesh):
    tok_spec = P('pp', 'ep', None, None)
    wt_spec = P('pp', None, None, None)

    def device_step(expert_out, expert_ids, slot_ids, gate_vals, residual, norm_w, w_query, w_key, w_value, w_out):
        seq_len, d_model = residual.shape[2:]

        def choices(array):
            return array.reshape(seq_len, array.shape[3]).T

        result = run_stage(
            expert_out.reshape(SIDE, SIDE, SIDE, SLOTS, d_model),
            choices(expert_ids), choices(slot_ids), choices(gate_vals),
            residual.reshape(seq_len, d_model), norm_w, w_query[0], w_key[0], w_value[0], w_out[0].reshape(-1, d_model),
        )
        return result.reshape(residual.shape)

    return jax.shard_map(device_step, mesh=mesh, in_specs=(tok_spec, tok_spec, tok_spec, tok_spec, tok_spec, P('pp', None), wt_spec, wt_spec, wt_spec, wt_spec), out_specs=tok_spec, check_vma=False)
```

```python
import jax
import jax.numpy as jnp
from jax import lax
from jax.experimental import pallas as pl
from jax.experimental.pallas import tpu as pltpu
from jax.sharding import PartitionSpec as P

NORM_EPS = 1e-6
MESH = pl.DeviceIdType.MESH
SIDE = 4
COLORS = 3
SLOTS = 24
ORDERS = ((2, 1, 0), (1, 0, 2), (0, 2, 1))
WIDTHS = (640, 640, 768)
STARTS = (0, 640, 1280)
COLS = [slice(at, at + w) for at, w in zip(STARTS, WIDTHS)]
SPANS = [pl.ds(at, w) for at, w in zip(STARTS, WIDTHS)]
HELD = 16 * SLOTS
LOW, HIGH = pl.ds(0, 64), pl.ds(64, 64)


def stage_kernel(o_ref, ids_ref, slots_ref, gates_ref, h_ref, norm_ref, wq_ref, wk_ref, wv_ref, wo_ref, z_ref, *scratch):
    held1, tie1, held2, tie2, mine = [scratch[3 * k:3 * k + 3] for k in range(5)]
    (sums, tin, got, ids_in, slots_in, gates_in, g_mat, norm_in, flat, wo_in, raw, x_in, qkv,
     kg_sem, side_sem, local_sem, mine_sem, raw_sem, send_sem, recv1, recv2, tin_sem, got_sem) = scratch[15:]
    stage = lax.axis_index('pp')
    me = lax.axis_index('ep')
    other = 1 - stage
    pos = (me // 16, (me // 4) % 4, me % 4)
    sign = [1 - 2 * (p % 2) for p in pos]
    to_a = [lax.rem(p + s + SIDE, SIDE) for p, s in zip(pos, sign)]
    to_b = [lax.rem(p - s + SIDE, SIDE) for p, s in zip(pos, sign)]
    far = [lax.rem(p + 2, SIDE) for p in pos]
    seq, d_model = x_in.shape
    depth, piece_rows = raw.shape[:2]
    pieces = flat.shape[1] // piece_rows

    def rank(axis, value):
        z, y, x = [value if k == axis else p for k, p in enumerate(pos)]
        return z * 16 + y * 4 + x

    near_a = [rank(k, to_a[k]) for k in range(3)]
    near_b = [rank(k, to_b[k]) for k in range(3)]
    remote = [rank(k, far[k]) for k in range(3)]

    barrier = pltpu.get_barrier_semaphore()
    peers = [(other, me)]
    for k in range(3):
        peers.append((stage, remote[k]))
        for where in (near_a[k], near_b[k]):
            peers += [(stage, where), (other, where)]
    for peer in peers:
        pl.semaphore_signal(barrier, inc=1, device_id=peer, device_id_type=MESH)
    pl.semaphore_wait(barrier, len(peers))

    def copy_to(src, dst, send_s, recv_s, peer):
        return pltpu.make_async_remote_copy(src_ref=src, dst_ref=dst, send_sem=send_s, recv_sem=recv_s, device_id=peer, device_id_type=MESH)

    def send(*args):
        copy_to(*args).start()

    def wait(ref, sem):
        pltpu.make_async_copy(ref, ref, sem).wait()

    def table(c, fixed):
        return o_ref.at[tuple(fixed.get(k, slice(None)) for k in range(3)) + (slice(None), SPANS[c])]

    def from_first(c, r1, fixed):
        d1 = ORDERS[c][0]
        if r1 == 0:
            return table(c, {d1: pos[d1], **fixed})
        return held1[c].at[(r1 - 1,) + tuple(fixed.get(k, slice(None)) for k in range(3) if k != d1)]

    def phase1():
        for c in range(COLORS):
            d = ORDERS[c][0]
            for half in range(2):
                some = pl.ds(2 * half, 2)
                send(table(c, {d: far[d], (d == 0) * 1: some}), tie1[c].at[some], send_sem.at[0, c], recv1.at[c, 4 * half], (stage, near_a[d]))
        for c in range(COLORS):
            d = ORDERS[c][0]
            send(table(c, {d: to_b[d]}), held1[c].at[2], send_sem.at[0, c], recv1.at[c, 3], (stage, near_b[d]))
        for c in range(COLORS):
            d = ORDERS[c][0]
            send(table(c, {d: to_a[d]}), held1[c].at[0], send_sem.at[0, c], recv1.at[c, 1], (stage, near_a[d]))

    def forward1(half):
        some = pl.ds(2 * half, 2)
        for c in range(COLORS):
            d = ORDERS[c][0]
            wait(tie1[c].at[some], recv1.at[c, 4 * half])
            send(tie1[c].at[some], held1[c].at[1, some], send_sem.at[3, c], recv1.at[c, 2], (stage, near_b[d]))

    def phase2(r1):
        for c in range(COLORS):
            d = ORDERS[c][1]
            if r1:
                wait(held1[c].at[r1 - 1], recv1.at[c, r1])
            send(from_first(c, r1, {d: to_b[d]}), held2[c].at[r1, 2], send_sem.at[1, c], recv2.at[c, r1, 3], (stage, near_b[d]))
            send(from_first(c, r1, {d: far[d]}), tie2[c].at[r1], send_sem.at[1, c], recv2.at[c, r1, 0], (stage, near_a[d]))

    def direct2(r1):
        for c in range(COLORS):
            d = ORDERS[c][1]
            send(from_first(c, r1, {d: to_a[d]}), held2[c].at[r1, 0], send_sem.at[1, c], recv2.at[c, r1, 1], (stage, near_a[d]))

    def forward2(r1):
        for c in range(COLORS):
            d = ORDERS[c][1]
            wait(tie2[c].at[r1], recv2.at[c, r1, 0])
            send(tie2[c].at[r1], held2[c].at[r1, 1], send_sem.at[4, c], recv2.at[c, r1, 2], (stage, near_b[d]))

    def partial(c, role):
        d1, d2, d = ORDERS[c]
        value = (pos, to_a, far, to_b)[role][d]
        kept = {d2: pos[d2], d: value}
        near = held1[c][(slice(None),) + tuple(kept[k] for k in range(3) if k != d1)]
        blocks = jnp.concatenate([held2[c][:, :, value].reshape(12 * SLOTS, -1), near.reshape(3 * SLOTS, -1), mine[c][value]], axis=0)
        part = jnp.dot(g_mat[c * 4 + role], blocks, preferred_element_type=jnp.float32)
        sums[role, :, COLS[c]] = part[:seq] + (part[seq:2 * seq] + part[2 * seq:])

    def send_sums(c, role):
        d = ORDERS[c][2]
        if role == 2:
            send(sums.at[2, LOW, SPANS[c]], tin.at[LOW, SPANS[c]], send_sem.at[2, c], tin_sem.at[c, 0], (stage, near_a[d]))
            send(sums.at[2, HIGH, SPANS[c]], tin.at[HIGH, SPANS[c]], send_sem.at[2, c], tin_sem.at[c, 1], (stage, near_b[d]))
        elif role == 3:
            send(sums.at[3, HIGH, SPANS[c]], got.at[2, HIGH, SPANS[c]], send_sem.at[2, c], got_sem.at[2, c], (other, near_b[d]))
        elif role == 1:
            send(sums.at[1, LOW, SPANS[c]], got.at[1, LOW, SPANS[c]], send_sem.at[2, c], got_sem.at[1, c], (other, near_a[d]))
        else:
            send(sums.at[0, :, SPANS[c]], got.at[0, :, SPANS[c]], send_sem.at[5, c], got_sem.at[0, c], (other, me))

    def merge(c, low):
        wait(tin.at[LOW if low else HIGH, SPANS[c]], tin_sem.at[c, 0 if low else 1])
        role, rows = (3, slice(0, 64)) if low else (1, slice(64, 128))
        sums[role, rows, COLS[c]] += tin[rows, COLS[c]]

    def send_merged(c, low):
        d = ORDERS[c][2]
        if low:
            send(sums.at[3, LOW, SPANS[c]], got.at[2, LOW, SPANS[c]], send_sem.at[2, c], got_sem.at[2, c], (other, near_b[d]))
        else:
            send(sums.at[1, HIGH, SPANS[c]], got.at[1, HIGH, SPANS[c]], send_sem.at[2, c], got_sem.at[1, c], (other, near_a[d]))

    choices = ((ids_ref, ids_in), (slots_ref, slots_in), (gates_ref, gates_in))

    def send_choices():
        for k, (src, dst) in enumerate(choices):
            pltpu.make_async_copy(src, dst.at[9], local_sem.at[2 + k]).start()
            for axis in range(3):
                for role, peer in ((1, near_a[axis]), (2, remote[axis]), (3, near_b[axis])):
                    send(src, dst.at[axis * 3 + role - 1], kg_sem.at[0, k], kg_sem.at[1, k], (stage, peer))

    side = copy_to(h_ref, x_in, side_sem.at[0], side_sem.at[1], (other, me))
    local = [pltpu.make_async_copy(src, dst, local_sem.at[k]) for k, (src, dst) in enumerate(((norm_ref, norm_in), (wo_ref, wo_in)))]
    own = [pltpu.make_async_copy(table(c, {ORDERS[c][0]: pos[ORDERS[c][0]], ORDERS[c][1]: pos[ORDERS[c][1]]}), mine[c], mine_sem.at[c]) for c in range(COLORS)]

    def build_gates():
        for k, (src, dst) in enumerate(choices):
            pltpu.make_async_copy(src, dst.at[9], local_sem.at[2 + k]).wait()
            wait(dst.at[pl.ds(0, 9)], kg_sem.at[1, k])
        columns = []
        for c in range(COLORS):
            d1, d2, d = ORDERS[c]
            for role in range(4):
                value = (pos, to_a, far, to_b)[role][d]
                which = 9 if role == 0 else d * 3 + role - 1
                ids, slot = ids_in[which], slots_in[which]
                at = [(ids >> shift) & 3 for shift in (4, 2, 0)]
                first, second = [(sign[k] * (at[k] - pos[k])) & 3 for k in (d1, d2)]
                block = jnp.where(second > 0, first * 3 + second - 1, jnp.where(first > 0, 11 + first, 15))
                column = block * SLOTS + slot - rank(d, value) * SLOTS
                columns.append(jnp.where((slot >= 0) & (at[d] == pos[d]), column, -1).astype(jnp.float32))
        places = jnp.concatenate(columns + [jnp.zeros((32, seq), jnp.float32)], axis=0).T
        gates = jnp.concatenate([gates_in[k] for k in range(10)] + [jnp.zeros((48, seq), jnp.float32)], axis=0).T
        step = 128
        for c in range(COLORS):
            for role in range(4):
                g = 8 * (9 if role == 0 else ORDERS[c][2] * 3 + role - 1)
                p = 8 * (c * 4 + role)
                for b in range(0, HELD, step):
                    col = (lax.broadcasted_iota(jnp.int32, (seq, step), 1) + b).astype(jnp.float32)
                    val = jnp.zeros((seq, step), jnp.float32)
                    for i in range(8):
                        val = jnp.where(places[:, p + i:p + i + 1] == col, gates[:, g + i:g + i + 1], val)
                    high = val.astype(jnp.bfloat16)
                    rest = val - high.astype(jnp.float32)
                    mid = rest.astype(jnp.bfloat16)
                    low = (rest - mid.astype(jnp.float32)).astype(jnp.bfloat16)
                    for k, piece in enumerate((high, mid, low)):
                        g_mat[c * 4 + role, k * seq:(k + 1) * seq, b:b + step] = piece

    weights = (wq_ref, wk_ref, wv_ref)

    def load(k, i):
        slot = lax.rem(i, depth)
        return pltpu.make_async_copy(weights[k].at[pl.ds(pl.multiple_of(i * piece_rows, piece_rows), piece_rows)], raw.at[slot], raw_sem.at[slot])

    def flatten(k, start, stop):
        step = 64

        def body(i, carry):
            load(k, i).wait()
            for j in range(0, piece_rows, step):
                flat[k, pl.ds(pl.multiple_of(i * piece_rows + j, step), step), :] = raw[lax.rem(i, depth), pl.ds(j, step)].reshape(step, d_model)

            @pl.when(i + depth < pieces)
            def _():
                load(k, i + depth).start()

            return carry

        if start == 0:
            for i in range(depth):
                load(k, i).start()
        lax.fori_loop(start, stop, body, 0)

    head = 128
    pair = 2 * head
    causal = lax.broadcasted_iota(jnp.int32, (seq, seq), 0) >= lax.broadcasted_iota(jnp.int32, (seq, seq), 1)

    def norm():
        side.wait_recv()
        total = jnp.zeros((seq, 1), jnp.float32)
        for c in range(COLORS):
            for slot in range(3):
                wait(got.at[slot, :, SPANS[c]], got_sem.at[slot, c])
        for cols in spans(0, d_model):
            y = x_in[:, cols].astype(jnp.float32) + (got[0, :, cols] + (got[1, :, cols] + got[2, :, cols]))
            y = y.astype(jnp.bfloat16).astype(jnp.float32)
            got[0, :, cols] = y
            total += jnp.sum(y * y, axis=1, keepdims=True)
        inv = lax.rsqrt(total * (1.0 / d_model) + NORM_EPS)
        for cols in spans(0, d_model):
            x_in[:, cols] = (got[0, :, cols] * inv * norm_in[:, cols]).astype(jnp.bfloat16)

    def project(k, p):
        cols = slice(p * pair, (p + 1) * pair)
        qkv[k, :, cols] = jnp.dot(x_in[...], flat[k, :, cols], preferred_element_type=jnp.float32).astype(jnp.bfloat16)

    def softmax(cols):
        scores = jnp.where(causal, tin[:, cols] * (head ** -0.5), -jnp.inf)
        grown = jnp.exp(scores - jnp.max(scores, axis=1, keepdims=True))
        qkv[0, :, cols] = (grown * (1.0 / jnp.sum(grown, axis=1, keepdims=True))).astype(jnp.bfloat16)

    def attend():
        heads = [slice(h * head, (h + 1) * head) for h in range(d_model // head)]
        for k in range(2):
            for p in range(d_model // pair):
                project(k, p)
        for cols in heads:
            tin[:, cols] = lax.dot_general(qkv[0, :, cols], qkv[1, :, cols], (((1,), (1,)), ((), ())), preferred_element_type=jnp.float32)
        for p in range(d_model // pair):
            softmax(heads[2 * p])
            softmax(heads[2 * p + 1])
            project(2, p)
        for cols in heads:
            x_in[:, cols] = jnp.dot(qkv[0, :, cols], qkv[2, :, cols], preferred_element_type=jnp.float32).astype(jnp.bfloat16)

    send_choices()
    phase1()
    side.start()
    phase2(0)
    direct2(0)
    for copy in local + own:
        copy.start()
    flatten(0, 0, 3 * pieces // 4)
    forward1(0)
    flatten(0, 3 * pieces // 4, pieces)
    forward1(1)
    phase2(3)
    direct2(3)
    build_gates()
    flatten(1, 0, 3 * pieces // 4)
    forward2(0)
    phase2(1)
    phase2(2)
    direct2(1)
    direct2(2)
    flatten(1, 3 * pieces // 4, pieces)
    flatten(2, 0, pieces // 4)
    forward2(3)
    flatten(2, pieces // 4, 3 * pieces // 4)
    forward2(1)
    forward2(2)
    for copy in own:
        copy.wait()
    for c in range(COLORS):
        for r1 in range(4):
            for r2 in (1, 2, 3):
                wait(held2[c].at[r1, r2 - 1], recv2.at[c, r1, r2])
    before = None
    for role in (2, 3, 1, 0):
        for c in range(COLORS):
            partial(c, role)
            if before is not None:
                send_sums(*before)
            before = (c, role)
    send_sums(*before)
    flatten(2, 3 * pieces // 4, pieces)
    before = None
    for low in (True, False):
        for c in range(COLORS):
            merge(c, low)
            if before is not None:
                send_merged(*before)
            before = (c, low)
    for copy in local:
        copy.wait()
    send_merged(*before)
    norm()
    attend()
    for p in range(d_model // pair):
        cols = slice(p * pair, (p + 1) * pair)
        out = jnp.dot(x_in[...], wo_in[:, cols], preferred_element_type=jnp.float32).astype(jnp.bfloat16)
        z_ref[:, cols] = (got[0, :, cols] + out.astype(jnp.float32)).astype(jnp.bfloat16)

    side.wait_send()
    for k, (src, dst) in enumerate(choices):
        wait(dst.at[pl.ds(0, 9)], kg_sem.at[0, k])
    for c in range(COLORS):
        wait(held1[c], send_sem.at[0, c])
        wait(held2[c], send_sem.at[1, c])
        wait(sums.at[pl.ds(1, 3), :, SPANS[c]], send_sem.at[2, c])
        wait(tie1[c], send_sem.at[3, c])
        wait(tie2[c], send_sem.at[4, c])
        wait(sums.at[0, :, SPANS[c]], send_sem.at[5, c])


def spans(lo, hi):
    return [slice(b, min(b + 512, hi)) for b in range(lo, hi, 512)]


def run_stage(o_tab, ids, slots, gates, h, norm_w, wq, wk, wv, wo):
    seq, d = h.shape
    dma = pltpu.SemaphoreType.DMA
    piece = 128

    def per_colour(*lead):
        return [pltpu.VMEM(lead + (SLOTS, w), jnp.bfloat16) for w in WIDTHS]

    return pl.pallas_call(
        stage_kernel,
        out_shape=pltpu.VMEM((seq, d), jnp.bfloat16),
        in_specs=[pl.BlockSpec(memory_space=pl.ANY)] * 10,
        out_specs=pl.BlockSpec(memory_space=pltpu.VMEM),
        scratch_shapes=[
            *per_colour(3, 4, 4),
            *per_colour(4, 4),
            *per_colour(4, 3, 4),
            *per_colour(4, 4),
            *per_colour(4),
            pltpu.VMEM((4, seq, d), jnp.float32),
            pltpu.VMEM((seq, d), jnp.float32),
            pltpu.VMEM((3, seq, d), jnp.float32),
            pltpu.VMEM((10,) + ids.shape, jnp.int32),
            pltpu.VMEM((10,) + slots.shape, jnp.int32),
            pltpu.VMEM((10,) + gates.shape, jnp.float32),
            pltpu.VMEM((4 * COLORS, 3 * seq, HELD), jnp.bfloat16),
            pltpu.VMEM(norm_w.shape, jnp.float32),
            pltpu.VMEM((3, d, d), jnp.bfloat16),
            pltpu.VMEM((d, d), jnp.bfloat16),
            pltpu.VMEM((3, piece) + wq.shape[1:], jnp.bfloat16),
            pltpu.VMEM((seq, d), jnp.bfloat16),
            pltpu.VMEM((3, seq, d), jnp.bfloat16),
            dma((2, 3)),
            dma((2,)),
            dma((5,)),
            dma((COLORS,)),
            dma((3,)),
            dma((6, COLORS)),
            dma((COLORS, 5)),
            dma((COLORS, 4, 4)),
            dma((COLORS, 2)),
            dma((3, COLORS)),
        ],
        compiler_params=pltpu.CompilerParams(collective_id=0, has_side_effects=True, vmem_limit_bytes=66400000),
        name='stage',
    )(o_tab, ids, slots, gates, h, norm_w, wq, wk, wv, wo)


def solution(mesh):
    tok_spec = P('pp', 'ep', None, None)
    wt_spec = P('pp', None, None, None)

    def device_step(expert_out, expert_ids, slot_ids, gate_vals, residual, norm_w, w_query, w_key, w_value, w_out):
        seq_len, d_model = residual.shape[2:]

        def choices(array):
            return array.reshape(seq_len, array.shape[3]).T

        result = run_stage(
            expert_out.reshape(SIDE, SIDE, SIDE, SLOTS, d_model),
            choices(expert_ids), choices(slot_ids), choices(gate_vals),
            residual.reshape(seq_len, d_model), norm_w, w_query[0], w_key[0], w_value[0], w_out[0].reshape(-1, d_model),
        )
        return result.reshape(residual.shape)

    return jax.shard_map(device_step, mesh=mesh, in_specs=(tok_spec, tok_spec, tok_spec, tok_spec, tok_spec, P('pp', None), wt_spec, wt_spec, wt_spec, wt_spec), out_specs=tok_spec, check_vma=False)
```

```python
import jax
import jax.numpy as jnp
from jax import lax
from jax.experimental import pallas as pl
from jax.experimental.pallas import tpu as pltpu
from jax.sharding import PartitionSpec as P

NORM_EPS = 1e-6
MESH = pl.DeviceIdType.MESH
SIDE = 4
COLORS = 3
SLOTS = 24
ORDERS = ((2, 1, 0), (1, 0, 2), (0, 2, 1))
WIDTHS = (640, 640, 768)
STARTS = (0, 640, 1280)
COLS = [slice(at, at + w) for at, w in zip(STARTS, WIDTHS)]
SPANS = [pl.ds(at, w) for at, w in zip(STARTS, WIDTHS)]
HELD = 16 * SLOTS
LOW, HIGH = pl.ds(0, 64), pl.ds(64, 64)


def stage_kernel(o_ref, ids_ref, slots_ref, gates_ref, h_ref, norm_ref, wq_ref, wk_ref, wv_ref, wo_ref, z_ref, *scratch):
    held1, tie1, held2, tie2, mine = [scratch[3 * k:3 * k + 3] for k in range(5)]
    (sums, tin, got, ids_in, slots_in, gates_in, g_mat, norm_in, flat, wo_in, raw, x_in, qkv,
     kg_sem, side_sem, local_sem, mine_sem, raw_sem, send_sem, recv1, recv2, tin_sem, got_sem) = scratch[15:]
    stage = lax.axis_index('pp')
    me = lax.axis_index('ep')
    other = 1 - stage
    pos = (me // 16, (me // 4) % 4, me % 4)
    sign = [1 - 2 * (p % 2) for p in pos]
    to_a = [lax.rem(p + s + SIDE, SIDE) for p, s in zip(pos, sign)]
    to_b = [lax.rem(p - s + SIDE, SIDE) for p, s in zip(pos, sign)]
    far = [lax.rem(p + 2, SIDE) for p in pos]
    seq, d_model = x_in.shape
    depth, piece_rows = raw.shape[:2]
    pieces = flat.shape[1] // piece_rows

    def rank(axis, value):
        z, y, x = [value if k == axis else p for k, p in enumerate(pos)]
        return z * 16 + y * 4 + x

    near_a = [rank(k, to_a[k]) for k in range(3)]
    near_b = [rank(k, to_b[k]) for k in range(3)]
    remote = [rank(k, far[k]) for k in range(3)]

    barrier = pltpu.get_barrier_semaphore()
    peers = [(other, me)]
    for k in range(3):
        peers.append((stage, remote[k]))
        for where in (near_a[k], near_b[k]):
            peers += [(stage, where), (other, where)]
    for peer in peers:
        pl.semaphore_signal(barrier, inc=1, device_id=peer, device_id_type=MESH)
    pl.semaphore_wait(barrier, len(peers))

    def copy_to(src, dst, send_s, recv_s, peer):
        return pltpu.make_async_remote_copy(src_ref=src, dst_ref=dst, send_sem=send_s, recv_sem=recv_s, device_id=peer, device_id_type=MESH)

    def send(*args):
        copy_to(*args).start()

    def wait(ref, sem):
        pltpu.make_async_copy(ref, ref, sem).wait()

    def table(c, fixed):
        return o_ref.at[tuple(fixed.get(k, slice(None)) for k in range(3)) + (slice(None), SPANS[c])]

    def from_first(c, r1, fixed):
        d1 = ORDERS[c][0]
        if r1 == 0:
            return table(c, {d1: pos[d1], **fixed})
        return held1[c].at[(r1 - 1,) + tuple(fixed.get(k, slice(None)) for k in range(3) if k != d1)]

    def phase1():
        for c in range(COLORS):
            d = ORDERS[c][0]
            for half in range(2):
                some = pl.ds(2 * half, 2)
                send(table(c, {d: far[d], (d == 0) * 1: some}), tie1[c].at[some], send_sem.at[0, c], recv1.at[c, 4 * half], (stage, near_a[d]))
        for c in range(COLORS):
            d = ORDERS[c][0]
            send(table(c, {d: to_b[d]}), held1[c].at[2], send_sem.at[0, c], recv1.at[c, 3], (stage, near_b[d]))
        for c in range(COLORS):
            d = ORDERS[c][0]
            send(table(c, {d: to_a[d]}), held1[c].at[0], send_sem.at[0, c], recv1.at[c, 1], (stage, near_a[d]))

    def forward1(half):
        some = pl.ds(2 * half, 2)
        for c in range(COLORS):
            d = ORDERS[c][0]
            wait(tie1[c].at[some], recv1.at[c, 4 * half])
            send(tie1[c].at[some], held1[c].at[1, some], send_sem.at[3, c], recv1.at[c, 2], (stage, near_b[d]))

    def phase2(r1):
        for c in range(COLORS):
            d = ORDERS[c][1]
            if r1:
                wait(held1[c].at[r1 - 1], recv1.at[c, r1])
            send(from_first(c, r1, {d: to_b[d]}), held2[c].at[r1, 2], send_sem.at[1, c], recv2.at[c, r1, 3], (stage, near_b[d]))
            send(from_first(c, r1, {d: far[d]}), tie2[c].at[r1], send_sem.at[1, c], recv2.at[c, r1, 0], (stage, near_a[d]))

    def direct2(r1):
        for c in range(COLORS):
            d = ORDERS[c][1]
            send(from_first(c, r1, {d: to_a[d]}), held2[c].at[r1, 0], send_sem.at[1, c], recv2.at[c, r1, 1], (stage, near_a[d]))

    def forward2(r1):
        for c in range(COLORS):
            d = ORDERS[c][1]
            wait(tie2[c].at[r1], recv2.at[c, r1, 0])
            send(tie2[c].at[r1], held2[c].at[r1, 1], send_sem.at[4, c], recv2.at[c, r1, 2], (stage, near_b[d]))

    def partial(c, role):
        d1, d2, d = ORDERS[c]
        value = (pos, to_a, far, to_b)[role][d]
        kept = {d2: pos[d2], d: value}
        near = held1[c][(slice(None),) + tuple(kept[k] for k in range(3) if k != d1)]
        blocks = jnp.concatenate([held2[c][:, :, value].reshape(12 * SLOTS, -1), near.reshape(3 * SLOTS, -1), mine[c][value]], axis=0)
        part = jnp.dot(g_mat[c * 4 + role], blocks, preferred_element_type=jnp.float32)
        sums[role, :, COLS[c]] = part[:seq] + (part[seq:2 * seq] + part[2 * seq:])

    def send_sums(c, role):
        d = ORDERS[c][2]
        if role == 2:
            send(sums.at[2, LOW, SPANS[c]], tin.at[LOW, SPANS[c]], send_sem.at[2, c], tin_sem.at[c, 0], (stage, near_a[d]))
            send(sums.at[2, HIGH, SPANS[c]], tin.at[HIGH, SPANS[c]], send_sem.at[2, c], tin_sem.at[c, 1], (stage, near_b[d]))
        elif role == 3:
            send(sums.at[3, HIGH, SPANS[c]], got.at[2, HIGH, SPANS[c]], send_sem.at[2, c], got_sem.at[2, c], (other, near_b[d]))
        elif role == 1:
            send(sums.at[1, LOW, SPANS[c]], got.at[1, LOW, SPANS[c]], send_sem.at[2, c], got_sem.at[1, c], (other, near_a[d]))
        else:
            send(sums.at[0, :, SPANS[c]], got.at[0, :, SPANS[c]], send_sem.at[5, c], got_sem.at[0, c], (other, me))

    def merge(c, low):
        wait(tin.at[LOW if low else HIGH, SPANS[c]], tin_sem.at[c, 0 if low else 1])
        role, rows = (3, slice(0, 64)) if low else (1, slice(64, 128))
        sums[role, rows, COLS[c]] += tin[rows, COLS[c]]

    def send_merged(c, low):
        d = ORDERS[c][2]
        if low:
            send(sums.at[3, LOW, SPANS[c]], got.at[2, LOW, SPANS[c]], send_sem.at[2, c], got_sem.at[2, c], (other, near_b[d]))
        else:
            send(sums.at[1, HIGH, SPANS[c]], got.at[1, HIGH, SPANS[c]], send_sem.at[2, c], got_sem.at[1, c], (other, near_a[d]))

    choices = ((ids_ref, ids_in), (slots_ref, slots_in), (gates_ref, gates_in))

    def send_choices():
        for k, (src, dst) in enumerate(choices):
            pltpu.make_async_copy(src, dst.at[9], local_sem.at[2 + k]).start()
            for axis in range(3):
                for role, peer in ((1, near_a[axis]), (2, remote[axis]), (3, near_b[axis])):
                    send(src, dst.at[axis * 3 + role - 1], kg_sem.at[0, k], kg_sem.at[1, k], (stage, peer))

    side = copy_to(h_ref, x_in, side_sem.at[0], side_sem.at[1], (other, me))
    local = [pltpu.make_async_copy(src, dst, local_sem.at[k]) for k, (src, dst) in enumerate(((norm_ref, norm_in), (wo_ref, wo_in)))]
    own = [pltpu.make_async_copy(table(c, {ORDERS[c][0]: pos[ORDERS[c][0]], ORDERS[c][1]: pos[ORDERS[c][1]]}), mine[c], mine_sem.at[c]) for c in range(COLORS)]

    def build_gates():
        for k, (src, dst) in enumerate(choices):
            pltpu.make_async_copy(src, dst.at[9], local_sem.at[2 + k]).wait()
            wait(dst.at[pl.ds(0, 9)], kg_sem.at[1, k])
        columns = []
        for c in range(COLORS):
            d1, d2, d = ORDERS[c]
            for role in range(4):
                value = (pos, to_a, far, to_b)[role][d]
                which = 9 if role == 0 else d * 3 + role - 1
                ids, slot = ids_in[which], slots_in[which]
                at = [(ids >> shift) & 3 for shift in (4, 2, 0)]
                first, second = [(sign[k] * (at[k] - pos[k])) & 3 for k in (d1, d2)]
                block = jnp.where(second > 0, first * 3 + second - 1, jnp.where(first > 0, 11 + first, 15))
                column = block * SLOTS + slot - rank(d, value) * SLOTS
                columns.append(jnp.where((slot >= 0) & (at[d] == pos[d]), column, -1).astype(jnp.float32))
        places = jnp.concatenate(columns + [jnp.zeros((32, seq), jnp.float32)], axis=0).T
        gates = jnp.concatenate([gates_in[k] for k in range(10)] + [jnp.zeros((48, seq), jnp.float32)], axis=0).T
        step = 128
        for c in range(COLORS):
            for role in range(4):
                g = 8 * (9 if role == 0 else ORDERS[c][2] * 3 + role - 1)
                p = 8 * (c * 4 + role)
                for b in range(0, HELD, step):
                    col = (lax.broadcasted_iota(jnp.int32, (seq, step), 1) + b).astype(jnp.float32)
                    val = jnp.zeros((seq, step), jnp.float32)
                    for i in range(8):
                        val = jnp.where(places[:, p + i:p + i + 1] == col, gates[:, g + i:g + i + 1], val)
                    high = val.astype(jnp.bfloat16)
                    rest = val - high.astype(jnp.float32)
                    mid = rest.astype(jnp.bfloat16)
                    low = (rest - mid.astype(jnp.float32)).astype(jnp.bfloat16)
                    for k, piece in enumerate((high, mid, low)):
                        g_mat[c * 4 + role, k * seq:(k + 1) * seq, b:b + step] = piece

    weights = (wq_ref, wk_ref, wv_ref)

    def load(k, i):
        slot = lax.rem(i, depth)
        return pltpu.make_async_copy(weights[k].at[pl.ds(pl.multiple_of(i * piece_rows, piece_rows), piece_rows)], raw.at[slot], raw_sem.at[slot])

    def flatten(k, start, stop):
        step = 64

        def body(i, carry):
            load(k, i).wait()
            for j in range(0, piece_rows, step):
                flat[k, pl.ds(pl.multiple_of(i * piece_rows + j, step), step), :] = raw[lax.rem(i, depth), pl.ds(j, step)].reshape(step, d_model)

            @pl.when(i + depth < pieces)
            def _():
                load(k, i + depth).start()

            return carry

        if start == 0:
            for i in range(depth):
                load(k, i).start()
        lax.fori_loop(start, stop, body, 0)

    head = 128
    pair = 2 * head
    causal = lax.broadcasted_iota(jnp.int32, (seq, seq), 0) >= lax.broadcasted_iota(jnp.int32, (seq, seq), 1)

    def norm():
        side.wait_recv()
        total = jnp.zeros((seq, 1), jnp.float32)
        for c in range(COLORS):
            for slot in range(3):
                wait(got.at[slot, :, SPANS[c]], got_sem.at[slot, c])
        for cols in spans(0, d_model):
            y = x_in[:, cols].astype(jnp.float32) + (got[0, :, cols] + (got[1, :, cols] + got[2, :, cols]))
            y = y.astype(jnp.bfloat16).astype(jnp.float32)
            got[0, :, cols] = y
            total += jnp.sum(y * y, axis=1, keepdims=True)
        inv = lax.rsqrt(total * (1.0 / d_model) + NORM_EPS)
        for cols in spans(0, d_model):
            x_in[:, cols] = (got[0, :, cols] * inv * norm_in[:, cols]).astype(jnp.bfloat16)

    def project(k, p):
        cols = slice(p * pair, (p + 1) * pair)
        qkv[k, :, cols] = jnp.dot(x_in[...], flat[k, :, cols], preferred_element_type=jnp.float32).astype(jnp.bfloat16)

    def softmax(cols):
        scores = jnp.where(causal, tin[:, cols] * (head ** -0.5), -jnp.inf)
        grown = jnp.exp(scores - jnp.max(scores, axis=1, keepdims=True))
        qkv[0, :, cols] = (grown * (1.0 / jnp.sum(grown, axis=1, keepdims=True))).astype(jnp.bfloat16)

    def attend():
        heads = [slice(h * head, (h + 1) * head) for h in range(d_model // head)]
        for k in range(2):
            for p in range(d_model // pair):
                project(k, p)
        for cols in heads:
            tin[:, cols] = lax.dot_general(qkv[0, :, cols], qkv[1, :, cols], (((1,), (1,)), ((), ())), preferred_element_type=jnp.float32)
        for p in range(d_model // pair):
            softmax(heads[2 * p])
            softmax(heads[2 * p + 1])
            project(2, p)
        for cols in heads:
            x_in[:, cols] = jnp.dot(qkv[0, :, cols], qkv[2, :, cols], preferred_element_type=jnp.float32).astype(jnp.bfloat16)

    send_choices()
    phase1()
    side.start()
    phase2(0)
    direct2(0)
    for copy in local + own:
        copy.start()
    flatten(0, 0, 3 * pieces // 4)
    forward1(0)
    flatten(0, 3 * pieces // 4, pieces)
    forward1(1)
    phase2(3)
    direct2(3)
    build_gates()
    flatten(1, 0, 3 * pieces // 4)
    forward2(0)
    phase2(1)
    phase2(2)
    direct2(1)
    direct2(2)
    flatten(1, 3 * pieces // 4, pieces)
    flatten(2, 0, pieces // 4)
    forward2(3)
    flatten(2, pieces // 4, 3 * pieces // 4)
    forward2(1)
    forward2(2)
    for copy in own:
        copy.wait()
    before = None
    for c in range(COLORS):
        for r1 in range(4):
            for r2 in (1, 2, 3):
                wait(held2[c].at[r1, r2 - 1], recv2.at[c, r1, r2])
        for role in (2, 3, 1, 0):
            partial(c, role)
            if before is not None:
                send_sums(*before)
            before = (c, role)
    flatten(2, 3 * pieces // 4, pieces)
    send_sums(*before)
    before = None
    for c in range(COLORS):
        for low in (True, False):
            merge(c, low)
            if before is not None:
                send_merged(*before)
            before = (c, low)
    for copy in local:
        copy.wait()
    send_merged(*before)
    norm()
    attend()
    for p in range(d_model // pair):
        cols = slice(p * pair, (p + 1) * pair)
        out = jnp.dot(x_in[...], wo_in[:, cols], preferred_element_type=jnp.float32).astype(jnp.bfloat16)
        z_ref[:, cols] = (got[0, :, cols] + out.astype(jnp.float32)).astype(jnp.bfloat16)

    side.wait_send()
    for k, (src, dst) in enumerate(choices):
        wait(dst.at[pl.ds(0, 9)], kg_sem.at[0, k])
    for c in range(COLORS):
        wait(held1[c], send_sem.at[0, c])
        wait(held2[c], send_sem.at[1, c])
        wait(sums.at[pl.ds(1, 3), :, SPANS[c]], send_sem.at[2, c])
        wait(tie1[c], send_sem.at[3, c])
        wait(tie2[c], send_sem.at[4, c])
        wait(sums.at[0, :, SPANS[c]], send_sem.at[5, c])


def spans(lo, hi):
    return [slice(b, min(b + 512, hi)) for b in range(lo, hi, 512)]


def run_stage(o_tab, ids, slots, gates, h, norm_w, wq, wk, wv, wo):
    seq, d = h.shape
    dma = pltpu.SemaphoreType.DMA
    piece = 128

    def per_colour(*lead):
        return [pltpu.VMEM(lead + (SLOTS, w), jnp.bfloat16) for w in WIDTHS]

    return pl.pallas_call(
        stage_kernel,
        out_shape=pltpu.VMEM((seq, d), jnp.bfloat16),
        in_specs=[pl.BlockSpec(memory_space=pl.ANY)] * 10,
        out_specs=pl.BlockSpec(memory_space=pltpu.VMEM),
        scratch_shapes=[
            *per_colour(3, 4, 4),
            *per_colour(4, 4),
            *per_colour(4, 3, 4),
            *per_colour(4, 4),
            *per_colour(4),
            pltpu.VMEM((4, seq, d), jnp.float32),
            pltpu.VMEM((seq, d), jnp.float32),
            pltpu.VMEM((3, seq, d), jnp.float32),
            pltpu.VMEM((10,) + ids.shape, jnp.int32),
            pltpu.VMEM((10,) + slots.shape, jnp.int32),
            pltpu.VMEM((10,) + gates.shape, jnp.float32),
            pltpu.VMEM((4 * COLORS, 3 * seq, HELD), jnp.bfloat16),
            pltpu.VMEM(norm_w.shape, jnp.float32),
            pltpu.VMEM((3, d, d), jnp.bfloat16),
            pltpu.VMEM((d, d), jnp.bfloat16),
            pltpu.VMEM((3, piece) + wq.shape[1:], jnp.bfloat16),
            pltpu.VMEM((seq, d), jnp.bfloat16),
            pltpu.VMEM((3, seq, d), jnp.bfloat16),
            dma((2, 3)),
            dma((2,)),
            dma((5,)),
            dma((COLORS,)),
            dma((3,)),
            dma((6, COLORS)),
            dma((COLORS, 5)),
            dma((COLORS, 4, 4)),
            dma((COLORS, 2)),
            dma((3, COLORS)),
        ],
        compiler_params=pltpu.CompilerParams(collective_id=0, has_side_effects=True, vmem_limit_bytes=66400000),
        name='stage',
    )(o_tab, ids, slots, gates, h, norm_w, wq, wk, wv, wo)


def solution(mesh):
    tok_spec = P('pp', 'ep', None, None)
    wt_spec = P('pp', None, None, None)

    def device_step(expert_out, expert_ids, slot_ids, gate_vals, residual, norm_w, w_query, w_key, w_value, w_out):
        seq_len, d_model = residual.shape[2:]

        def choices(array):
            return array.reshape(seq_len, array.shape[3]).T

        result = run_stage(
            expert_out.reshape(SIDE, SIDE, SIDE, SLOTS, d_model),
            choices(expert_ids), choices(slot_ids), choices(gate_vals),
            residual.reshape(seq_len, d_model), norm_w, w_query[0], w_key[0], w_value[0], w_out[0].reshape(-1, d_model),
        )
        return result.reshape(residual.shape)

    return jax.shard_map(device_step, mesh=mesh, in_specs=(tok_spec, tok_spec, tok_spec, tok_spec, tok_spec, P('pp', None), wt_spec, wt_spec, wt_spec, wt_spec), out_specs=tok_spec, check_vma=False)
```
